32 devices in a mesh: dp: 8 (over y, x, core), mp: 4 (over z).
Axes of the slice: x: 2, y: 2, z: 4, core: 2. Of those that a mesh axis runs over, the one named last changes fastest.
Arguments:
- hidden_in: float32 [16384, 768], P(('dp', 'mp')), may hold values from -6 to 6
- first_values: bfloat16 [16384, 384], P('dp', 'mp'), may hold values from -6 to 6
- first_length: int32 [8], P('dp'), may hold values from 1024 to 2048, as said below
- pre_gain: float32 [768], replicated, may hold values from 0.25 to 1.75
- pre_shift: float32 [768], replicated, may hold values from -1.75 to 1.75
- w_query: bfloat16 [768, 768], P(None, 'mp'), may hold values from -0.21875 to 0.21875
- b_query: float32 [768], P('mp'), may hold values from -3 to 3
- w_key: bfloat16 [768, 768], P(None, 'mp'), may hold values from -0.21875 to 0.21875
- w_value: bfloat16 [768, 384], P(None, 'mp'), may hold values from -0.21875 to 0.21875
- b_value: float32 [384], P('mp'), may hold values from -3 to 3
- w_out: bfloat16 [768, 768], P('mp'), may hold values from -1.75 to 1.75
- b_out: float32 [768], replicated, may hold values from -3 to 3
- mid_gain: float32 [768], replicated, may hold values from 0.25 to 1.75
- mid_shift: float32 [768], replicated, may hold values from -1.75 to 1.75
- w_up: bfloat16 [768, 3072], P(None, 'mp'), may hold values from -0.21875 to 0.21875
- b_up: float32 [3072], P('mp'), may hold values from -3 to 3
- w_down: bfloat16 [3072, 768], P('mp'), may hold values from -0.109375 to 0.109375
- b_down: float32 [768], replicated, may hold values from -3 to 3
- grad_out: float32 [16384, 768], P(('dp', 'mp')), may hold values from -6 to 6
Outputs:
- layer_out: float32 [16384, 768], P(('dp', 'mp'))
- grad_in: float32 [16384, 768], P(('dp', 'mp'))
- grad_first_values: float32 [16384, 384], P('dp', 'mp')
- grad_pre_gain: float32 [768], replicated
- grad_pre_shift: float32 [768], replicated
- grad_w_query: float32 [768, 768], P(None, 'mp')
- grad_b_query: float32 [768], P('mp')
- grad_w_key: float32 [768, 768], P(None, 'mp')
- grad_w_value: float32 [768, 384], P(None, 'mp')
- grad_b_value: float32 [384], P('mp')
- grad_w_out: float32 [768, 768], P('mp')
- grad_b_out: float32 [768], replicated
- grad_mid_gain: float32 [768], replicated
- grad_mid_shift: float32 [768], replicated
- grad_w_up: float32 [768, 3072], P(None, 'mp')
- grad_b_up: float32 [3072], P('mp')
- grad_w_down: float32 [3072, 768], P('mp')
- grad_b_down: float32 [768], replicated
The draws below stay inside these ranges and needn't reach their ends.
Inputs may be any that keep to these rules, and one draw needn't show every extreme that they name: `first_length`: each entry is 2048 / 2 (two documents in the block) or 2048 (one document); half of the entries take each value.
All inputs are finite; a program needn't handle non-finite values.
Results may differ from the reference program's by a relative error of at most 0.02.
Values may be sent and summed in bfloat16 or wider, within the bound.
A program may use at most 192 MiB of HBM per device.

```python
import jax
import jax.numpy as jnp
from jax import lax

D = 768
HEADS = 12
HEAD_DIM = 64
FF = 3072
FRESH = 6
TOK_DEV = 2048
TOKENS = 16384
N_DP = 8


def draw_first_length(key, part):
    order = jax.random.permutation(key, N_DP)
    return jnp.where(order < N_DP // 2, TOK_DEV, TOK_DEV // 2).astype(jnp.int32)


def level_of(own_key, dims, shards, least, largest):
    loudness, own = 1.0, jax.random.fold_in(own_key, 6)
    for dim, parts in shards:
        draws = jnp.exp(jax.random.uniform(jax.random.fold_in(own, dim), (parts,), jnp.float32, least / len(shards), largest / len(shards)))
        loudness = loudness * jnp.repeat(draws, dims[dim] // parts).reshape([-1 if axis == dim else 1 for axis in range(len(dims))])
    return loudness


def gaussian(rng, dims, scale, reach, pieces=(), held_as=jnp.bfloat16):
    array = scale * jax.random.normal(rng, dims, jnp.float32)
    if pieces:
        array = array * level_of(rng, dims, pieces, -0.22, 0.18)
    return jnp.clip(array, -reach, reach).astype(held_as)


def setup_inputs(seed: int = 0) -> dict:
    arg_keys = jax.random.split(jax.random.key(seed), 20)
    return {
        "hidden_in": gaussian(arg_keys[0], (TOKENS, D), 1.0, 6.0, ((0, 32),), jnp.float32),
        "first_values": gaussian(arg_keys[1], (TOKENS, FRESH * HEAD_DIM), 1.0, 6.0, ((0, 8), (1, 4))),
        "first_length": draw_first_length(jax.random.fold_in(arg_keys[19], 71), 0),
        "pre_gain": jnp.clip(1.0 + 0.15 * jax.random.normal(arg_keys[3], (D,), jnp.float32), 0.25, 1.75),
        "pre_shift": gaussian(arg_keys[4], (D,), 0.3, 1.75, (), jnp.float32),
        "w_query": gaussian(arg_keys[5], (D, D), D ** -0.5, 0.21875, ((1, 4),)),
        "b_query": gaussian(arg_keys[6], (D,), 0.5, 3.0, ((0, 4),), jnp.float32),
        "w_key": gaussian(arg_keys[7], (D, D), D ** -0.5, 0.21875, ((1, 4),)),
        "w_value": gaussian(arg_keys[8], (D, FRESH * HEAD_DIM), D ** -0.5, 0.21875, ((1, 4),)),
        "b_value": gaussian(arg_keys[9], (FRESH * HEAD_DIM,), 0.5, 3.0, ((0, 4),), jnp.float32),
        "w_out": gaussian(arg_keys[10], (D, D), (max(D // 64, 1)) ** -0.5, 1.75, ((0, 4),)),
        "b_out": gaussian(arg_keys[11], (D,), 0.5, 3.0, (), jnp.float32),
        "mid_gain": jnp.clip(1.0 + 0.15 * jax.random.normal(arg_keys[12], (D,), jnp.float32), 0.25, 1.75),
        "mid_shift": gaussian(arg_keys[13], (D,), 0.3, 1.75, (), jnp.float32),
        "w_up": gaussian(arg_keys[14], (D, FF), D ** -0.5, 0.21875, ((1, 4),)),
        "b_up": gaussian(arg_keys[15], (FF,), 0.5, 3.0, ((0, 4),), jnp.float32),
        "w_down": gaussian(arg_keys[16], (FF, D), FF ** -0.5, 0.109375, ((0, 4),)),
        "b_down": gaussian(arg_keys[17], (D,), 0.5, 3.0, (), jnp.float32),
        "grad_out": gaussian(arg_keys[18], (TOKENS, D), 1.0, 6.0, ((0, 32),), jnp.float32),
    }


@jax.custom_vjp
def low(v):
    return lax.optimization_barrier(v.astype(jnp.bfloat16)).astype(jnp.float32)

@jax.custom_vjp
def low_back(v):
    return v

def low_keep(v):
    return (low(v), None)

def low_pass(kept, grad):
    return (grad,)

def back_keep(v):
    return (v, None)

def back_low(kept, grad):
    return (low(grad),)
low.defvjp(low_keep, low_pass)
low_back.defvjp(back_keep, back_low)
EPSILON = 1e-05

def layer_norm(values, gain, shift):
    center = values - lax.optimization_barrier(jnp.mean(values, -1, keepdims=True))
    spread = lax.optimization_barrier(jnp.mean(center * center, -1, keepdims=True))
    return center * lax.rsqrt(spread + EPSILON) * gain + shift

def gelu_tanh(values):
    return 0.5 * values * (1.0 + jnp.tanh(0.7978845608028654 * (values + 0.044715 * values * values * values)))

def matmul(left, right):
    return jnp.dot(left, right, precision=lax.Precision.HIGHEST, preferred_element_type=jnp.float32)

def group_layer(params, hidden_in, first_values, first_length):
    pre_gain, pre_shift, w_query, b_query, w_key, w_value, b_value, w_out, b_out, mid_gain, mid_shift, w_up, b_up, w_down, b_down = params
    length = hidden_in.shape[0]
    normed = low(layer_norm(hidden_in, pre_gain, pre_shift))
    queries = low(low_back(matmul(normed, w_query) + b_query))
    keys_all = low(low_back(matmul(normed, w_key)))
    fresh_values = low(low_back(matmul(normed, w_value) + b_value))
    values_all = jnp.concatenate([fresh_values, first_values], 1)
    heads_query = queries.reshape(length, HEADS, HEAD_DIM)
    heads_key = keys_all.reshape(length, HEADS, HEAD_DIM)
    heads_value = values_all.reshape(length, HEADS, HEAD_DIM)
    position = jnp.arange(length, dtype=jnp.int32)
    second = position >= first_length
    allowed = (position[None, :] <= position[:, None]) & (second[None, :] == second[:, None])
    scores = low_back(jnp.einsum('qhd,khd->hqk', heads_query, heads_key, precision=lax.Precision.HIGHEST) * HEAD_DIM ** (-0.5))
    scores = jnp.where(allowed[None], scores, -1e+30)
    row_max = lax.optimization_barrier(jnp.max(scores, -1, keepdims=True))
    exponent = jnp.exp(scores - row_max)
    probabilities = low(exponent / lax.optimization_barrier(jnp.sum(exponent, -1, keepdims=True)))
    context = jnp.einsum('hqk,khd->qhd', probabilities, heads_value, precision=lax.Precision.HIGHEST).reshape(length, HEADS * HEAD_DIM)
    context = low(low_back(context))
    attended = low_back(matmul(context, w_out) + b_out)
    middle = hidden_in + attended
    normed_mid = low(layer_norm(middle, mid_gain, mid_shift))
    up_values = low_back(matmul(normed_mid, w_up) + b_up)
    activated = low(gelu_tanh(up_values))
    return middle + low_back(matmul(activated, w_down) + b_down)

def reference(hidden_in, first_values, first_length, pre_gain, pre_shift, w_query, b_query, w_key, w_value, b_value, w_out, b_out, mid_gain, mid_shift, w_up, b_up, w_down, b_down, grad_out):
    params = tuple((item.astype(jnp.float32) for item in (pre_gain, pre_shift, w_query, b_query, w_key, w_value, b_value, w_out, b_out, mid_gain, mid_shift, w_up, b_up, w_down, b_down)))
    blocks_in = hidden_in.astype(jnp.float32).reshape(N_DP, TOK_DEV, D)
    blocks_first = first_values.astype(jnp.float32).reshape(N_DP, TOK_DEV, FRESH * HEAD_DIM)
    blocks_grad = grad_out.astype(jnp.float32).reshape(N_DP, TOK_DEV, D)
    lengths = first_length.astype(jnp.int32)

    def forward(weights, inputs, firsts):

        def one_group(items):
            return group_layer(weights, items[0], items[1], items[2])
        return lax.map(jax.checkpoint(one_group), (inputs, firsts, lengths))
    result, pullback = jax.vjp(forward, params, blocks_in, blocks_first)
    grad_params, grad_input, grad_first = pullback(blocks_grad)
    return (result.reshape(TOKENS, D), grad_input.reshape(TOKENS, D), grad_first.reshape(TOKENS, FRESH * HEAD_DIM), grad_params[0], grad_params[1], grad_params[2], grad_params[3], grad_params[4], grad_params[5], grad_params[6], grad_params[7], grad_params[8], grad_params[9], grad_params[10], grad_params[11], grad_params[12], grad_params[13], grad_params[14])
```

```python
import functools

import jax
import jax.numpy as jnp
from jax import lax
from jax.experimental import pallas as pl
from jax.experimental.pallas import tpu as pltpu
from jax.sharding import PartitionSpec as P

HEAD_DIM = 64
EPSILON = 1e-05
NEG_LARGE = -1e30
MESH = pl.DeviceIdType.MESH
BF = jnp.bfloat16
F32 = jnp.float32
ANY = pl.BlockSpec(memory_space=pl.ANY)
VM = pl.BlockSpec(memory_space=pltpu.VMEM)
SM = pl.BlockSpec(memory_space=pltpu.SMEM)
VMEM_LIMIT = 60 << 20
LANE = 128
PLANE = 8
RING = 4
HEADS_AT = ((0, 1, 6), (2, 7, 8), (3, 9, 10), (4, 5, 11))
FRESH = ((0, 0, 96, 0, 0), (1, 0, 32, 0, 96), (1, 32, 64, 1, 0), (2, 0, 64, 2, 0), (2, 64, 32, 3, 0), (3, 0, 96, 3, 32))
KEPT = ((0, 0, 64, 128), (1, 0, 96, 96), (2, 0, 96, 64), (3, 32, 64, 128))
MOVED = ((0, 64, 32, 1, 64), (3, 0, 32, 2, 160))


def dot(left, right, left_dim, right_dim):
    return lax.dot_general(
        left, right, (((left_dim,), (right_dim,)), ((), ())), preferred_element_type=F32
    )


def layer_norm(values, gain, shift):
    center = values - jnp.mean(values, -1, keepdims=True)
    spread = jnp.mean(center * center, -1, keepdims=True)
    return center * lax.rsqrt(spread + EPSILON) * gain + shift


def gelu_tanh(values):
    return (
        0.5
        * values
        * (1.0 + jnp.tanh(0.7978845608028654 * (values + 0.044715 * values * values * values)))
    )


def lanes(start, size):
    return pl.ds(pl.multiple_of(start, LANE), size)


def rows_of(start, size, unit):
    return pl.ds(pl.multiple_of(start, unit), size)


class Place:
    def __init__(self, ring, planes=1):
        self.ring = ring
        self.planes = planes
        self.d = lax.axis_index("dp")
        self.m = lax.axis_index("mp")
        d = self.d
        self.core = lax.rem(d, 2)
        self.x = lax.rem(d // 2, 2)
        self.y = lax.rem(d // 4, 2)
        self.to_core = (d + 1 - 2 * self.core, self.m)
        self.to_x = (d + 2 - 4 * self.x, self.m)
        self.to_y = (d + 4 - 8 * self.y, self.m)
        self.pair = self.m + 1 - 2 * lax.rem(self.m, 2)
        self.across = lax.rem(self.m + 2, RING)
        self.corner = RING - 1 - self.m

    def z(self, shift):
        return lax.rem(self.m + shift, self.ring)

    def to_z(self, shift):
        return (self.d, self.z(shift))

    def shift_to(self, position):
        return lax.rem(position - self.m + self.ring, self.ring)

    def head(self, slot):
        value = HEADS_AT[RING - 1][slot]
        for k in range(RING - 1):
            value = jnp.where(self.m == k, HEADS_AT[k][slot], value)
        return value

    def steps(self):
        return [PLANE << b for b in range(self.planes.bit_length() - 1)]

    def to_plane(self, step):
        return (self.d + step - 2 * step * lax.rem(self.d // step, 2), self.m)

    def barrier(self):
        sem = pltpu.get_barrier_semaphore()
        peers = [self.to_z(j) for j in range(1, self.ring)]
        peers += [self.to_core, self.to_x, self.to_y]
        peers += [self.to_plane(step) for step in self.steps()]
        for peer in peers:
            pl.semaphore_signal(sem, inc=1, device_id=peer, device_id_type=MESH)
        pl.semaphore_wait(sem, len(peers))

    def slot(self, x_first):
        if x_first:
            return self.core * 4 + self.y * 2 + self.x
        return self.core * 4 + self.x * 2 + self.y


def remote(src, dst, send, recv, device):
    return pltpu.make_async_remote_copy(
        src_ref=src,
        dst_ref=dst,
        send_sem=send,
        recv_sem=recv,
        device_id=device,
        device_id_type=MESH,
    )


class Gather:
    def __init__(self, place, src, dst, send, recv, item, first_row, rows, x_first):
        self.place, self.src, self.dst = place, src, dst
        self.send, self.recv, self.item = send, recv, item
        self.first_row, self.part, self.x_first = first_row, rows // PLANE, x_first

    def window(self, start, size):
        part = self.part
        return rows_of(self.first_row + start * part, size * part, part & -part)

    def copy(self, stage, k):
        place = self.place
        slot = place.slot(self.x_first)
        near, far = (place.to_x, place.to_y) if self.x_first else (place.to_y, place.to_x)
        shard = (place.across, place.pair, place.corner)[k]
        window = self.window(slot, 1)
        if stage == 0:
            shard, target = place.m, (place.d, place.across)
        elif stage == 1:
            shard, target = (place.m, place.across)[k], (place.d, place.pair)
        elif stage == 2:
            target = near
        elif stage == 3:
            window, target = self.window((slot // 2) * 2, 2), far
        else:
            window, target = self.window(place.core * 4, 4), place.to_core
        own = stage == 0 or (stage == 1 and k == 0)
        source = self.src.at[window] if own else self.dst.at[shard, window]
        return remote(
            source,
            self.dst.at[shard, window],
            self.send.at[self.item, stage, k],
            self.recv.at[self.item, stage, k],
            target,
        )

    def start(self, stage):
        if stage == 0:
            self.copy(0, 0).start()
            self.copy(1, 0).start()
        elif stage == 1:
            self.copy(0, 0).wait_recv()
            self.copy(1, 1).start()
        else:
            for k in range(2 if stage == 2 else 3):
                self.copy(stage - 1, k).wait_recv()
            for k in range(3):
                self.copy(stage, k).start()

    def arrive(self):
        for k in range(3):
            self.copy(4, k).wait_recv()

    def drain(self):
        for stage, copies in enumerate((1, 2, 3, 3, 3)):
            for k in range(copies):
                self.copy(stage, k).wait_send()


class Reduce:
    def __init__(self, place, src, bufs, out, send, recv, item, x_first):
        self.place, self.src, self.out = place, src, out
        self.r_core, self.r_far, self.r_near, self.r_z, self.r_plane = bufs
        self.send, self.recv, self.item, self.x_first = send, recv, item, x_first
        self.part = out.shape[0] // PLANE
        if x_first:
            self.near, self.far = place.to_x, place.to_y
            self.near_bit, self.far_bit = place.x, place.y
        else:
            self.near, self.far = place.to_y, place.to_x
            self.near_bit, self.far_bit = place.y, place.x

    def rows(self, start, size):
        return rows_of(start * self.part, size * self.part, self.part & -self.part)

    def copy(self, stage, k):
        place = self.place
        if stage == 0:
            src = self.src.at[k, self.rows((1 - place.core) * 4, 4)]
            dst, target = self.r_core.at[k], place.to_core
        elif stage == 1:
            src = self.r_core.at[k, self.rows((1 - self.far_bit) * 2, 2)]
            dst, target = self.r_far.at[k], self.far
        elif stage == 2:
            src = self.r_far.at[k, self.rows(1 - self.near_bit, 1)]
            dst, target = self.r_near.at[k], self.near
        elif stage == 3:
            src = self.r_near.at[(place.pair, place.corner)[k]]
            dst, target = self.r_z.at[k], (place.d, place.pair)
        elif stage == 4:
            src = self.r_near.at[place.across]
            dst, target = self.r_z.at[2], (place.d, place.across)
        else:
            slot = place.slot(self.x_first)
            if stage == 5:
                window, target = self.rows(slot, 1), self.near
            elif stage == 6:
                window, target = self.rows((slot // 2) * 2, 2), self.far
            else:
                window, target = self.rows(place.core * 4, 4), place.to_core
            src = dst = self.out.at[window]
        return remote(
            src, dst, self.send.at[self.item, stage, k], self.recv.at[self.item, stage, k], target
        )

    def members(self, stage):
        return range((RING, RING, RING, 2, 1, 1, 1, 1)[stage])

    def start(self, stage):
        for k in self.members(stage):
            self.copy(stage, k).start()

    def wait(self, stage):
        for k in self.members(stage):
            self.copy(stage, k).wait_recv()

    def fold_one(self, stage, k):
        place, part = self.place, self.part
        if stage == 0:
            kept, base, into, size = self.src, place.core * 4 * part, self.r_core, 4 * part
        elif stage == 1:
            kept, base, into, size = self.r_core, self.far_bit * 2 * part, self.r_far, 2 * part
        else:
            kept, base, into, size = self.r_far, self.near_bit * part, self.r_near, part
        unit = part & -part
        step = min(part, 32)
        self.copy(stage, k).wait_recv()

        def add(i, carry):
            mine = kept[k, rows_of(base + i * step, step, min(unit, step)), :].astype(F32)
            here = rows_of(i * step, step, step)
            into[k, here, :] = (into[k, here, :].astype(F32) + mine).astype(BF)
            return carry

        lax.fori_loop(0, size // step, add, 0)
        if stage < 2:
            self.copy(stage + 1, k).start()

    def fold(self, stage):
        for k in self.members(stage):
            self.fold_one(stage, k)
        if stage == 2:
            self.start(3)

    def fold_pair(self):
        place = self.place
        self.wait(3)
        other = self.r_near[place.across].astype(F32) + self.r_z[1].astype(F32)
        self.r_near[place.across] = other.astype(BF)
        self.start(4)
        mine = self.r_near[place.m].astype(F32) + self.r_z[0].astype(F32)
        self.r_near[place.m] = mine.astype(BF)

    def finish_sum(self):
        place = self.place
        self.wait(4)
        here = self.rows(place.slot(self.x_first), 1)
        value = self.r_near[place.m].astype(F32) + self.r_z[2].astype(F32)
        self.out[here, :] = value.astype(BF)
        for b, step in enumerate(place.steps()):
            copy = remote(
                self.out.at[here],
                self.r_plane.at[b],
                self.send.at[self.item, 8 + b, 0],
                self.recv.at[self.item, 8 + b, 0],
                place.to_plane(step),
            )
            copy.start()
            copy.wait()
            mine = self.out[here, :].astype(F32)
            self.out[here, :] = (mine + self.r_plane[b].astype(F32)).astype(BF)
        self.start(5)

    def spread(self, stage):
        self.wait(stage - 1)
        self.start(stage)

    def drain(self, first):
        for stage in range(first, 8):
            for k in self.members(stage):
                self.copy(stage, k).wait_send()

    @staticmethod
    def buffers(rows, width, planes):
        part = rows // PLANE
        extra = max(planes.bit_length() - 1, 1)
        return [
            pltpu.VMEM((RING, 4 * part, width), BF),
            pltpu.VMEM((RING, 2 * part, width), BF),
            pltpu.VMEM((RING, part, width), BF),
            pltpu.VMEM((3, part, width), BF),
            pltpu.VMEM((extra, part, width), BF),
        ]


def diagonal_mask(scores, key_start, query_start):
    keys = lax.broadcasted_iota(jnp.int32, scores.shape, 0) + key_start
    queries = lax.broadcasted_iota(jnp.int32, scores.shape, 1) + query_start
    return keys <= queries


def other_document(boundary, key_start, query_start):
    crossing = jnp.logical_and(boundary > key_start, boundary <= query_start)
    return jnp.where(crossing, NEG_LARGE, 0.0)


def forward_kernel(
    ring,
    heads_here,
    length_ref,
    hidden_ref,
    gain_ref,
    shift_ref,
    wt_ref,
    bias_ref,
    first_ref,
    wo_ref,
    wu_ref,
    wd_ref,
    context_ref,
    normed_ref,
    qk_ref,
    v_ref,
    lse_ref,
    exact_ref,
    wt_all,
    bias_all,
    wo_far,
    wu_far,
    wd_far,
    y_send,
    vy_send,
    c_send,
    keys,
    gsend,
    grecv,
    bsend,
    brecv,
    qsend,
    qrecv,
    vsend,
    vrecv,
    fsend,
    frecv,
    csend,
    crecv,
):
    place = Place(ring)
    m = place.m
    count = hidden_ref.shape[0]
    total = ring * count
    piece = first_ref.shape[0]
    half = total // 2
    hd = HEAD_DIM
    pack_rows = wt_ref.shape[0]
    place.barrier()
    half_pack = pack_rows // 2
    small = [
        Gather(place, wt_ref, wt_all, gsend, grecv, i, i * half_pack, half_pack, i == 0)
        for i in range(2)
    ]
    big = [
        Gather(place, wo_ref, wo_far, gsend, grecv, 2, 0, wo_ref.shape[0], True),
        Gather(place, wu_ref, wu_far, gsend, grecv, 3, 0, wu_ref.shape[0], True),
        Gather(place, wd_ref, wd_far, gsend, grecv, 4, 0, wd_ref.shape[0], False),
    ]
    for item in small:
        item.start(0)

    def bias_copy(j):
        return remote(
            bias_ref, bias_all.at[m], bsend.at[j - 1], brecv.at[j - 1], place.to_z(j)
        )

    for j in range(1, ring):
        bias_copy(j).start()

    def moved_copy(i):
        _, row, rows, to, row_there = MOVED[i]
        return remote(
            first_ref.at[pl.ds(row, rows)],
            v_ref.at[pl.ds(row_there, rows)],
            fsend.at[0],
            frecv.at[0],
            (place.d, to),
        )

    for i, move in enumerate(MOVED):

        @pl.when(m == move[0])
        def _(i=i):
            moved_copy(i).start()

    for at, row, rows, row_there in KEPT:

        @pl.when(m == at)
        def _(row=row, rows=rows, row_there=row_there):
            v_ref[row_there : row_there + rows, :] = first_ref[row : row + rows, :]

    for item in big:
        item.start(0)

    normed_ref[...] = layer_norm(hidden_ref[...], gain_ref[...], shift_ref[...]).astype(BF)
    wt_all[m] = wt_ref[...]
    bias_all[m] = bias_ref[...]

    for stage in (1, 2):
        for item in small:
            item.start(stage)
    for item in big:
        item.start(1)
    for stage in (3, 4):
        for item in small:
            item.start(stage)
    for j in range(1, ring):
        bias_copy(j).wait_recv()
    for item in small:
        item.arrive()

    own = lanes(m * count, count)

    def qk_copy(slot, to):
        return remote(
            y_send.at[to, slot],
            qk_ref.at[slot, :, own],
            qsend.at[to, slot],
            qrecv.at[slot, place.shift_to(to) - 1],
            (place.d, to),
        )

    def v_copy(i):
        shard, row, rows, to, row_there = FRESH[i]
        return remote(
            vy_send.at[shard, pl.ds(row, rows)],
            v_ref.at[pl.ds(row_there, rows), own],
            vsend.at[i],
            vrecv.at[i, place.shift_to(to) - 1],
            (place.d, to),
        )

    where_is = {head: (to, slot) for to, heads in enumerate(HEADS_AT) for slot, head in enumerate(heads)}
    v_row = 2 * hd * heads_here

    for shard in range(ring):
        out = dot(wt_all[shard], normed_ref[...], 1, 1)
        out = out + jnp.transpose(bias_all[shard, :, 0:pack_rows])[:, 0:1]
        for i in range(heads_here):
            to, slot = where_is[heads_here * shard + i]
            row = 2 * hd * i
            y_send[to, slot, 0:hd, :] = (out[row : row + hd] * (hd**-0.5)).astype(BF)
            y_send[to, slot, hd : 2 * hd, :] = out[row + hd : row + 2 * hd].astype(BF)
        vy_send[shard] = out[v_row : v_row + piece].astype(BF)

    def share(slot):
        for to in range(ring):

            @pl.when(m == to)
            def _(to=to):
                qk_ref[slot, :, own] = y_send[to, slot]

            @pl.when(m != to)
            def _(to=to):
                qk_copy(slot, to).start()

    share(0)
    for i, (shard, row, rows, to, row_there) in enumerate(FRESH):

        @pl.when(m == to)
        def _(shard=shard, row=row, rows=rows, row_there=row_there):
            v_ref[row_there : row_there + rows, own] = vy_send[shard, row : row + rows, :]

        @pl.when(m != to)
        def _(i=i):
            v_copy(i).start()

    for slot in range(1, heads_here):
        share(slot)

    def qk_arrive(slot):
        for shift in range(1, ring):
            remote(
                y_send.at[0, slot],
                qk_ref.at[slot, :, own],
                qsend.at[0, slot],
                qrecv.at[slot, shift - 1],
                place.to_z(shift),
            ).wait_recv()

    qk_arrive(0)
    for i, (shard, row, rows, to, row_there) in enumerate(FRESH):

        @pl.when(m == to)
        def _(i=i, shard=shard, row=row, rows=rows, row_there=row_there):
            for shift in range(1, ring):
                remote(
                    vy_send.at[shard, pl.ds(row, rows)],
                    v_ref.at[pl.ds(row_there, rows), own],
                    vsend.at[i],
                    vrecv.at[i, shift - 1],
                    place.to_z(shift),
                ).wait_recv()

    for i, move in enumerate(MOVED):

        @pl.when(m == move[3])
        def _(i=i):
            moved_copy(i).wait_recv()

    boundary = length_ref[0]
    block = count

    def context_copy(h, j):
        return remote(
            c_send.at[pl.ds(hd * h, hd), lanes(place.z(j) * count, count)],
            context_ref.at[rows_of(place.head(h) * hd, hd, hd)],
            csend.at[h, j - 1],
            crecv.at[h, j - 1],
            place.to_z(j),
        )

    for h in range(heads_here):
        if h > 0:
            qk_arrive(h)
        keys[...] = jnp.transpose(qk_ref[h, hd : 2 * hd, :])
        for qi in range(ring):
            query_start = qi * block
            q = qk_ref[h, 0:hd, query_start : query_start + block]
            top = None
            for ki in range(qi + 1):
                key_start = ki * block
                v = v_ref[hd * h : hd * h + hd, key_start : key_start + block]
                scores = dot(keys[key_start : key_start + block, :], q, 1, 0)
                if ki == qi:
                    scores = jnp.where(
                        diagonal_mask(scores, key_start, query_start), scores, NEG_LARGE
                    )
                elif key_start < half <= query_start:
                    scores = scores + other_document(boundary, key_start, query_start)
                block_top = jnp.max(scores, 0, keepdims=True)
                new_top = block_top if top is None else jnp.maximum(top, block_top)
                p = jnp.exp(scores - new_top)
                p_sum = jnp.sum(p, 0, keepdims=True)
                part = dot(v, p.astype(BF), 1, 0)
                if top is None:
                    run_sum, running = p_sum, part
                else:
                    factor = jnp.exp(top - new_top)
                    run_sum = run_sum * factor + p_sum
                    running = running * factor + part
                top = new_top
            result = running / run_sum
            exact_ref[hd * h : hd * h + hd, query_start : query_start + block] = result
            c_send[hd * h : hd * h + hd, query_start : query_start + block] = result.astype(BF)
            lse_ref[h, :, query_start : query_start + block] = top + jnp.log(run_sum)
        for j in range(1, ring):
            context_copy(h, j).start()
        context_ref[rows_of(place.head(h) * hd, hd, hd), :] = c_send[hd * h : hd * h + hd, own]
        for item in big:
            item.start(2 + h)

    for item in big:
        item.arrive()
    for h in range(heads_here):
        for j in range(1, ring):
            context_copy(h, j).wait_recv()
    for item in small + big:
        item.drain()
    for j in range(1, ring):
        bias_copy(j).wait_send()
        for h in range(heads_here):
            context_copy(h, j).wait_send()
    for to in range(ring):

        @pl.when(m != to)
        def _(to=to):
            for slot in range(heads_here):
                qk_copy(slot, to).wait_send()

    for i, (shard, row, rows, to, row_there) in enumerate(FRESH):

        @pl.when(m != to)
        def _(i=i):
            v_copy(i).wait_send()

    for i, move in enumerate(MOVED):

        @pl.when(m == move[0])
        def _(i=i):
            moved_copy(i).wait_send()


def forward_call(ring, heads_here, length, hidden, gain, shift, wt, bias, first_t, wo, wu, wd):
    count, width = hidden.shape
    total = ring * count
    hd = HEAD_DIM
    piece = first_t.shape[0]
    others = ring - 1
    sds = jax.ShapeDtypeStruct
    dma = pltpu.SemaphoreType.DMA
    return pl.pallas_call(
        functools.partial(forward_kernel, ring, heads_here),
        out_shape=(
            sds((ring * heads_here * hd, count), BF),
            sds((count, width), BF),
            sds((heads_here, 2 * hd, total), BF),
            sds((heads_here * hd, total), BF),
            sds((heads_here, 1, total), F32),
            sds((heads_here * hd, total), F32),
            sds((ring,) + wt.shape, BF),
            sds((ring,) + bias.shape, F32),
            sds((ring,) + wo.shape, BF),
            sds((ring,) + wu.shape, BF),
            sds((ring,) + wd.shape, BF),
        ),
        in_specs=[SM] + [VM] * 6 + [ANY] * 3,
        out_specs=[VM] * 8 + [ANY] * 3,
        scratch_shapes=[
            pltpu.VMEM((ring, heads_here, 2 * hd, count), BF),
            pltpu.VMEM((ring, piece, count), BF),
            pltpu.VMEM((heads_here * hd, total), BF),
            pltpu.VMEM((total, hd), BF),
            dma((5, 5, 3)),
            dma((5, 5, 3)),
            dma((others,)),
            dma((others,)),
            dma((ring, heads_here)),
            dma((heads_here, others)),
            dma((len(FRESH),)),
            dma((len(FRESH), others)),
            dma((1,)),
            dma((1,)),
            dma((heads_here, others)),
            dma((heads_here, others)),
        ],
        compiler_params=pltpu.CompilerParams(
            collective_id=0, has_side_effects=True, vmem_limit_bytes=VMEM_LIMIT
        ),
        name="forward",
    )(length, hidden, gain, shift, wt, bias, first_t, wo, wu, wd)


def backward_kernel(
    ring,
    heads_here,
    planes,
    length_ref,
    context_ref,
    hidden_ref,
    grad_out_ref,
    pre_gain_ref,
    rows_ref,
    bias_ref,
    qk_hbm,
    v_hbm,
    lse_hbm,
    exact_hbm,
    normed_hbm,
    wt_hbm,
    wo_hbm,
    wo_far_hbm,
    wu_hbm,
    wu_far_hbm,
    wd_hbm,
    wd_far_hbm,
    layer_ref,
    grad_in_ref,
    first_ref,
    pack_sum,
    wo_sum,
    wu_sum,
    wd_sum,
    vector_sum,
    qk_ref,
    v_ref,
    lse_ref,
    exact_ref,
    normed_ref,
    wt_all,
    wo_all,
    wu_all,
    wd_all,
    middle_ref,
    mid_ref,
    mid_t,
    down_ref,
    down_t,
    act_ref,
    gup_ref,
    wo_share,
    g_all,
    keys,
    vals,
    delta,
    dq,
    dqk_send,
    dv_send,
    grad_ref,
    vector_held,
    vector_came,
    lsem,
    gsend,
    grecv,
    qsend,
    qrecv,
    vsend,
    vrecv,
    fsend,
    frecv,
    rsend,
    rrecv,
    wsend,
    wrecv,
    *bufs,
):
    place = Place(ring, planes)
    m = place.m
    count, width = hidden_ref.shape
    total = ring * count
    half = total // 2
    hd = HEAD_DIM
    piece = first_ref.shape[0]
    out_rows = wo_hbm.shape[0]
    pack_lanes = grad_ref.shape[1]
    tile = count // 4
    own = lanes(m * count, count)

    def shard_of(j):
        return lax.rem(m - j + ring, ring)

    loads = {}

    def load(name, src, dst):
        loads[name] = pltpu.make_async_copy(src, dst, lsem.at[len(loads)])
        loads[name].start()

    for j in range(ring):
        into = wo_all.at[rows_of(shard_of(j) * out_rows, out_rows, 16)]
        load(("wo", j), wo_hbm if j == 0 else wo_far_hbm.at[shard_of(j)], into)
    for j in range(ring):
        s = shard_of(j)
        load(("wu", j), wu_hbm if j == 0 else wu_far_hbm.at[s], wu_all.at[s])
        load(("wd", j), wd_hbm if j == 0 else wd_far_hbm.at[s], wd_all.at[s])
    load("v", v_hbm, v_ref)
    load("qk", qk_hbm, qk_ref)
    load("lse", lse_hbm, lse_ref)
    load("exact", exact_hbm, exact_ref)
    load("normed", normed_hbm, normed_ref)
    load("wt", wt_hbm, wt_all)
    place.barrier()

    def row(i):
        return rows_ref[i : i + 1, :]

    b_out, mid_gain, mid_shift, b_down = row(0), row(1), row(2), row(3)
    act_ref[...] = jnp.transpose(context_ref[...])
    vector_held[0] = jnp.zeros_like(vector_held[0])
    wo_share[:, out_rows:, :] = jnp.zeros_like(wo_share[:, out_rows:, :])
    grad_ref[:, 2 * hd * heads_here + piece :, :] = jnp.zeros_like(
        grad_ref[:, 2 * hd * heads_here + piece :, :]
    )
    for j in range(ring):
        loads[("wo", j)].wait()

    def project(i, carry):
        here = rows_of(i * tile, tile, tile)
        attended = dot(act_ref[here, :], wo_all[...], 1, 0) + b_out
        middle = hidden_ref[here, :] + attended
        middle_ref[here, :] = middle
        layer_ref[here, :] = middle + b_down
        mid_ref[here, :] = layer_norm(middle, mid_gain, mid_shift).astype(BF)
        grad_down = grad_out_ref[here, :].astype(BF)
        down_ref[here, :] = grad_down
        grad_in_ref[here, :] = jnp.zeros((tile, width), F32)
        return carry + jnp.sum(grad_down.astype(F32), 0, keepdims=True)

    zero_row = jnp.zeros((1, width), F32)
    grad_b_down = lax.fori_loop(0, count // tile, project, zero_row)
    mid_t[...] = jnp.transpose(mid_ref[...])
    down_t[...] = jnp.transpose(down_ref[...])

    down = Reduce(place, wd_all, bufs[0:5], wd_sum, rsend, rrecv, 0, False)
    up = Reduce(place, wu_all, bufs[5:10], wu_sum, rsend, rrecv, 1, True)
    out = Reduce(place, wo_share, bufs[10:15], wo_sum, rsend, rrecv, 2, True)
    pack = Reduce(
        place, wu_all.at[:, pl.ds(0, pack_lanes)], bufs[15:20], pack_sum, rsend, rrecv, 3, True
    )

    big = count // 2
    for j in range(ring):
        loads[("wu", j)].wait()
        loads[("wd", j)].wait()
        s = shard_of(j)
        b_up = bias_ref[s, 0:1, pack_lanes:]

        def feed(i, carry, j=s, b_up=b_up):
            here = rows_of(i * big, big, big)
            u = dot(mid_ref[here, :], wu_all[j], 1, 0) + b_up
            grad_act = dot(down_ref[here, :], wd_all[j], 1, 1)
            square = u * u
            t = jnp.tanh(0.7978845608028654 * (u + 0.044715 * u * square))
            act = (0.5 * u * (1.0 + t)).astype(BF)
            slope = 0.5 * (1.0 + t) + (0.5 * 0.7978845608028654) * u * (1.0 - t * t) * (
                1.0 + 0.134145 * square
            )
            grad_up = (grad_act * slope).astype(BF)
            act_ref[here, :] = act
            gup_ref[here, :] = grad_up
            layer_ref[here, :] += dot(act, wd_all[j], 1, 0)
            grad_in_ref[here, :] += dot(grad_up, wu_all[j], 1, 1)
            return carry + jnp.sum(grad_up.astype(F32), 0, keepdims=True)

        grad_b_up = lax.fori_loop(0, count // big, feed, jnp.zeros((1, wu_all.shape[2]), F32))
        vector_held[0, pl.ds(s, 1), pack_lanes:] = grad_b_up

        def weigh(i, carry, j=s):
            here = lanes(i * 256, 256)
            wu_all[j, :, here] = dot(mid_t[...], gup_ref[:, here], 1, 0).astype(BF)
            wd_all[j, :, here] = dot(down_t[...], act_ref[:, here], 1, 0).astype(BF)
            return carry

        lax.fori_loop(0, wu_all.shape[2] // 256, weigh, 0)
        down.copy(0, s).start()
        up.copy(0, s).start()
        if j > 0:
            down.fold_one(0, shard_of(j - 1))
            up.fold_one(0, shard_of(j - 1))

    def middle_back(i, carry):
        here = rows_of(i * tile, tile, tile)
        middle = middle_ref[here, :]
        center = middle - jnp.mean(middle, -1, keepdims=True)
        scale = lax.rsqrt(jnp.mean(center * center, -1, keepdims=True) + EPSILON)
        unit = center * scale
        grad = grad_in_ref[here, :]
        grad_unit = grad * mid_gain
        grad_middle = grad_out_ref[here, :] + scale * (
            grad_unit
            - jnp.mean(grad_unit, -1, keepdims=True)
            - unit * jnp.mean(grad_unit * unit, -1, keepdims=True)
        )
        middle_ref[here, :] = grad_middle
        grad_attn = grad_middle.astype(BF)
        down_ref[here, :] = grad_attn
        sums = (
            jnp.sum(grad_attn.astype(F32), 0, keepdims=True),
            jnp.sum(grad * unit, 0, keepdims=True),
            jnp.sum(grad, 0, keepdims=True),
        )
        return tuple(x + y for x, y in zip(carry, sums))

    sums = lax.fori_loop(0, count // tile, middle_back, (zero_row,) * 3)
    for i, value in enumerate(sums + (grad_b_down,)):
        vector_held[0, ring + 2 + i : ring + 3 + i, 0:width] = value
    for i in range(ring):
        here = slice(i * out_rows, (i + 1) * out_rows)
        mid_t[here, :] = dot(wo_all[here, :], down_ref[...], 1, 1).astype(BF)
    g_ref = mid_t

    def g_copy(slot, to):
        return remote(
            g_ref.at[pl.ds(HEADS_AT[to][slot] * hd, hd)],
            g_all.at[slot, :, own],
            gsend.at[slot, to],
            grecv.at[slot, place.shift_to(to) - 1],
            (place.d, to),
        )

    for slot in range(heads_here):
        for to in range(ring):

            @pl.when(m == to)
            def _(slot=slot, to=to):
                row = HEADS_AT[to][slot] * hd
                g_all[slot, :, own] = g_ref[row : row + hd, :]

            @pl.when(m != to)
            def _(slot=slot, to=to):
                g_copy(slot, to).start()

    for j in range(ring):
        here = rows_of(shard_of(j) * out_rows, out_rows, 16)
        wo_share[shard_of(j), 0:out_rows, :] = dot(
            context_ref[here, :], down_ref[...], 1, 0
        ).astype(BF)
        out.copy(0, shard_of(j)).start()
    down.fold_one(0, shard_of(ring - 1))
    up.fold_one(0, shard_of(ring - 1))
    out.fold(0)
    for name in ("v", "qk", "lse", "exact"):
        loads[name].wait()

    def qk_row(h):
        head = place.head(h)
        return head // heads_here, lax.rem(head, heads_here) * 2 * hd

    def qk_copy(h, j):
        shard, row = qk_row(h)
        return remote(
            dqk_send.at[h, :, lanes(place.z(j) * count, count)],
            grad_ref.at[shard, rows_of(row, 2 * hd, 2 * hd)],
            qsend.at[h, j - 1],
            qrecv.at[h, j - 1],
            place.to_z(j),
        )

    v_row = 2 * hd * heads_here

    def v_copy(i, j):
        shard, row, rows, _, row_there = FRESH[i]
        return remote(
            dv_send.at[pl.ds(row_there, rows), lanes(place.z(j) * count, count)],
            grad_ref.at[shard, pl.ds(v_row + row, rows)],
            vsend.at[i, j - 1],
            vrecv.at[i, j - 1],
            place.to_z(j),
        )

    def moved_copy(i):
        to, row, rows, _, row_there = MOVED[i]
        return remote(
            dv_send.at[pl.ds(row_there, rows)],
            first_ref.at[pl.ds(row, rows)],
            fsend.at[0],
            frecv.at[0],
            (place.d, to),
        )

    def send_fresh():
        for i, (shard, row, rows, at, row_there) in enumerate(FRESH):

            @pl.when(m == at)
            def _(i=i, shard=shard, row=row, rows=rows, row_there=row_there):
                for j in range(1, ring):
                    v_copy(i, j).start()
                grad_ref[shard, v_row + row : v_row + row + rows, :] = dv_send[
                    pl.ds(row_there, rows), own
                ]

    def send_reused():
        for i, move in enumerate(MOVED):

            @pl.when(m == move[3])
            def _(i=i):
                moved_copy(i).start()

        for at, row, rows, row_there in KEPT:

            @pl.when(m == at)
            def _(row=row, rows=rows, row_there=row_there):
                first_ref[row : row + rows, :] = dv_send[row_there : row_there + rows, :]

    boundary = length_ref[0]
    block = count
    for h in range(heads_here):
        keys[...] = jnp.transpose(qk_ref[h, hd : 2 * hd, :])
        vals[...] = jnp.transpose(v_ref[hd * h : hd * h + hd, :])
        for j in range(1, ring):
            remote(
                g_ref.at[pl.ds(0, hd)],
                g_all.at[h, :, own],
                gsend.at[h, 0],
                grecv.at[h, j - 1],
                place.to_z(j),
            ).wait_recv()
        delta[...] = jnp.sum(
            g_all[h].astype(F32) * exact_ref[hd * h : hd * h + hd, :], 0, keepdims=True
        )
        for ki in range(ring):
            key_start = ki * block
            key_rows = keys[key_start : key_start + block, :]
            val_rows = vals[key_start : key_start + block, :]
            key_t = qk_ref[h, hd : 2 * hd, key_start : key_start + block]
            grad_k = None
            for qi in range(ki, ring):
                query_start = qi * block
                here = slice(query_start, query_start + block)
                q = qk_ref[h, 0:hd, here]
                g = g_all[h, :, here]
                scores = dot(key_rows, q, 1, 0) - lse_ref[h, :, here]
                if ki == qi:
                    scores = jnp.where(
                        diagonal_mask(scores, key_start, query_start), scores, NEG_LARGE
                    )
                elif key_start < half <= query_start:
                    scores = scores + other_document(boundary, key_start, query_start)
                p = jnp.exp(scores)
                grad_p = dot(val_rows, g, 1, 0)
                grad_s = (p * (grad_p - delta[:, here])).astype(BF)
                part_v = dot(g, p.astype(BF), 1, 1)
                part_k = dot(q, grad_s, 1, 1)
                if grad_k is None:
                    grad_v, grad_k = part_v, part_k
                else:
                    grad_v, grad_k = grad_v + part_v, grad_k + part_k
                part_q = dot(key_t, grad_s, 1, 0)
                if ki == 0:
                    dq[:, here] = part_q
                else:
                    dq[:, here] += part_q
            dqk_send[h, hd : 2 * hd, key_start : key_start + block] = grad_k.astype(BF)
            dv_send[hd * h : hd * h + hd, key_start : key_start + block] = grad_v.astype(BF)
        dqk_send[h, 0:hd, :] = (dq[...] * (hd**-0.5)).astype(BF)
        for j in range(1, ring):
            qk_copy(h, j).start()
        shard, row = qk_row(h)
        grad_ref[shard, rows_of(row, 2 * hd, 2 * hd), :] = dqk_send[h, :, own]
        if h == 0:
            for item in (down, up, out):
                item.fold(1)
        if h == 1:
            send_fresh()
        if h == 2:
            send_reused()
    for item in (down, up, out):
        item.fold(2)
    for h in range(heads_here):
        for j in range(1, ring):
            qk_copy(h, j).wait_recv()
            qk_copy(h, j).wait_send()
    for to in range(ring):

        @pl.when(m != to)
        def _(to=to):
            for slot in range(heads_here):
                g_copy(slot, to).wait_send()

    for i, (shard, row, rows, at, row_there) in enumerate(FRESH):

        @pl.when(m == at)
        def _(i=i):
            for j in range(1, ring):
                v_copy(i, j).wait_send()

        @pl.when(m != at)
        def _(i=i, shard=shard, row=row, rows=rows, at=at, row_there=row_there):
            shift = lax.rem(m - at + ring, ring)
            remote(
                dv_send.at[pl.ds(row_there, rows), own],
                grad_ref.at[shard, pl.ds(v_row + row, rows)],
                vsend.at[i, shift - 1],
                vrecv.at[i, shift - 1],
                place.to_z(shift),
            ).wait_recv()

    for i, move in enumerate(MOVED):

        @pl.when(m == move[3])
        def _(i=i):
            moved_copy(i).wait_send()

        @pl.when(m == move[0])
        def _(i=i):
            moved_copy(i).wait_recv()

    for name in ("normed", "wt"):
        loads[name].wait()
    ones = jnp.ones((8, count), BF)
    for j in range(ring):
        up.copy(0, j).wait_send()
        wu_all[j, 0:pack_lanes, :] = dot(grad_ref[j], normed_ref[...], 1, 0).astype(BF)
        pack.copy(0, j).start()
        sums = dot(ones, grad_ref[j], 1, 1)
        vector_held[0, j : j + 1, 0:pack_lanes] = sums[0:1]

    def input_back(i, carry):
        here = lanes(i * tile, tile)
        grad = None
        for j in range(ring):
            part = dot(grad_ref[j, :, here], wt_all[j], 0, 0)
            grad = part if grad is None else grad + part
        here = rows_of(i * tile, tile, tile)
        value = hidden_ref[here, :]
        center = value - jnp.mean(value, -1, keepdims=True)
        scale = lax.rsqrt(jnp.mean(center * center, -1, keepdims=True) + EPSILON)
        unit = center * scale
        grad_unit = grad * pre_gain_ref[...]
        grad_in_ref[here, :] = middle_ref[here, :] + scale * (
            grad_unit
            - jnp.mean(grad_unit, -1, keepdims=True)
            - unit * jnp.mean(grad_unit * unit, -1, keepdims=True)
        )
        sums = (
            jnp.sum(grad * unit, 0, keepdims=True),
            jnp.sum(grad, 0, keepdims=True),
        )
        return tuple(x + y for x, y in zip(carry, sums))

    sums = lax.fori_loop(0, count // tile, input_back, (zero_row,) * 2)
    for i, value in enumerate(sums):
        vector_held[0, ring + i : ring + 1 + i, 0:width] = value

    routes = [place.to_core, place.to_x, place.to_y]
    routes += [place.to_plane(step) for step in place.steps()]
    bit = 1
    while bit < ring:
        routes.append((place.d, m + bit - 2 * bit * lax.rem(m // bit, 2)))
        bit *= 2

    def vector_copy(k):
        return remote(
            vector_held.at[k], vector_came.at[k], wsend.at[k], wrecv.at[k], routes[k]
        )

    def vector_fold(k):
        vector_copy(k).wait_recv()
        value = vector_held[k] + vector_came[k]
        if k + 1 < len(routes):
            vector_held[k + 1] = value
            vector_copy(k + 1).start()
        else:
            vector_sum[...] = value

    vector_copy(0).start()
    ffn = (down, up, out)
    pack.fold(0)
    for item in ffn:
        item.fold_pair()
    vector_fold(0)
    pack.fold(1)
    for item in ffn:
        item.finish_sum()
    vector_fold(1)
    pack.fold(2)
    vector_fold(2)
    for item in ffn:
        item.spread(6)
    pack.fold_pair()
    for k in range(3, len(routes) - 1):
        vector_fold(k)
    for item in ffn:
        item.spread(7)
    pack.finish_sum()
    vector_fold(len(routes) - 1)
    pack.spread(6)
    pack.spread(7)
    everything = (down, up, out, pack)
    for item in everything:
        item.wait(7)
        item.drain(1 if item is up else 0)
    for k in range(len(routes)):
        vector_copy(k).wait_send()


def backward_call(
    ring, heads_here, planes, length, context, hidden, grad_out, pre_gain, rows, bias,
    qk, v, lse, exact, normed, wt, wo, wo_far, wu, wu_far, wd, wd_far, piece,
):
    count, width = hidden.shape
    total = ring * count
    hd = HEAD_DIM
    others = ring - 1
    sds = jax.ShapeDtypeStruct
    dma = pltpu.SemaphoreType.DMA
    hops = 3 + (planes.bit_length() - 1) + (ring.bit_length() - 1)
    stages = 8 + planes.bit_length() - 1
    pack_rows = wt.shape[1]
    out_pad = wo.shape[0] + -wo.shape[0] % (16 * PLANE)
    sizes = [wd.shape[0], wu.shape[0], out_pad, pack_rows]
    bufs = [buf for rows_ in sizes for buf in Reduce.buffers(rows_, width, planes)]
    vector = (ring + 6 + -(ring + 6) % 8, bias.shape[2])
    vm = pltpu.VMEM
    return pl.pallas_call(
        functools.partial(backward_kernel, ring, heads_here, planes),
        out_shape=(
            sds(hidden.shape, F32),
            sds(hidden.shape, F32),
            sds((piece, total), BF),
            sds(wt.shape[1:], BF),
            sds((out_pad, width), BF),
            sds(wu.shape, BF),
            sds(wd.shape, BF),
            sds(vector, F32),
        ),
        in_specs=[SM] + [VM] * 6 + [ANY] * 12,
        out_specs=[VM] * 8,
        scratch_shapes=[
            vm(qk.shape, BF),
            vm(v.shape, BF),
            vm(lse.shape, F32),
            vm(exact.shape, F32),
            vm(normed.shape, BF),
            vm(wt.shape, BF),
            vm((ring * wo.shape[0], width), BF),
            vm((ring,) + wu.shape, BF),
            vm((ring,) + wd.shape, BF),
            vm((count, width), F32),
            vm((count, width), BF),
            vm((width, count), BF),
            vm((count, width), BF),
            vm((width, count), BF),
            vm((count, width), BF),
            vm((count, width), BF),
            vm((ring, out_pad, width), BF),
            vm((heads_here, hd, total), BF),
            vm((total, hd), BF),
            vm((total, hd), BF),
            vm((1, total), F32),
            vm((hd, total), F32),
            vm((heads_here, 2 * hd, total), BF),
            vm((heads_here * hd, total), BF),
            vm((ring, pack_rows, count), BF),
            vm((hops,) + vector, F32),
            vm((hops,) + vector, F32),
            dma((3 * ring + 6,)),
            dma((heads_here, ring)),
            dma((heads_here, others)),
            dma((heads_here, others)),
            dma((heads_here, others)),
            dma((len(FRESH), others)),
            dma((len(FRESH), others)),
            dma((1,)),
            dma((1,)),
            dma((4, stages, ring)),
            dma((4, stages, ring)),
            dma((hops,)),
            dma((hops,)),
        ]
        + bufs,
        compiler_params=pltpu.CompilerParams(
            collective_id=1, has_side_effects=True, vmem_limit_bytes=67043328
        ),
        name="backward",
    )(
        length, context, hidden, grad_out, pre_gain, rows, bias, qk, v, lse, exact,
        normed, wt, wo, wo_far, wu, wu_far, wd, wd_far,
    )


def shards(
    hidden_in,
    first_values,
    first_length,
    pre_gain,
    pre_shift,
    w_query,
    b_query,
    w_key,
    w_value,
    b_value,
    w_out,
    b_out,
    mid_gain,
    mid_shift,
    w_up,
    b_up,
    w_down,
    b_down,
    grad_out,
):
    ring = lax.axis_size("mp")
    m = lax.axis_index("mp")
    hd = HEAD_DIM
    count, width = hidden_in.shape
    head_width = w_query.shape[1]
    heads_here = head_width // hd
    piece = w_value.shape[1]
    pack_rows = 2 * hd * (heads_here + 1)
    wq = w_query.T.reshape(heads_here, 1, hd, width)
    wk = w_key.T.reshape(heads_here, 1, hd, width)
    spare = pack_rows - 2 * head_width - piece
    wt = jnp.concatenate(
        [
            jnp.concatenate([wq, wk], 1).reshape(2 * head_width, width),
            w_value.T,
            jnp.zeros((spare, width), BF),
        ],
        0,
    )
    bq = b_query.reshape(heads_here, 1, hd)
    bias = jnp.concatenate(
        [
            jnp.concatenate([bq, jnp.zeros_like(bq)], 1).reshape(-1),
            b_value,
            jnp.zeros((spare,), F32),
            b_up,
        ]
    )
    bias = jnp.broadcast_to(bias[None], (8, bias.shape[0]))
    context_t, normed, qk, v, lse, exact, wt_all, bias_all, wo_far, wu_far, wd_far = forward_call(
        ring,
        heads_here,
        first_length,
        hidden_in,
        pre_gain[None],
        pre_shift[None],
        wt,
        bias,
        first_values.T,
        w_out,
        w_up,
        w_down,
    )
    rows = jnp.stack([b_out, mid_gain, mid_shift, b_down] * 2)
    layer_out, grad_input, grad_first, pack_sum, wo_sum, wu_sum, wd_sum, vector = backward_call(
        ring,
        heads_here,
        lax.axis_size("dp") // PLANE,
        first_length,
        context_t,
        hidden_in,
        grad_out,
        pre_gain[None],
        rows,
        bias_all,
        qk,
        v,
        lse,
        exact,
        normed,
        wt_all,
        w_out,
        wo_far,
        w_up,
        wu_far,
        w_down,
        wd_far,
        piece,
    )
    own_vector = lax.dynamic_index_in_dim(vector, m, 0, False)
    qk_grad = pack_sum[: 2 * head_width].astype(F32).reshape(heads_here, 2, hd, width)
    v_grad = pack_sum[2 * head_width : 2 * head_width + piece].astype(F32)
    rows = [vector[ring + i, :width] for i in range(6)]
    return (
        layer_out,
        grad_input,
        grad_first.astype(F32).T,
        rows[0],
        rows[1],
        qk_grad[:, 0].reshape(head_width, width).T,
        own_vector[: 2 * head_width].reshape(heads_here, 2, hd)[:, 0].reshape(-1),
        qk_grad[:, 1].reshape(head_width, width).T,
        v_grad.T,
        own_vector[2 * head_width : 2 * head_width + piece],
        wo_sum[:head_width].astype(F32),
        rows[2],
        rows[3],
        rows[4],
        wu_sum.astype(F32),
        own_vector[pack_rows:],
        wd_sum.astype(F32).T,
        rows[5],
    )


def solution(mesh):
    rows, cols = P(("dp", "mp"), None), P(None, "mp")
    return jax.shard_map(
        shards,
        mesh=mesh,
        in_specs=(
            rows,
            P("dp", "mp"),
            P("dp"),
            P(),
            P(),
            cols,
            P("mp"),
            cols,
            cols,
            P("mp"),
            P("mp", None),
            P(),
            P(),
            P(),
            cols,
            P("mp"),
            P("mp", None),
            P(),
            rows,
        ),
        out_specs=(
            rows,
            rows,
            P("dp", "mp"),
            P(),
            P(),
            cols,
            P("mp"),
            cols,
            cols,
            P("mp"),
            P("mp", None),
            P(),
            P(),
            P(),
            cols,
            P("mp"),
            P("mp", None),
            P(),
        ),
        check_vma=False,
    )
```

```python
import functools

import jax
import jax.numpy as jnp
from jax import lax
from jax.experimental import pallas as pl
from jax.experimental.pallas import tpu as pltpu
from jax.sharding import PartitionSpec as P

HEAD_DIM = 64
EPSILON = 1e-05
NEG_LARGE = -1e30
MESH = pl.DeviceIdType.MESH
BF = jnp.bfloat16
F32 = jnp.float32
ANY = pl.BlockSpec(memory_space=pl.ANY)
VM = pl.BlockSpec(memory_space=pltpu.VMEM)
SM = pl.BlockSpec(memory_space=pltpu.SMEM)
VMEM_LIMIT = 60 << 20
LANE = 128
PLANE = 8
RING = 4
HEADS_AT = ((0, 1, 6), (7, 8, 2), (9, 10, 3), (4, 5, 11))
FRESH = (
    (0, 0, 96, 0, 0),
    (1, 0, 32, 0, 96),
    (1, 32, 64, 1, 128),
    (2, 0, 64, 2, 128),
    (2, 64, 32, 3, 0),
    (3, 0, 96, 3, 32),
)
KEPT = ((0, 0, 64, 128), (1, 0, 96, 32), (2, 0, 96, 0), (3, 32, 64, 128))
MOVED = ((0, 64, 32, 1, 0), (3, 0, 32, 2, 96))


def dot(left, right, left_dim, right_dim):
    return lax.dot_general(
        left, right, (((left_dim,), (right_dim,)), ((), ())), preferred_element_type=F32
    )


def layer_norm(values, gain, shift):
    center = values - jnp.mean(values, -1, keepdims=True)
    spread = jnp.mean(center * center, -1, keepdims=True)
    return center * lax.rsqrt(spread + EPSILON) * gain + shift


def gelu_tanh(values):
    return (
        0.5
        * values
        * (1.0 + jnp.tanh(0.7978845608028654 * (values + 0.044715 * values * values * values)))
    )


def lanes(start, size):
    return pl.ds(pl.multiple_of(start, LANE), size)


def rows_of(start, size, unit):
    return pl.ds(pl.multiple_of(start, unit), size)


class Place:
    def __init__(self, ring, planes=1):
        self.ring = ring
        self.planes = planes
        self.d = lax.axis_index("dp")
        self.m = lax.axis_index("mp")
        d = self.d
        self.core = lax.rem(d, 2)
        self.x = lax.rem(d // 2, 2)
        self.y = lax.rem(d // 4, 2)
        self.to_core = (d + 1 - 2 * self.core, self.m)
        self.to_x = (d + 2 - 4 * self.x, self.m)
        self.to_y = (d + 4 - 8 * self.y, self.m)
        self.pair = self.m + 1 - 2 * lax.rem(self.m, 2)
        self.across = lax.rem(self.m + 2, RING)
        self.corner = RING - 1 - self.m

    def z(self, shift):
        return lax.rem(self.m + shift, self.ring)

    def to_z(self, shift):
        return (self.d, self.z(shift))

    def shift_to(self, position):
        return lax.rem(position - self.m + self.ring, self.ring)

    def head(self, slot):
        value = 0
        for k, heads in enumerate(HEADS_AT):
            for at, head in enumerate(heads):
                value = jnp.where(jnp.logical_and(self.m == k, slot == at), head, value)
        return value

    def shard(self, slot):
        return self.head(slot) // len(HEADS_AT[0])

    def steps(self):
        return [PLANE << b for b in range(self.planes.bit_length() - 1)]

    def to_plane(self, step):
        return (self.d + step - 2 * step * lax.rem(self.d // step, 2), self.m)

    def barrier(self):
        sem = pltpu.get_barrier_semaphore()
        peers = [self.to_z(j) for j in range(1, self.ring)]
        peers += [self.to_core, self.to_x, self.to_y]
        peers += [self.to_plane(step) for step in self.steps()]
        for peer in peers:
            pl.semaphore_signal(sem, inc=1, device_id=peer, device_id_type=MESH)
        pl.semaphore_wait(sem, len(peers))

    def slot(self, x_first):
        if x_first:
            return self.core * 4 + self.y * 2 + self.x
        return self.core * 4 + self.x * 2 + self.y


def remote(src, dst, send, recv, device):
    return pltpu.make_async_remote_copy(
        src_ref=src,
        dst_ref=dst,
        send_sem=send,
        recv_sem=recv,
        device_id=device,
        device_id_type=MESH,
    )


class Gather:
    def __init__(self, place, src, dst, send, recv, item, first_row, rows, x_first):
        self.place, self.src, self.dst = place, src, dst
        self.send, self.recv, self.item = send, recv, item
        self.first_row, self.part, self.x_first = first_row, rows // PLANE, x_first

    def window(self, start, size):
        part = self.part
        return rows_of(self.first_row + start * part, size * part, part & -part)

    def copy(self, stage, k):
        place = self.place
        slot = place.slot(self.x_first)
        near, far = (place.to_x, place.to_y) if self.x_first else (place.to_y, place.to_x)
        shard = (place.across, place.pair, place.corner)[k]
        window = self.window(slot, 1)
        if stage == 0:
            shard, target = place.m, (place.d, place.across)
        elif stage == 1:
            shard, target = (place.m, place.across)[k], (place.d, place.pair)
        elif stage == 2:
            target = near
        elif stage == 3:
            window, target = self.window((slot // 2) * 2, 2), far
        else:
            window, target = self.window(place.core * 4, 4), place.to_core
        own = stage == 0 or (stage == 1 and k == 0)
        source = self.src.at[window] if own else self.dst.at[shard, window]
        return remote(
            source,
            self.dst.at[shard, window],
            self.send.at[self.item, stage, k],
            self.recv.at[self.item, stage, k],
            target,
        )

    def start(self, stage):
        if stage == 0:
            self.copy(0, 0).start()
            self.copy(1, 0).start()
        elif stage == 1:
            self.copy(0, 0).wait_recv()
            self.copy(1, 1).start()
        else:
            for k in range(2 if stage == 2 else 3):
                self.copy(stage - 1, k).wait_recv()
            for k in range(3):
                self.copy(stage, k).start()

    def arrive(self):
        for k in range(3):
            self.copy(4, k).wait_recv()

    def drain(self):
        for stage, copies in enumerate((1, 2, 3, 3, 3)):
            for k in range(copies):
                self.copy(stage, k).wait_send()


class Reduce:
    def __init__(self, place, src, bufs, out, send, recv, item, x_first, first_row=0):
        self.place, self.src, self.out = place, src, out
        self.first_row = first_row
        self.r_core, self.r_far, self.r_near, self.r_z, self.r_plane = bufs
        self.send, self.recv, self.item, self.x_first = send, recv, item, x_first
        self.part = out.shape[0] // PLANE
        if x_first:
            self.near, self.far = place.to_x, place.to_y
            self.near_bit, self.far_bit = place.x, place.y
        else:
            self.near, self.far = place.to_y, place.to_x
            self.near_bit, self.far_bit = place.y, place.x

    def rows(self, start, size):
        return rows_of(start * self.part, size * self.part, self.part & -self.part)

    def copy(self, stage, k):
        place = self.place
        if stage == 0:
            begin = self.first_row + (1 - place.core) * 4 * self.part
            src = self.src.at[k, rows_of(begin, 4 * self.part, self.part & -self.part)]
            dst, target = self.r_core.at[k], place.to_core
        elif stage == 1:
            src = self.r_core.at[k, self.rows((1 - self.far_bit) * 2, 2)]
            dst, target = self.r_far.at[k], self.far
        elif stage == 2:
            src = self.r_far.at[k, self.rows(1 - self.near_bit, 1)]
            dst, target = self.r_near.at[k], self.near
        elif stage == 3:
            src = self.r_near.at[(place.pair, place.corner)[k]]
            dst, target = self.r_z.at[k], (place.d, place.pair)
        elif stage == 4:
            src = self.r_near.at[place.across]
            dst, target = self.r_z.at[2], (place.d, place.across)
        else:
            slot = place.slot(self.x_first)
            if stage == 5:
                window, target = self.rows(slot, 1), self.near
            elif stage == 6:
                window, target = self.rows((slot // 2) * 2, 2), self.far
            else:
                window, target = self.rows(place.core * 4, 4), place.to_core
            src = dst = self.out.at[window]
        return remote(
            src, dst, self.send.at[self.item, stage, k], self.recv.at[self.item, stage, k], target
        )

    def members(self, stage):
        return range((RING, RING, RING, 2, 1, 1, 1, 1)[stage])

    def start(self, stage):
        for k in self.members(stage):
            self.copy(stage, k).start()

    def wait(self, stage):
        for k in self.members(stage):
            self.copy(stage, k).wait_recv()

    def fold_one(self, stage, k):
        place, part = self.place, self.part
        if stage == 0:
            base = self.first_row + place.core * 4 * part
            kept, into, size = self.src, self.r_core, 4 * part
        elif stage == 1:
            kept, base, into, size = self.r_core, self.far_bit * 2 * part, self.r_far, 2 * part
        else:
            kept, base, into, size = self.r_far, self.near_bit * part, self.r_near, part
        unit = part & -part
        step = min(part, 32)
        self.copy(stage, k).wait_recv()

        def add(i, carry):
            mine = kept[k, rows_of(base + i * step, step, min(unit, step)), :].astype(F32)
            here = rows_of(i * step, step, step)
            into[k, here, :] = (into[k, here, :].astype(F32) + mine).astype(BF)
            return carry

        lax.fori_loop(0, size // step, add, 0)
        if stage < 2:
            self.copy(stage + 1, k).start()

    def fold(self, stage):
        for k in self.members(stage):
            self.fold_one(stage, k)
        if stage == 2:
            self.start(3)

    def fold_pair(self):
        place = self.place
        self.wait(3)
        other = self.r_near[place.across].astype(F32) + self.r_z[1].astype(F32)
        self.r_near[place.across] = other.astype(BF)
        self.start(4)
        mine = self.r_near[place.m].astype(F32) + self.r_z[0].astype(F32)
        self.r_near[place.m] = mine.astype(BF)

    def finish_sum(self):
        place = self.place
        self.wait(4)
        here = self.rows(place.slot(self.x_first), 1)
        value = self.r_near[place.m].astype(F32) + self.r_z[2].astype(F32)
        self.out[here, :] = value.astype(BF)
        for b, step in enumerate(place.steps()):
            copy = remote(
                self.out.at[here],
                self.r_plane.at[b],
                self.send.at[self.item, 8 + b, 0],
                self.recv.at[self.item, 8 + b, 0],
                place.to_plane(step),
            )
            copy.start()
            copy.wait()
            mine = self.out[here, :].astype(F32)
            self.out[here, :] = (mine + self.r_plane[b].astype(F32)).astype(BF)
        self.start(5)

    def spread(self, stage):
        self.wait(stage - 1)
        self.start(stage)

    def drain(self, first):
        for stage in range(first, 8):
            for k in self.members(stage):
                self.copy(stage, k).wait_send()

    @staticmethod
    def buffers(rows, width, planes):
        part = rows // PLANE
        extra = max(planes.bit_length() - 1, 1)
        return [
            pltpu.VMEM((RING, 4 * part, width), BF),
            pltpu.VMEM((RING, 2 * part, width), BF),
            pltpu.VMEM((RING, part, width), BF),
            pltpu.VMEM((3, part, width), BF),
            pltpu.VMEM((extra, part, width), BF),
        ]


def diagonal_mask(scores, key_start, query_start):
    keys = lax.broadcasted_iota(jnp.int32, scores.shape, 0) + key_start
    queries = lax.broadcasted_iota(jnp.int32, scores.shape, 1) + query_start
    return keys <= queries


def other_document(boundary, key_start, query_start):
    crossing = jnp.logical_and(boundary > key_start, boundary <= query_start)
    return jnp.where(crossing, NEG_LARGE, 0.0)


def forward_kernel(
    ring,
    heads_here,
    length_ref,
    hidden_ref,
    gain_ref,
    shift_ref,
    wt_ref,
    bias_ref,
    first_ref,
    wo_ref,
    wu_ref,
    wd_ref,
    context_ref,
    normed_ref,
    qk_ref,
    v_ref,
    lse_ref,
    exact_ref,
    wt_all,
    bias_all,
    wo_far,
    wu_far,
    wd_far,
    y_send,
    vy_send,
    c_send,
    keys,
    gsend,
    grecv,
    bsend,
    brecv,
    qsend,
    qrecv,
    vsend,
    vrecv,
    fsend,
    frecv,
    csend,
    crecv,
):
    place = Place(ring)
    m = place.m
    count = hidden_ref.shape[0]
    total = ring * count
    piece = first_ref.shape[0]
    half = total // 2
    hd = HEAD_DIM
    pack_rows = wt_ref.shape[0]
    place.barrier()
    half_pack = pack_rows // 2
    small = [
        Gather(place, wt_ref, wt_all, gsend, grecv, i, i * half_pack, half_pack, i == 0)
        for i in range(2)
    ]
    big = [
        Gather(place, wo_ref, wo_far, gsend, grecv, 2, 0, wo_ref.shape[0], True),
        Gather(place, wu_ref, wu_far, gsend, grecv, 3, 0, wu_ref.shape[0], True),
        Gather(place, wd_ref, wd_far, gsend, grecv, 4, 0, wd_ref.shape[0], False),
    ]
    for item in small:
        item.start(0)

    def bias_copy(j):
        return remote(
            bias_ref, bias_all.at[m], bsend.at[j - 1], brecv.at[j - 1], place.to_z(j)
        )

    for j in range(1, ring):
        bias_copy(j).start()

    def moved_copy(i):
        _, row, rows, to, row_there = MOVED[i]
        return remote(
            first_ref.at[pl.ds(row, rows)],
            v_ref.at[pl.ds(row_there, rows)],
            fsend.at[0],
            frecv.at[0],
            (place.d, to),
        )

    for i, move in enumerate(MOVED):

        @pl.when(m == move[0])
        def _(i=i):
            moved_copy(i).start()

    for at, row, rows, row_there in KEPT:

        @pl.when(m == at)
        def _(row=row, rows=rows, row_there=row_there):
            v_ref[row_there : row_there + rows, :] = first_ref[row : row + rows, :]

    normed_ref[...] = layer_norm(hidden_ref[...], gain_ref[...], shift_ref[...]).astype(BF)
    wt_all[m] = wt_ref[...]
    bias_all[m] = bias_ref[...]

    for item in small:
        item.start(1)
    for item in big:
        item.start(0)
    for item in small:
        item.start(2)
    for item in big:
        item.start(1)
    for stage in (3, 4):
        for item in small:
            item.start(stage)
    for j in range(1, ring):
        bias_copy(j).wait_recv()
    for item in small:
        item.arrive()

    own = lanes(m * count, count)

    def qk_copy(slot, to):
        return remote(
            y_send.at[to, slot],
            qk_ref.at[slot, :, own],
            qsend.at[to, slot],
            qrecv.at[slot, place.shift_to(to) - 1],
            (place.d, to),
        )

    def v_copy(i):
        shard, row, rows, to, row_there = FRESH[i]
        return remote(
            vy_send.at[shard, pl.ds(row, rows)],
            v_ref.at[pl.ds(row_there, rows), own],
            vsend.at[i],
            vrecv.at[i, place.shift_to(to) - 1],
            (place.d, to),
        )

    where_is = {
        (head // heads_here, slot): to
        for to, heads in enumerate(HEADS_AT)
        for slot, head in enumerate(heads)
    }
    v_row = 2 * hd * heads_here

    for shard in range(ring):
        out = dot(wt_all[shard], normed_ref[...], 1, 1)
        out = out + jnp.transpose(bias_all[shard, :, 0:pack_rows])[:, 0:1]
        for slot in range(heads_here):
            to = where_is[shard, slot]
            row = 2 * hd * slot
            y_send[to, slot, 0:hd, :] = (out[row : row + hd] * (hd**-0.5)).astype(BF)
            y_send[to, slot, hd : 2 * hd, :] = out[row + hd : row + 2 * hd].astype(BF)
        vy_send[shard] = out[v_row : v_row + piece].astype(BF)

    def share(slot):
        for to in range(ring):

            @pl.when(m == to)
            def _(to=to):
                qk_ref[slot, :, own] = y_send[to, slot]

            @pl.when(m != to)
            def _(to=to):
                qk_copy(slot, to).start()

    share(0)
    for i, (shard, row, rows, to, row_there) in enumerate(FRESH):

        @pl.when(m == to)
        def _(shard=shard, row=row, rows=rows, row_there=row_there):
            v_ref[row_there : row_there + rows, own] = vy_send[shard, row : row + rows, :]

        @pl.when(m != to)
        def _(i=i):
            v_copy(i).start()

    for slot in range(1, heads_here):
        share(slot)
    for stage in (2, 3):
        for item in big:
            item.start(stage)

    def qk_arrive(slot):
        for shift in range(1, ring):
            remote(
                y_send.at[0, slot],
                qk_ref.at[slot, :, own],
                qsend.at[0, slot],
                qrecv.at[slot, shift - 1],
                place.to_z(shift),
            ).wait_recv()

    for i, (shard, row, rows, to, row_there) in enumerate(FRESH):

        @pl.when(m == to)
        def _(i=i, shard=shard, row=row, rows=rows, row_there=row_there):
            for shift in range(1, ring):
                remote(
                    vy_send.at[shard, pl.ds(row, rows)],
                    v_ref.at[pl.ds(row_there, rows), own],
                    vsend.at[i],
                    vrecv.at[i, shift - 1],
                    place.to_z(shift),
                ).wait_recv()

    for i, move in enumerate(MOVED):

        @pl.when(m == move[3])
        def _(i=i):
            moved_copy(i).wait_recv()

    boundary = length_ref[0]
    block = count

    def context_copy(h, j):
        return remote(
            c_send.at[rows_of(hd * h, hd, hd), lanes(place.z(j) * count, count)],
            context_ref.at[rows_of(place.head(h) * hd, hd, hd)],
            csend.at[h, j - 1],
            crecv.at[h, j - 1],
            place.to_z(j),
        )

    def attend(h, carry):
        qk_arrive(h)
        here_h = rows_of(hd * h, hd, hd)
        keys[...] = jnp.transpose(qk_ref[h, hd : 2 * hd, :])
        for qi in range(ring):
            query_start = qi * block
            queries = slice(query_start, query_start + block)
            q = qk_ref[h, 0:hd, queries]
            top = None
            for ki in range(qi + 1):
                key_start = ki * block
                v = v_ref[here_h, key_start : key_start + block]
                scores = dot(keys[key_start : key_start + block, :], q, 1, 0)
                if ki == qi:
                    scores = jnp.where(
                        diagonal_mask(scores, key_start, query_start), scores, NEG_LARGE
                    )
                elif key_start < half <= query_start:
                    scores = scores + other_document(boundary, key_start, query_start)
                block_top = jnp.max(scores, 0, keepdims=True)
                new_top = block_top if top is None else jnp.maximum(top, block_top)
                p = jnp.exp(scores - new_top)
                p_sum = jnp.sum(p, 0, keepdims=True)
                part = dot(v, p.astype(BF), 1, 0)
                if top is None:
                    run_sum, running = p_sum, part
                else:
                    factor = jnp.exp(top - new_top)
                    run_sum = run_sum * factor + p_sum
                    running = running * factor + part
                top = new_top
            result = running / run_sum
            exact_ref[here_h, queries] = result
            c_send[here_h, queries] = result.astype(BF)
            lse_ref[h, :, queries] = top + jnp.log(run_sum)
        for j in range(1, ring):
            context_copy(h, j).start()
        context_ref[rows_of(place.head(h) * hd, hd, hd), :] = c_send[here_h, own]

        @pl.when(h == 1)
        def _():
            for item in big:
                item.start(4)

        return carry

    lax.fori_loop(0, heads_here, attend, 0)
    for item in big:
        item.arrive()
    for h in range(heads_here):
        for j in range(1, ring):
            context_copy(h, j).wait_recv()
    for item in small + big:
        item.drain()
    for j in range(1, ring):
        bias_copy(j).wait_send()
        for h in range(heads_here):
            context_copy(h, j).wait_send()
    for to in range(ring):

        @pl.when(m != to)
        def _(to=to):
            for slot in range(heads_here):
                qk_copy(slot, to).wait_send()

    for i, (shard, row, rows, to, row_there) in enumerate(FRESH):

        @pl.when(m != to)
        def _(i=i):
            v_copy(i).wait_send()

    for i, move in enumerate(MOVED):

        @pl.when(m == move[0])
        def _(i=i):
            moved_copy(i).wait_send()


def forward_call(ring, heads_here, length, hidden, gain, shift, wt, bias, first_t, wo, wu, wd):
    count, width = hidden.shape
    total = ring * count
    hd = HEAD_DIM
    piece = first_t.shape[0]
    others = ring - 1
    sds = jax.ShapeDtypeStruct
    dma = pltpu.SemaphoreType.DMA
    return pl.pallas_call(
        functools.partial(forward_kernel, ring, heads_here),
        out_shape=(
            sds((ring * heads_here * hd, count), BF),
            sds((count, width), BF),
            sds((heads_here, 2 * hd, total), BF),
            sds((heads_here * hd, total), BF),
            sds((heads_here, 1, total), F32),
            sds((heads_here * hd, total), F32),
            sds((ring,) + wt.shape, BF),
            sds((ring,) + bias.shape, F32),
            sds((ring,) + wo.shape, BF),
            sds((ring,) + wu.shape, BF),
            sds((ring,) + wd.shape, BF),
        ),
        in_specs=[SM] + [VM] * 6 + [ANY] * 3,
        out_specs=[VM] * 8 + [ANY] * 3,
        scratch_shapes=[
            pltpu.VMEM((ring, heads_here, 2 * hd, count), BF),
            pltpu.VMEM((ring, piece, count), BF),
            pltpu.VMEM((heads_here * hd, total), BF),
            pltpu.VMEM((total, hd), BF),
            dma((5, 5, 3)),
            dma((5, 5, 3)),
            dma((others,)),
            dma((others,)),
            dma((ring, heads_here)),
            dma((heads_here, others)),
            dma((len(FRESH),)),
            dma((len(FRESH), others)),
            dma((1,)),
            dma((1,)),
            dma((heads_here, others)),
            dma((heads_here, others)),
        ],
        compiler_params=pltpu.CompilerParams(
            collective_id=0, has_side_effects=True, vmem_limit_bytes=VMEM_LIMIT
        ),
        name="forward",
    )(length, hidden, gain, shift, wt, bias, first_t, wo, wu, wd)


def backward_kernel(
    ring,
    heads_here,
    planes,
    length_ref,
    context_ref,
    hidden_ref,
    grad_out_ref,
    pre_gain_ref,
    rows_ref,
    bias_ref,
    qk_hbm,
    v_hbm,
    lse_hbm,
    exact_hbm,
    normed_hbm,
    wt_hbm,
    wo_hbm,
    wo_far_hbm,
    wu_hbm,
    wu_far_hbm,
    wd_hbm,
    wd_far_hbm,
    layer_ref,
    grad_in_ref,
    first_ref,
    pack_sum,
    wo_sum,
    wu_sum,
    wd_sum,
    vector_sum,
    qk_ref,
    v_ref,
    lse_ref,
    exact_ref,
    wt_all,
    wo_all,
    wu_all,
    wd_all,
    middle_ref,
    mid_ref,
    mid_t,
    down_ref,
    down_t,
    act_ref,
    gup_ref,
    g_ref,
    wo_share,
    g_all,
    keys,
    vals,
    delta,
    dq,
    grad_ref,
    vector_held,
    vector_came,
    lsem,
    gsend,
    grecv,
    qsend,
    qrecv,
    vsend,
    vrecv,
    fsend,
    frecv,
    rsend,
    rrecv,
    wsend,
    wrecv,
    *bufs,
):
    place = Place(ring, planes)
    m = place.m
    count, width = hidden_ref.shape
    total = ring * count
    half = total // 2
    hd = HEAD_DIM
    piece = first_ref.shape[0]
    out_rows = wo_hbm.shape[0]
    pack_lanes = grad_ref.shape[1]
    tile = count // 4
    own = lanes(m * count, count)

    def shard_of(j):
        return lax.rem(m - j + ring, ring)

    loads = {}

    def load(name, src, dst):
        loads[name] = pltpu.make_async_copy(src, dst, lsem.at[len(loads)])
        loads[name].start()

    for j in range(ring):
        into = wo_all.at[rows_of(shard_of(j) * out_rows, out_rows, 16)]
        load(("wo", j), wo_hbm if j == 0 else wo_far_hbm.at[shard_of(j)], into)
    for j in range(ring):
        s = shard_of(j)
        load(("wu", j), wu_hbm if j == 0 else wu_far_hbm.at[s], wu_all.at[s])
        load(("wd", j), wd_hbm if j == 0 else wd_far_hbm.at[s], wd_all.at[s])
    load("v", v_hbm, v_ref)
    load("qk", qk_hbm, qk_ref)
    load("lse", lse_hbm, lse_ref)
    load("exact", exact_hbm, exact_ref)
    load("wt", wt_hbm, wt_all)
    place.barrier()

    def row(i):
        return rows_ref[i : i + 1, :]

    b_out, mid_gain, mid_shift, b_down = row(0), row(1), row(2), row(3)
    act_ref[0] = jnp.transpose(context_ref[...])
    vector_held[0] = jnp.zeros_like(vector_held[0])
    wo_share[:, out_rows:, :] = jnp.zeros_like(wo_share[:, out_rows:, :])
    grad_ref[:, 2 * hd * heads_here + piece :, :] = jnp.zeros_like(
        grad_ref[:, 2 * hd * heads_here + piece :, :]
    )
    for j in range(ring):
        loads[("wo", j)].wait()

    def project(i, carry):
        here = rows_of(i * tile, tile, tile)
        attended = dot(act_ref[0, here, :], wo_all[...], 1, 0) + b_out
        middle = hidden_ref[here, :] + attended
        middle_ref[here, :] = middle
        layer_ref[here, :] = middle + b_down
        mid_ref[here, :] = layer_norm(middle, mid_gain, mid_shift).astype(BF)
        grad_down = grad_out_ref[here, :].astype(BF)
        down_ref[here, :] = grad_down
        grad_in_ref[here, :] = jnp.zeros((tile, width), F32)
        return carry + jnp.sum(grad_down.astype(F32), 0, keepdims=True)

    zero_row = jnp.zeros((1, width), F32)
    grad_b_down = lax.fori_loop(0, count // tile, project, zero_row)
    mid_t[...] = jnp.transpose(mid_ref[...])
    down_t[...] = jnp.transpose(down_ref[...])

    down = Reduce(place, wd_all, bufs[0:5], wd_sum, rsend, rrecv, 0, False)
    up = Reduce(place, wu_all, bufs[5:10], wu_sum, rsend, rrecv, 1, True)
    out = Reduce(place, wo_share, bufs[10:15], wo_sum, rsend, rrecv, 2, True)
    group = 2 * hd
    packs = [
        Reduce(
            place,
            wu_all,
            bufs[15 + 5 * i : 20 + 5 * i],
            pack_sum.at[pl.ds(group * i, group)],
            rsend,
            rrecv,
            3 + i,
            i % 2 == 0,
            group * i,
        )
        for i in range(heads_here + 1)
    ]

    big = count // 2

    def feed_shard(j, carry):
        s = shard_of(j)
        for i, hbm, ref in ((0, wu_hbm, wu_all), (1, wd_hbm, wd_all)):
            pltpu.make_async_copy(hbm, ref.at[s], lsem.at[ring + 2 * j + i]).wait()
        b_up = bias_ref[s, 0:1, pack_lanes:]

        def feed(i, carry):
            here = rows_of(i * big, big, big)
            u = dot(mid_ref[here, :], wu_all[s], 1, 0) + b_up
            grad_act = dot(down_ref[here, :], wd_all[s], 1, 1)
            square = u * u
            t = jnp.tanh(0.7978845608028654 * (u + 0.044715 * u * square))
            act = (0.5 * u * (1.0 + t)).astype(BF)
            slope = 0.5 * (1.0 + t) + (0.5 * 0.7978845608028654) * u * (1.0 - t * t) * (
                1.0 + 0.134145 * square
            )
            grad_up = (grad_act * slope).astype(BF)
            act_ref[s, here, :] = act
            gup_ref[s, here, :] = grad_up
            layer_ref[here, :] += dot(act, wd_all[s], 1, 0)
            grad_in_ref[here, :] += dot(grad_up, wu_all[s], 1, 1)
            return carry + jnp.sum(grad_up.astype(F32), 0, keepdims=True)

        grad_b_up = lax.fori_loop(0, count // big, feed, jnp.zeros((1, wu_all.shape[2]), F32))
        vector_held[0, pl.ds(s, 1), pack_lanes:] = grad_b_up
        return carry

    lax.fori_loop(0, ring, feed_shard, 0)
    load("normed", normed_hbm, mid_ref)

    def middle_back(i, carry):
        here = rows_of(i * tile, tile, tile)
        middle = middle_ref[here, :]
        center = middle - jnp.mean(middle, -1, keepdims=True)
        scale = lax.rsqrt(jnp.mean(center * center, -1, keepdims=True) + EPSILON)
        unit = center * scale
        grad = grad_in_ref[here, :]
        grad_unit = grad * mid_gain
        grad_middle = grad_out_ref[here, :] + scale * (
            grad_unit
            - jnp.mean(grad_unit, -1, keepdims=True)
            - unit * jnp.mean(grad_unit * unit, -1, keepdims=True)
        )
        middle_ref[here, :] = grad_middle
        grad_attn = grad_middle.astype(BF)
        down_ref[here, :] = grad_attn
        sums = (
            jnp.sum(grad_attn.astype(F32), 0, keepdims=True),
            jnp.sum(grad * unit, 0, keepdims=True),
            jnp.sum(grad, 0, keepdims=True),
        )
        return tuple(x + y for x, y in zip(carry, sums))

    sums = lax.fori_loop(0, count // tile, middle_back, (zero_row,) * 3)
    for i, value in enumerate(sums + (grad_b_down,)):
        vector_held[0, ring + 2 + i : ring + 3 + i, 0:width] = value
    for i in range(ring):
        here = slice(i * out_rows, (i + 1) * out_rows)
        g_ref[here, :] = dot(wo_all[here, :], down_ref[...], 1, 1).astype(BF)

    def g_copy(slot, to):
        return remote(
            g_ref.at[pl.ds(HEADS_AT[to][slot] * hd, hd)],
            g_all.at[slot, :, own],
            gsend.at[slot, to],
            grecv.at[slot, place.shift_to(to) - 1],
            (place.d, to),
        )

    for slot in range(heads_here):
        for to in range(ring):

            @pl.when(m == to)
            def _(slot=slot, to=to):
                row = HEADS_AT[to][slot] * hd
                g_all[slot, :, own] = g_ref[row : row + hd, :]

            @pl.when(m != to)
            def _(slot=slot, to=to):
                g_copy(slot, to).start()

    for j in range(ring):
        here = rows_of(shard_of(j) * out_rows, out_rows, 16)
        wo_share[shard_of(j), 0:out_rows, :] = dot(
            context_ref[here, :], down_ref[...], 1, 0
        ).astype(BF)
        out.copy(0, shard_of(j)).start()

    def weigh_shard(j, carry):
        s = shard_of(j)

        def weigh(i, carry):
            here = lanes(i * 256, 256)
            wu_all[s, :, here] = dot(mid_t[...], gup_ref[s, :, here], 1, 0).astype(BF)
            wd_all[s, :, here] = dot(down_t[...], act_ref[s, :, here], 1, 0).astype(BF)
            return carry

        lax.fori_loop(0, wu_all.shape[2] // 256, weigh, 0)
        down.copy(0, s).start()
        up.copy(0, s).start()

        @pl.when(j > 0)
        def _():
            down.fold_one(0, shard_of(j - 1))
            up.fold_one(0, shard_of(j - 1))

        return carry

    lax.fori_loop(0, ring, weigh_shard, 0)
    out.fold(0)
    down.fold_one(0, shard_of(ring - 1))
    up.fold_one(0, shard_of(ring - 1))
    for name in ("v", "qk", "lse", "exact"):
        loads[name].wait()

    def qk_copy(h, j):
        return remote(
            qk_ref.at[h, :, lanes(place.z(j) * count, count)],
            grad_ref.at[place.shard(h), rows_of(2 * hd * h, 2 * hd, 2 * hd)],
            qsend.at[h, j - 1],
            qrecv.at[h, j - 1],
            place.to_z(j),
        )

    v_row = 2 * hd * heads_here

    def v_copy(i, j):
        shard, row, rows, _, row_there = FRESH[i]
        return remote(
            v_ref.at[pl.ds(row_there, rows), lanes(place.z(j) * count, count)],
            grad_ref.at[shard, pl.ds(v_row + row, rows)],
            vsend.at[i, j - 1],
            vrecv.at[i, j - 1],
            place.to_z(j),
        )

    def moved_copy(i):
        to, row, rows, _, row_there = MOVED[i]
        return remote(
            v_ref.at[pl.ds(row_there, rows)],
            first_ref.at[pl.ds(row, rows)],
            fsend.at[0],
            frecv.at[0],
            (place.d, to),
        )

    def send_fresh(slot):
        for i, (shard, row, rows, at, row_there) in enumerate(FRESH):
            if (row_there + rows > 2 * hd) != (slot == 2):
                continue

            @pl.when(m == at)
            def _(i=i, shard=shard, row=row, rows=rows, row_there=row_there):
                for j in range(1, ring):
                    v_copy(i, j).start()
                grad_ref[shard, v_row + row : v_row + row + rows, :] = v_ref[
                    pl.ds(row_there, rows), own
                ]

    def send_reused():
        for i, move in enumerate(MOVED):

            @pl.when(m == move[3])
            def _(i=i):
                moved_copy(i).start()

        for at, row, rows, row_there in KEPT:

            @pl.when(m == at)
            def _(row=row, rows=rows, row_there=row_there):
                first_ref[row : row + rows, :] = v_ref[row_there : row_there + rows, :]

    ones = jnp.ones((8, count), BF)

    def process(i):
        if i == 0:
            for name in ("normed", "wt"):
                loads[name].wait()
            for k in range(ring):
                up.copy(0, k).wait_send()
        if i < heads_here:
            for j in range(1, ring):
                qk_copy(i, j).wait_recv()
        begin = group * i
        here = slice(begin, begin + group)
        for k in range(ring):
            wu_all[k, here, :] = dot(grad_ref[k, here, :], mid_ref[...], 1, 0).astype(BF)
            packs[i].copy(0, k).start()
        for k in range(ring):
            sums = dot(ones, grad_ref[k, here, :], 1, 1)
            vector_held[0, k : k + 1, here] = sums[0:1]
        weights = jnp.concatenate([wt_all[k, here, :] for k in range(ring)], 0)

        def add(t, carry):
            toks = lanes(t * tile, tile)
            grads = jnp.concatenate([grad_ref[k, here, toks] for k in range(ring)], 0)
            part = dot(grads, weights, 0, 0)
            rows = rows_of(t * tile, tile, tile)
            grad_in_ref[rows, :] = part if i == 0 else grad_in_ref[rows, :] + part
            return carry

        lax.fori_loop(0, count // tile, add, 0)

    boundary = length_ref[0]
    block = count
    def attend_back(h, carry):
        here_h = rows_of(hd * h, hd, hd)
        keys[...] = jnp.transpose(qk_ref[h, hd : 2 * hd, :])
        vals[...] = jnp.transpose(v_ref[here_h, :])
        for j in range(1, ring):
            remote(
                g_ref.at[pl.ds(0, hd)],
                g_all.at[h, :, own],
                gsend.at[h, 0],
                grecv.at[h, j - 1],
                place.to_z(j),
            ).wait_recv()
        delta[...] = jnp.sum(
            g_all[h].astype(F32) * exact_ref[here_h, :], 0, keepdims=True
        )
        for ki in range(ring):
            key_start = ki * block
            key_rows = keys[key_start : key_start + block, :]
            val_rows = vals[key_start : key_start + block, :]
            key_t = qk_ref[h, hd : 2 * hd, key_start : key_start + block]
            grad_k = None
            for qi in range(ki, ring):
                query_start = qi * block
                here = slice(query_start, query_start + block)
                q = qk_ref[h, 0:hd, here]
                g = g_all[h, :, here]
                scores = dot(key_rows, q, 1, 0) - lse_ref[h, :, here]
                if ki == qi:
                    scores = jnp.where(
                        diagonal_mask(scores, key_start, query_start), scores, NEG_LARGE
                    )
                elif key_start < half <= query_start:
                    scores = scores + other_document(boundary, key_start, query_start)
                p = jnp.exp(scores)
                grad_p = dot(val_rows, g, 1, 0)
                grad_s = (p * (grad_p - delta[:, here])).astype(BF)
                part_v = dot(g, p.astype(BF), 1, 1)
                part_k = dot(q, grad_s, 1, 1)
                if grad_k is None:
                    grad_v, grad_k = part_v, part_k
                else:
                    grad_v, grad_k = grad_v + part_v, grad_k + part_k
                part_q = dot(key_t, grad_s, 1, 0)
                if ki == 0:
                    dq[:, here] = part_q
                else:
                    dq[:, here] += part_q
            qk_ref[h, hd : 2 * hd, key_start : key_start + block] = grad_k.astype(BF)
            v_ref[here_h, key_start : key_start + block] = grad_v.astype(BF)
        qk_ref[h, 0:hd, :] = (dq[...] * (hd**-0.5)).astype(BF)
        for j in range(1, ring):
            qk_copy(h, j).start()
        grad_ref[place.shard(h), rows_of(2 * hd * h, 2 * hd, 2 * hd), :] = qk_ref[h, :, own]

        @pl.when(h == 1)
        def _():
            send_fresh(1)

        return carry

    lax.fori_loop(0, heads_here, attend_back, 0)
    send_fresh(2)
    send_reused()
    ffn = (down, up, out)
    for item in ffn:
        item.fold(1)
    process(0)
    process(1)
    packs[0].fold(0)
    packs[1].fold(0)
    packs[0].fold(1)
    for item in ffn:
        item.fold(2)
    packs[1].fold(1)
    packs[0].fold(2)
    for to in range(ring):

        @pl.when(m != to)
        def _(to=to):
            for slot in range(heads_here):
                g_copy(slot, to).wait_send()

    for i, (shard, row, rows, at, row_there) in enumerate(FRESH):

        @pl.when(m == at)
        def _(i=i):
            for j in range(1, ring):
                v_copy(i, j).wait_send()

        @pl.when(m != at)
        def _(i=i, shard=shard, row=row, rows=rows, at=at, row_there=row_there):
            shift = lax.rem(m - at + ring, ring)
            remote(
                v_ref.at[pl.ds(row_there, rows), own],
                grad_ref.at[shard, pl.ds(v_row + row, rows)],
                vsend.at[i, shift - 1],
                vrecv.at[i, shift - 1],
                place.to_z(shift),
            ).wait_recv()

    for i, move in enumerate(MOVED):

        @pl.when(m == move[3])
        def _(i=i):
            moved_copy(i).wait_send()

        @pl.when(m == move[0])
        def _(i=i):
            moved_copy(i).wait_recv()

    process(2)
    process(3)

    def input_back(i, carry):
        here = rows_of(i * tile, tile, tile)
        grad = grad_in_ref[here, :]
        value = hidden_ref[here, :]
        center = value - jnp.mean(value, -1, keepdims=True)
        scale = lax.rsqrt(jnp.mean(center * center, -1, keepdims=True) + EPSILON)
        unit = center * scale
        grad_unit = grad * pre_gain_ref[...]
        grad_in_ref[here, :] = middle_ref[here, :] + scale * (
            grad_unit
            - jnp.mean(grad_unit, -1, keepdims=True)
            - unit * jnp.mean(grad_unit * unit, -1, keepdims=True)
        )
        sums = (
            jnp.sum(grad * unit, 0, keepdims=True),
            jnp.sum(grad, 0, keepdims=True),
        )
        return tuple(x + y for x, y in zip(carry, sums))

    sums = lax.fori_loop(0, count // tile, input_back, (zero_row,) * 2)
    for i, value in enumerate(sums):
        vector_held[0, ring + i : ring + 1 + i, 0:width] = value

    routes = [place.to_core, place.to_x, place.to_y]
    routes += [place.to_plane(step) for step in place.steps()]
    bit = 1
    while bit < ring:
        routes.append((place.d, m + bit - 2 * bit * lax.rem(m // bit, 2)))
        bit *= 2

    def vector_copy(k):
        return remote(
            vector_held.at[k], vector_came.at[k], wsend.at[k], wrecv.at[k], routes[k]
        )

    def vector_fold(k):
        vector_copy(k).wait_recv()
        value = vector_held[k] + vector_came[k]
        if k + 1 < len(routes):
            vector_held[k + 1] = value
            vector_copy(k + 1).start()
        else:
            vector_sum[...] = value

    vector_copy(0).start()
    first, second, third, fourth = packs
    second.fold(2)
    third.fold(0)
    fourth.fold(0)
    vector_fold(0)
    for item in ffn:
        item.fold_pair()
    third.fold(1)
    fourth.fold(1)
    vector_fold(1)
    first.fold_pair()
    second.fold_pair()
    for item in ffn:
        item.finish_sum()
    third.fold(2)
    fourth.fold(2)
    vector_fold(2)
    first.finish_sum()
    second.finish_sum()
    third.fold_pair()
    fourth.fold_pair()
    for item in ffn:
        item.spread(6)
    for k in range(3, len(routes) - 1):
        vector_fold(k)
    first.spread(6)
    second.spread(6)
    third.finish_sum()
    fourth.finish_sum()
    for item in ffn:
        item.spread(7)
    vector_fold(len(routes) - 1)
    for item in packs:
        item.spread(6 if item in (third, fourth) else 7)
    third.spread(7)
    fourth.spread(7)
    everything = ffn + tuple(packs)
    for item in everything:
        item.wait(7)
        item.drain(1 if item is up else 0)
    for k in range(len(routes)):
        vector_copy(k).wait_send()
    for h in range(heads_here):
        for j in range(1, ring):
            qk_copy(h, j).wait_send()


def backward_call(
    ring, heads_here, planes, length, context, hidden, grad_out, pre_gain, rows, bias,
    qk, v, lse, exact, normed, wt, wo, wo_far, wu, wu_far, wd, wd_far, piece,
):
    count, width = hidden.shape
    total = ring * count
    hd = HEAD_DIM
    others = ring - 1
    sds = jax.ShapeDtypeStruct
    dma = pltpu.SemaphoreType.DMA
    hops = 3 + (planes.bit_length() - 1) + (ring.bit_length() - 1)
    stages = 8 + planes.bit_length() - 1
    pack_rows = wt.shape[1]
    out_pad = wo.shape[0] + -wo.shape[0] % (16 * PLANE)
    sizes = [wd.shape[0], wu.shape[0], out_pad] + [2 * hd] * (heads_here + 1)
    bufs = [buf for rows_ in sizes for buf in Reduce.buffers(rows_, width, planes)]
    vector = (ring + 6 + -(ring + 6) % 8, bias.shape[2])
    vm = pltpu.VMEM
    return pl.pallas_call(
        functools.partial(backward_kernel, ring, heads_here, planes),
        out_shape=(
            sds(hidden.shape, F32),
            sds(hidden.shape, F32),
            sds((piece, total), BF),
            sds(wt.shape[1:], BF),
            sds((out_pad, width), BF),
            sds(wu.shape, BF),
            sds(wd.shape, BF),
            sds(vector, F32),
        ),
        in_specs=[SM] + [VM] * 6 + [ANY] * 12,
        out_specs=[VM] * 8,
        scratch_shapes=[
            vm(qk.shape, BF),
            vm(v.shape, BF),
            vm(lse.shape, F32),
            vm(exact.shape, F32),
            vm(wt.shape, BF),
            vm((ring * wo.shape[0], width), BF),
            vm((ring,) + wu.shape, BF),
            vm((ring,) + wd.shape, BF),
            vm((count, width), F32),
            vm((count, width), BF),
            vm((width, count), BF),
            vm((count, width), BF),
            vm((width, count), BF),
            vm((ring, count, width), BF),
            vm((ring, count, width), BF),
            vm((width, count), BF),
            vm((ring, out_pad, width), BF),
            vm((heads_here, hd, total), BF),
            vm((total, hd), BF),
            vm((total, hd), BF),
            vm((1, total), F32),
            vm((hd, total), F32),
            vm((ring, pack_rows, count), BF),
            vm((hops,) + vector, F32),
            vm((hops,) + vector, F32),
            dma((3 * ring + 6,)),
            dma((heads_here, ring)),
            dma((heads_here, others)),
            dma((heads_here, others)),
            dma((heads_here, others)),
            dma((len(FRESH), others)),
            dma((len(FRESH), others)),
            dma((1,)),
            dma((1,)),
            dma((3 + heads_here + 1, stages, ring)),
            dma((3 + heads_here + 1, stages, ring)),
            dma((hops,)),
            dma((hops,)),
        ]
        + bufs,
        compiler_params=pltpu.CompilerParams(
            collective_id=1, has_side_effects=True, vmem_limit_bytes=67043328
        ),
        name="backward",
    )(
        length, context, hidden, grad_out, pre_gain, rows, bias, qk, v, lse, exact,
        normed, wt, wo, wo_far, wu, wu_far, wd, wd_far,
    )


def shards(
    hidden_in,
    first_values,
    first_length,
    pre_gain,
    pre_shift,
    w_query,
    b_query,
    w_key,
    w_value,
    b_value,
    w_out,
    b_out,
    mid_gain,
    mid_shift,
    w_up,
    b_up,
    w_down,
    b_down,
    grad_out,
):
    ring = lax.axis_size("mp")
    m = lax.axis_index("mp")
    hd = HEAD_DIM
    count, width = hidden_in.shape
    head_width = w_query.shape[1]
    heads_here = head_width // hd
    piece = w_value.shape[1]
    pack_rows = 2 * hd * (heads_here + 1)
    turned = jnp.logical_or(m == 1, m == 2)

    def to_slots(value):
        return jnp.where(turned, jnp.roll(value, -1, 0), value)

    def from_slots(value):
        return jnp.where(turned, jnp.roll(value, 1, 0), value)

    wq = to_slots(w_query.T.reshape(heads_here, 1, hd, width))
    wk = to_slots(w_key.T.reshape(heads_here, 1, hd, width))
    spare = pack_rows - 2 * head_width - piece
    wt = jnp.concatenate(
        [
            jnp.concatenate([wq, wk], 1).reshape(2 * head_width, width),
            w_value.T,
            jnp.zeros((spare, width), BF),
        ],
        0,
    )
    bq = to_slots(b_query.reshape(heads_here, 1, hd))
    bias = jnp.concatenate(
        [
            jnp.concatenate([bq, jnp.zeros_like(bq)], 1).reshape(-1),
            b_value,
            jnp.zeros((spare,), F32),
            b_up,
        ]
    )
    bias = jnp.broadcast_to(bias[None], (8, bias.shape[0]))
    context_t, normed, qk, v, lse, exact, wt_all, bias_all, wo_far, wu_far, wd_far = forward_call(
        ring,
        heads_here,
        first_length,
        hidden_in,
        pre_gain[None],
        pre_shift[None],
        wt,
        bias,
        first_values.T,
        w_out,
        w_up,
        w_down,
    )
    rows = jnp.stack([b_out, mid_gain, mid_shift, b_down] * 2)
    layer_out, grad_input, grad_first, pack_sum, wo_sum, wu_sum, wd_sum, vector = backward_call(
        ring,
        heads_here,
        lax.axis_size("dp") // PLANE,
        first_length,
        context_t,
        hidden_in,
        grad_out,
        pre_gain[None],
        rows,
        bias_all,
        qk,
        v,
        lse,
        exact,
        normed,
        wt_all,
        w_out,
        wo_far,
        w_up,
        wu_far,
        w_down,
        wd_far,
        piece,
    )
    own_vector = lax.dynamic_index_in_dim(vector, m, 0, False)
    qk_grad = from_slots(pack_sum[: 2 * head_width].astype(F32).reshape(heads_here, 2, hd, width))
    v_grad = pack_sum[2 * head_width : 2 * head_width + piece].astype(F32)
    rows = [vector[ring + i, :width] for i in range(6)]
    return (
        layer_out,
        grad_input,
        grad_first.astype(F32).T,
        rows[0],
        rows[1],
        qk_grad[:, 0].reshape(head_width, width).T,
        from_slots(own_vector[: 2 * head_width].reshape(heads_here, 2, hd))[:, 0].reshape(-1),
        qk_grad[:, 1].reshape(head_width, width).T,
        v_grad.T,
        own_vector[2 * head_width : 2 * head_width + piece],
        wo_sum[:head_width].astype(F32),
        rows[2],
        rows[3],
        rows[4],
        wu_sum.astype(F32),
        own_vector[pack_rows:],
        wd_sum.astype(F32).T,
        rows[5],
    )


def solution(mesh):
    rows, cols = P(("dp", "mp"), None), P(None, "mp")
    return jax.shard_map(
        shards,
        mesh=mesh,
        in_specs=(
            rows,
            P("dp", "mp"),
            P("dp"),
            P(),
            P(),
            cols,
            P("mp"),
            cols,
            cols,
            P("mp"),
            P("mp", None),
            P(),
            P(),
            P(),
            cols,
            P("mp"),
            P("mp", None),
            P(),
            rows,
        ),
        out_specs=(
            rows,
            rows,
            P("dp", "mp"),
            P(),
            P(),
            cols,
            P("mp"),
            cols,
            cols,
            P("mp"),
            P("mp", None),
            P(),
            P(),
            P(),
            cols,
            P("mp"),
            P("mp", None),
            P(),
        ),
        check_vma=False,
    )
```

```python
import functools

import jax
import jax.numpy as jnp
from jax import lax
from jax.experimental import pallas as pl
from jax.experimental.pallas import tpu as pltpu
from jax.sharding import PartitionSpec as P

HEAD_DIM = 64
EPSILON = 1e-05
NEG_LARGE = -1e30
MESH = pl.DeviceIdType.MESH
BF = jnp.bfloat16
F32 = jnp.float32
ANY = pl.BlockSpec(memory_space=pl.ANY)
VM = pl.BlockSpec(memory_space=pltpu.VMEM)
SM = pl.BlockSpec(memory_space=pltpu.SMEM)
VMEM_LIMIT = 60 << 20
LANE = 128
PLANE = 8
RING = 4
HEADS_AT = ((0, 1, 6), (7, 8, 2), (9, 10, 3), (4, 5, 11))
FRESH = (
    (0, 0, 96, 0, 0),
    (1, 0, 32, 0, 96),
    (1, 32, 64, 1, 128),
    (2, 0, 64, 2, 128),
    (2, 64, 32, 3, 0),
    (3, 0, 96, 3, 32),
)
KEPT = ((0, 0, 64, 128), (1, 0, 96, 32), (2, 0, 96, 0), (3, 32, 64, 128))
MOVED = ((0, 64, 32, 1, 0), (3, 0, 32, 2, 96))


def dot(left, right, left_dim, right_dim):
    return lax.dot_general(
        left, right, (((left_dim,), (right_dim,)), ((), ())), preferred_element_type=F32
    )


def layer_norm(values, gain, shift):
    center = values - jnp.mean(values, -1, keepdims=True)
    spread = jnp.mean(center * center, -1, keepdims=True)
    return center * lax.rsqrt(spread + EPSILON) * gain + shift


def gelu_tanh(values):
    return (
        0.5
        * values
        * (1.0 + jnp.tanh(0.7978845608028654 * (values + 0.044715 * values * values * values)))
    )


def lanes(start, size):
    return pl.ds(pl.multiple_of(start, LANE), size)


def rows_of(start, size, unit):
    return pl.ds(pl.multiple_of(start, unit), size)


def flat(ref):
    return jnp.reshape(ref[...], (1, ref.shape[0]))


class Place:
    def __init__(self, ring, planes=1):
        self.ring = ring
        self.planes = planes
        self.d = lax.axis_index("dp")
        self.m = lax.axis_index("mp")
        d = self.d
        self.core = lax.rem(d, 2)
        self.x = lax.rem(d // 2, 2)
        self.y = lax.rem(d // 4, 2)
        self.to_core = (d + 1 - 2 * self.core, self.m)
        self.to_x = (d + 2 - 4 * self.x, self.m)
        self.to_y = (d + 4 - 8 * self.y, self.m)
        self.pair = self.m + 1 - 2 * lax.rem(self.m, 2)
        self.across = lax.rem(self.m + 2, RING)
        self.corner = RING - 1 - self.m

    def z(self, shift):
        return lax.rem(self.m + shift, self.ring)

    def to_z(self, shift):
        return (self.d, self.z(shift))

    def shift_to(self, position):
        return lax.rem(position - self.m + self.ring, self.ring)

    def head(self, slot):
        value = 0
        for k, heads in enumerate(HEADS_AT):
            for at, head in enumerate(heads):
                value = jnp.where(jnp.logical_and(self.m == k, slot == at), head, value)
        return value

    def shard(self, slot):
        return self.head(slot) // len(HEADS_AT[0])

    def steps(self):
        return [PLANE << b for b in range(self.planes.bit_length() - 1)]

    def to_plane(self, step):
        return (self.d + step - 2 * step * lax.rem(self.d // step, 2), self.m)

    def barrier(self):
        sem = pltpu.get_barrier_semaphore()
        peers = [self.to_z(j) for j in range(1, self.ring)]
        peers += [self.to_core, self.to_x, self.to_y]
        peers += [self.to_plane(step) for step in self.steps()]
        for peer in peers:
            pl.semaphore_signal(sem, inc=1, device_id=peer, device_id_type=MESH)
        pl.semaphore_wait(sem, len(peers))

    def slot(self, x_first):
        if x_first:
            return self.core * 4 + self.y * 2 + self.x
        return self.core * 4 + self.x * 2 + self.y


def remote(src, dst, send, recv, device):
    return pltpu.make_async_remote_copy(
        src_ref=src,
        dst_ref=dst,
        send_sem=send,
        recv_sem=recv,
        device_id=device,
        device_id_type=MESH,
    )


class Gather:
    def __init__(self, place, src, dst, send, recv, item, first_row, rows, x_first):
        self.place, self.src, self.dst = place, src, dst
        self.send, self.recv, self.item = send, recv, item
        self.first_row, self.part, self.x_first = first_row, rows // PLANE, x_first

    def window(self, start, size):
        part = self.part
        return rows_of(self.first_row + start * part, size * part, part & -part)

    def copy(self, stage, k):
        place = self.place
        slot = place.slot(self.x_first)
        near, far = (place.to_x, place.to_y) if self.x_first else (place.to_y, place.to_x)
        shard = (place.across, place.pair, place.corner)[k]
        window = self.window(slot, 1)
        if stage == 0:
            shard, target = place.m, (place.d, place.across)
        elif stage == 1:
            shard, target = (place.m, place.across)[k], (place.d, place.pair)
        elif stage == 2:
            target = near
        elif stage == 3:
            window, target = self.window((slot // 2) * 2, 2), far
        else:
            window, target = self.window(place.core * 4, 4), place.to_core
        own = stage == 0 or (stage == 1 and k == 0)
        source = self.src.at[window] if own else self.dst.at[shard, window]
        return remote(
            source,
            self.dst.at[shard, window],
            self.send.at[self.item, stage, k],
            self.recv.at[self.item, stage, k],
            target,
        )

    def start(self, stage):
        if stage == 0:
            self.copy(0, 0).start()
            self.copy(1, 0).start()
        elif stage == 1:
            self.copy(0, 0).wait_recv()
            self.copy(1, 1).start()
        else:
            for k in range(2 if stage == 2 else 3):
                self.copy(stage - 1, k).wait_recv()
            for k in range(3):
                self.copy(stage, k).start()

    def arrive(self):
        for k in range(3):
            self.copy(4, k).wait_recv()

    def drain(self):
        for stage, copies in enumerate((1, 2, 3, 3, 3)):
            for k in range(copies):
                self.copy(stage, k).wait_send()


class Reduce:
    def __init__(self, place, src, bufs, out, send, recv, item, x_first, first_row=0):
        self.place, self.src, self.out = place, src, out
        self.first_row = first_row
        self.r_core, self.r_far, self.r_near, self.r_z, self.r_plane = bufs
        self.send, self.recv, self.item, self.x_first = send, recv, item, x_first
        self.part = out.shape[0] // PLANE
        if x_first:
            self.near, self.far = place.to_x, place.to_y
            self.near_bit, self.far_bit = place.x, place.y
        else:
            self.near, self.far = place.to_y, place.to_x
            self.near_bit, self.far_bit = place.y, place.x

    def rows(self, start, size):
        return rows_of(start * self.part, size * self.part, self.part & -self.part)

    def copy(self, stage, k):
        place = self.place
        if stage == 0:
            begin = self.first_row + (1 - place.core) * 4 * self.part
            src = self.src.at[k, rows_of(begin, 4 * self.part, self.part & -self.part)]
            dst, target = self.r_core.at[k], place.to_core
        elif stage == 1:
            src = self.r_core.at[k, self.rows((1 - self.far_bit) * 2, 2)]
            dst, target = self.r_far.at[k], self.far
        elif stage == 2:
            src = self.r_far.at[k, self.rows(1 - self.near_bit, 1)]
            dst, target = self.r_near.at[k], self.near
        elif stage == 3:
            src = self.r_near.at[(place.pair, place.corner)[k]]
            dst, target = self.r_z.at[k], (place.d, place.pair)
        elif stage == 4:
            src = self.r_near.at[place.across]
            dst, target = self.r_z.at[2], (place.d, place.across)
        else:
            slot = place.slot(self.x_first)
            if stage == 5:
                window, target = self.rows(slot, 1), self.near
            elif stage == 6:
                window, target = self.rows((slot // 2) * 2, 2), self.far
            else:
                window, target = self.rows(place.core * 4, 4), place.to_core
            src = dst = self.out.at[window]
        return remote(
            src, dst, self.send.at[self.item, stage, k], self.recv.at[self.item, stage, k], target
        )

    def members(self, stage):
        return range((RING, RING, RING, 2, 1, 1, 1, 1)[stage])

    def start(self, stage):
        for k in self.members(stage):
            self.copy(stage, k).start()

    def wait(self, stage):
        for k in self.members(stage):
            self.copy(stage, k).wait_recv()

    def fold_one(self, stage, k):
        place, part = self.place, self.part
        if stage == 0:
            base = self.first_row + place.core * 4 * part
            kept, into, size = self.src, self.r_core, 4 * part
        elif stage == 1:
            kept, base, into, size = self.r_core, self.far_bit * 2 * part, self.r_far, 2 * part
        else:
            kept, base, into, size = self.r_far, self.near_bit * part, self.r_near, part
        unit = part & -part
        step = min(unit, 32)
        self.copy(stage, k).wait_recv()

        def add(i, carry):
            mine = kept[k, rows_of(base + i * step, step, min(unit, step)), :].astype(F32)
            here = rows_of(i * step, step, step)
            into[k, here, :] = (into[k, here, :].astype(F32) + mine).astype(BF)
            return carry

        lax.fori_loop(0, size // step, add, 0)
        if stage < 2:
            self.copy(stage + 1, k).start()

    def fold(self, stage):
        for k in self.members(stage):
            self.fold_one(stage, k)
        if stage == 2:
            self.start(3)

    def fold_pair(self):
        place = self.place
        self.wait(3)
        other = self.r_near[place.across].astype(F32) + self.r_z[1].astype(F32)
        self.r_near[place.across] = other.astype(BF)
        self.start(4)
        mine = self.r_near[place.m].astype(F32) + self.r_z[0].astype(F32)
        self.r_near[place.m] = mine.astype(BF)

    def finish_sum(self):
        place = self.place
        self.wait(4)
        here = self.rows(place.slot(self.x_first), 1)
        value = self.r_near[place.m].astype(F32) + self.r_z[2].astype(F32)
        self.out[here, :] = value.astype(BF)
        for b, step in enumerate(place.steps()):
            copy = remote(
                self.out.at[here],
                self.r_plane.at[b],
                self.send.at[self.item, 8 + b, 0],
                self.recv.at[self.item, 8 + b, 0],
                place.to_plane(step),
            )
            copy.start()
            copy.wait()
            mine = self.out[here, :].astype(F32)
            self.out[here, :] = (mine + self.r_plane[b].astype(F32)).astype(BF)
        self.start(5)

    def spread(self, stage):
        self.wait(stage - 1)
        self.start(stage)

    def drain(self, first):
        for stage in range(first, 8):
            for k in self.members(stage):
                self.copy(stage, k).wait_send()

    @staticmethod
    def buffers(rows, width, planes):
        part = rows // PLANE
        extra = max(planes.bit_length() - 1, 1)
        return [
            pltpu.VMEM((RING, 4 * part, width), BF),
            pltpu.VMEM((RING, 2 * part, width), BF),
            pltpu.VMEM((RING, part, width), BF),
            pltpu.VMEM((3, part, width), BF),
            pltpu.VMEM((extra, part, width), BF),
        ]


def diagonal_mask(scores, key_start, query_start):
    keys = lax.broadcasted_iota(jnp.int32, scores.shape, 0) + key_start
    queries = lax.broadcasted_iota(jnp.int32, scores.shape, 1) + query_start
    return keys <= queries


def other_document(boundary, key_start, query_start):
    crossing = jnp.logical_and(boundary > key_start, boundary <= query_start)
    return jnp.where(crossing, NEG_LARGE, 0.0)


def forward_kernel(
    ring,
    heads_here,
    length_ref,
    hidden_ref,
    gain_ref,
    shift_ref,
    wq_ref,
    wk_ref,
    wv_ref,
    bq_ref,
    bv_ref,
    bu_ref,
    first_ref,
    wo_ref,
    wu_ref,
    wd_ref,
    context_ref,
    normed_ref,
    qk_ref,
    v_ref,
    lse_ref,
    exact_ref,
    wt_all,
    bias_all,
    wo_far,
    wu_far,
    wd_far,
    y_send,
    vy_send,
    c_send,
    keys,
    gsend,
    grecv,
    bsend,
    brecv,
    qsend,
    qrecv,
    vsend,
    vrecv,
    fsend,
    frecv,
    csend,
    crecv,
):
    place = Place(ring)
    m = place.m
    count = hidden_ref.shape[0]
    total = ring * count
    piece = first_ref.shape[0]
    half = total // 2
    hd = HEAD_DIM
    pack_rows = wt_all.shape[1]
    v_row = 2 * hd * heads_here
    turned = jnp.logical_or(m == 1, m == 2)

    def slot_row(slot):
        return rows_of(hd * jnp.where(turned, (slot + 1) % heads_here, slot), hd, hd)

    bq, bv, bu = flat(bq_ref), flat(bv_ref), flat(bu_ref)
    bias_parts = []
    for slot in range(heads_here):
        row = 2 * hd * slot
        wt_all[m, row : row + hd, :] = wq_ref[slot_row(slot), :]
        wt_all[m, row + hd : row + 2 * hd, :] = wk_ref[slot_row(slot), :]
        here, after = hd * slot, hd * ((slot + 1) % heads_here)
        own_bias = jnp.where(turned, bq[:, after : after + hd], bq[:, here : here + hd])
        bias_parts += [own_bias, jnp.zeros_like(own_bias)]
    wt_all[m, v_row : v_row + piece, :] = wv_ref[...]
    spare = pack_rows - v_row - piece
    wt_all[m, v_row + piece :, :] = jnp.zeros((spare, wv_ref.shape[1]), BF)
    bias_parts += [bv, jnp.zeros((1, spare), F32), bu]
    bias_row = jnp.concatenate(bias_parts, 1)
    bias_all[m] = jnp.broadcast_to(bias_row, (8, bias_row.shape[1]))
    wt_ref = wt_all.at[m]
    bias_ref = bias_all.at[m]
    place.barrier()
    half_pack = pack_rows // 2
    small = [
        Gather(place, wt_ref, wt_all, gsend, grecv, i, i * half_pack, half_pack, i == 0)
        for i in range(2)
    ]
    big = [
        Gather(place, wo_ref, wo_far, gsend, grecv, 2, 0, wo_ref.shape[0], True),
        Gather(place, wu_ref, wu_far, gsend, grecv, 3, 0, wu_ref.shape[0], True),
        Gather(place, wd_ref, wd_far, gsend, grecv, 4, 0, wd_ref.shape[0], False),
    ]
    for item in small:
        item.start(0)

    def bias_copy(j):
        return remote(
            bias_ref, bias_all.at[m], bsend.at[j - 1], brecv.at[j - 1], place.to_z(j)
        )

    for j in range(1, ring):
        bias_copy(j).start()

    def moved_copy(i):
        _, row, rows, to, row_there = MOVED[i]
        return remote(
            first_ref.at[pl.ds(row, rows)],
            v_ref.at[pl.ds(row_there, rows)],
            fsend.at[0],
            frecv.at[0],
            (place.d, to),
        )

    for i, move in enumerate(MOVED):

        @pl.when(m == move[0])
        def _(i=i):
            moved_copy(i).start()

    for at, row, rows, row_there in KEPT:

        @pl.when(m == at)
        def _(row=row, rows=rows, row_there=row_there):
            v_ref[row_there : row_there + rows, :] = first_ref[row : row + rows, :]

    normed_ref[...] = layer_norm(hidden_ref[...], flat(gain_ref), flat(shift_ref)).astype(BF)

    for item in small:
        item.start(1)
    for item in big:
        item.start(0)
    for item in small:
        item.start(2)
    for item in big:
        item.start(1)
    for stage in (3, 4):
        for item in small:
            item.start(stage)
    for j in range(1, ring):
        bias_copy(j).wait_recv()
    for item in small:
        item.arrive()

    own = lanes(m * count, count)

    def qk_copy(slot, to):
        return remote(
            y_send.at[to, slot],
            qk_ref.at[slot, :, own],
            qsend.at[to, slot],
            qrecv.at[slot, place.shift_to(to) - 1],
            (place.d, to),
        )

    def v_copy(i):
        shard, row, rows, to, row_there = FRESH[i]
        return remote(
            vy_send.at[shard, pl.ds(row, rows)],
            v_ref.at[pl.ds(row_there, rows), own],
            vsend.at[i],
            vrecv.at[i, place.shift_to(to) - 1],
            (place.d, to),
        )

    where_is = {
        (head // heads_here, slot): to
        for to, heads in enumerate(HEADS_AT)
        for slot, head in enumerate(heads)
    }

    for shard in range(ring):
        out = dot(wt_all[shard], normed_ref[...], 1, 1)
        out = out + jnp.transpose(bias_all[shard, :, 0:pack_rows])[:, 0:1]
        for slot in range(heads_here):
            to = where_is[shard, slot]
            row = 2 * hd * slot
            y_send[to, slot, 0:hd, :] = (out[row : row + hd] * (hd**-0.5)).astype(BF)
            y_send[to, slot, hd : 2 * hd, :] = out[row + hd : row + 2 * hd].astype(BF)
        vy_send[shard] = out[v_row : v_row + piece].astype(BF)

    def share(slot):
        for to in range(ring):

            @pl.when(m == to)
            def _(to=to):
                qk_ref[slot, :, own] = y_send[to, slot]

            @pl.when(m != to)
            def _(to=to):
                qk_copy(slot, to).start()

    share(0)
    for i, (shard, row, rows, to, row_there) in enumerate(FRESH):

        @pl.when(m == to)
        def _(shard=shard, row=row, rows=rows, row_there=row_there):
            v_ref[row_there : row_there + rows, own] = vy_send[shard, row : row + rows, :]

        @pl.when(m != to)
        def _(i=i):
            v_copy(i).start()

    for slot in range(1, heads_here):
        share(slot)
    for stage in (2, 3):
        for item in big:
            item.start(stage)

    def qk_arrive(slot):
        for shift in range(1, ring):
            remote(
                y_send.at[0, slot],
                qk_ref.at[slot, :, own],
                qsend.at[0, slot],
                qrecv.at[slot, shift - 1],
                place.to_z(shift),
            ).wait_recv()

    for i, (shard, row, rows, to, row_there) in enumerate(FRESH):

        @pl.when(m == to)
        def _(i=i, shard=shard, row=row, rows=rows, row_there=row_there):
            for shift in range(1, ring):
                remote(
                    vy_send.at[shard, pl.ds(row, rows)],
                    v_ref.at[pl.ds(row_there, rows), own],
                    vsend.at[i],
                    vrecv.at[i, shift - 1],
                    place.to_z(shift),
                ).wait_recv()

    for i, move in enumerate(MOVED):

        @pl.when(m == move[3])
        def _(i=i):
            moved_copy(i).wait_recv()

    boundary = length_ref[0]
    block = count

    def context_copy(h, j):
        return remote(
            c_send.at[rows_of(hd * h, hd, hd), lanes(place.z(j) * count, count)],
            context_ref.at[rows_of(place.head(h) * hd, hd, hd)],
            csend.at[h, j - 1],
            crecv.at[h, j - 1],
            place.to_z(j),
        )

    def attend(h, carry):
        qk_arrive(h)
        here_h = rows_of(hd * h, hd, hd)
        keys[...] = jnp.transpose(qk_ref[h, hd : 2 * hd, :])
        for qi in range(ring):
            query_start = qi * block
            queries = slice(query_start, query_start + block)
            q = qk_ref[h, 0:hd, queries]
            top = None
            for ki in range(qi + 1):
                key_start = ki * block
                v = v_ref[here_h, key_start : key_start + block]
                scores = dot(keys[key_start : key_start + block, :], q, 1, 0)
                if ki == qi:
                    scores = jnp.where(
                        diagonal_mask(scores, key_start, query_start), scores, NEG_LARGE
                    )
                elif key_start < half <= query_start:
                    scores = scores + other_document(boundary, key_start, query_start)
                block_top = jnp.max(scores, 0, keepdims=True)
                new_top = block_top if top is None else jnp.maximum(top, block_top)
                p = jnp.exp(scores - new_top)
                p_sum = jnp.sum(p, 0, keepdims=True)
                part = dot(v, p.astype(BF), 1, 0)
                if top is None:
                    run_sum, running = p_sum, part
                else:
                    factor = jnp.exp(top - new_top)
                    run_sum = run_sum * factor + p_sum
                    running = running * factor + part
                top = new_top
            result = running / run_sum
            exact_ref[here_h, queries] = result
            c_send[here_h, queries] = result.astype(BF)
            lse_ref[h, :, queries] = top + jnp.log(run_sum)
        for j in range(1, ring):
            context_copy(h, j).start()
        context_ref[rows_of(place.head(h) * hd, hd, hd), :] = c_send[here_h, own]

        @pl.when(h == 1)
        def _():
            for item in big:
                item.start(4)

        return carry

    lax.fori_loop(0, heads_here, attend, 0)
    for item in big:
        item.arrive()
    for h in range(heads_here):
        for j in range(1, ring):
            context_copy(h, j).wait_recv()
    for item in small + big:
        item.drain()
    for j in range(1, ring):
        bias_copy(j).wait_send()
        for h in range(heads_here):
            context_copy(h, j).wait_send()
    for to in range(ring):

        @pl.when(m != to)
        def _(to=to):
            for slot in range(heads_here):
                qk_copy(slot, to).wait_send()

    for i, (shard, row, rows, to, row_there) in enumerate(FRESH):

        @pl.when(m != to)
        def _(i=i):
            v_copy(i).wait_send()

    for i, move in enumerate(MOVED):

        @pl.when(m == move[0])
        def _(i=i):
            moved_copy(i).wait_send()


def forward_call(
    ring, heads_here, length, hidden, gain, shift, wq, wk, wv, bq, bv, bu, first_t, wo, wu, wd
):
    count, width = hidden.shape
    total = ring * count
    hd = HEAD_DIM
    piece = first_t.shape[0]
    others = ring - 1
    pack_rows = 2 * hd * (heads_here + 1)
    sds = jax.ShapeDtypeStruct
    dma = pltpu.SemaphoreType.DMA
    return pl.pallas_call(
        functools.partial(forward_kernel, ring, heads_here),
        out_shape=(
            sds((ring * heads_here * hd, count), BF),
            sds((count, width), BF),
            sds((heads_here, 2 * hd, total), BF),
            sds((heads_here * hd, total), BF),
            sds((heads_here, 1, total), F32),
            sds((heads_here * hd, total), F32),
            sds((ring, pack_rows, width), BF),
            sds((ring, 8, pack_rows + bu.shape[0]), F32),
            sds((ring,) + wo.shape, BF),
            sds((ring,) + wu.shape, BF),
            sds((ring,) + wd.shape, BF),
        ),
        in_specs=[SM] + [VM] * 10 + [ANY] * 3,
        out_specs=[VM] * 8 + [ANY] * 3,
        scratch_shapes=[
            pltpu.VMEM((ring, heads_here, 2 * hd, count), BF),
            pltpu.VMEM((ring, piece, count), BF),
            pltpu.VMEM((heads_here * hd, total), BF),
            pltpu.VMEM((total, hd), BF),
            dma((5, 5, 3)),
            dma((5, 5, 3)),
            dma((others,)),
            dma((others,)),
            dma((ring, heads_here)),
            dma((heads_here, others)),
            dma((len(FRESH),)),
            dma((len(FRESH), others)),
            dma((1,)),
            dma((1,)),
            dma((heads_here, others)),
            dma((heads_here, others)),
        ],
        compiler_params=pltpu.CompilerParams(
            collective_id=0, has_side_effects=True, vmem_limit_bytes=VMEM_LIMIT
        ),
        name="forward",
    )(length, hidden, gain, shift, wq, wk, wv, bq, bv, bu, first_t, wo, wu, wd)


def backward_kernel(
    ring,
    heads_here,
    planes,
    length_ref,
    context_ref,
    hidden_ref,
    grad_out_ref,
    pre_gain_ref,
    b_out_ref,
    mid_gain_ref,
    mid_shift_ref,
    b_down_ref,
    bias_ref,
    qk_hbm,
    v_hbm,
    lse_hbm,
    exact_hbm,
    normed_hbm,
    wt_hbm,
    wo_hbm,
    wo_far_hbm,
    wu_hbm,
    wu_far_hbm,
    wd_hbm,
    wd_far_hbm,
    layer_ref,
    grad_in_ref,
    first_ref,
    wq_sum,
    wk_sum,
    wv_sum,
    wo_sum,
    wu_sum,
    wd_sum,
    vector_sum,
    qk_ref,
    v_ref,
    lse_ref,
    exact_ref,
    wt_all,
    wo_all,
    wu_all,
    wd_all,
    middle_ref,
    mid_ref,
    mid_t,
    down_ref,
    attn_ref,
    act_ref,
    gup_ref,
    g_ref,
    pack_held,
    wo_share,
    g_all,
    keys,
    vals,
    delta,
    dq,
    grad_ref,
    vector_held,
    vector_came,
    lsem,
    gsend,
    grecv,
    qsend,
    qrecv,
    vsend,
    vrecv,
    fsend,
    frecv,
    rsend,
    rrecv,
    wsend,
    wrecv,
    *bufs,
):
    place = Place(ring, planes)
    m = place.m
    count, width = hidden_ref.shape
    total = ring * count
    half = total // 2
    hd = HEAD_DIM
    piece = first_ref.shape[0]
    out_rows = wo_hbm.shape[0]
    pack_lanes = grad_ref.shape[1]
    tile = count // 4
    own = lanes(m * count, count)

    def shard_of(j):
        return lax.rem(m - j + ring, ring)

    loads = {}

    def load(name, src, dst):
        loads[name] = pltpu.make_async_copy(src, dst, lsem.at[len(loads)])
        loads[name].start()

    for j in range(ring):
        into = wo_all.at[rows_of(shard_of(j) * out_rows, out_rows, 16)]
        load(("wo", j), wo_hbm if j == 0 else wo_far_hbm.at[shard_of(j)], into)
    for j in range(ring):
        s = shard_of(j)
        load(("wu", j), wu_hbm if j == 0 else wu_far_hbm.at[s], wu_all.at[s])
        load(("wd", j), wd_hbm if j == 0 else wd_far_hbm.at[s], wd_all.at[s])
    load("v", v_hbm, v_ref)
    load("qk", qk_hbm, qk_ref)
    load("lse", lse_hbm, lse_ref)
    load("exact", exact_hbm, exact_ref)
    load("wt", wt_hbm, wt_all)
    place.barrier()

    b_out, mid_gain, mid_shift = flat(b_out_ref), flat(mid_gain_ref), flat(mid_shift_ref)
    b_down, pre_gain = flat(b_down_ref), flat(pre_gain_ref)
    act_ref[0] = jnp.transpose(context_ref[...])
    vector_held[0] = jnp.zeros_like(vector_held[0])
    wo_share[:, out_rows:, :] = jnp.zeros_like(wo_share[:, out_rows:, :])
    grad_ref[:, 2 * hd * heads_here + piece :, :] = jnp.zeros_like(
        grad_ref[:, 2 * hd * heads_here + piece :, :]
    )
    for j in range(ring):
        loads[("wo", j)].wait()

    def project(i, carry):
        here = rows_of(i * tile, tile, tile)
        attended = dot(act_ref[0, here, :], wo_all[...], 1, 0) + b_out
        middle = hidden_ref[here, :] + attended
        middle_ref[here, :] = middle
        layer_ref[here, :] = middle + b_down
        mid_ref[here, :] = layer_norm(middle, mid_gain, mid_shift).astype(BF)
        grad_down = grad_out_ref[here, :].astype(BF)
        down_ref[here, :] = grad_down
        grad_in_ref[here, :] = jnp.zeros((tile, width), F32)
        return carry + jnp.sum(grad_down.astype(F32), 0, keepdims=True)

    zero_row = jnp.zeros((1, width), F32)
    grad_b_down = lax.fori_loop(0, count // tile, project, zero_row)
    mid_t[...] = jnp.transpose(mid_ref[...])

    half_width = width // 2

    def half_of(share, total_ref, at, part, x_first):
        window = pl.ds(part * half_width, half_width)
        here = bufs[5 * at : 5 * at + 5]
        return Reduce(
            place, share, here, total_ref.at[window], rsend, rrecv, at, x_first, part * half_width
        )

    early = (half_of(wd_all, wd_sum, 0, 0, False), half_of(wu_all, wu_sum, 1, 0, True))
    late = (half_of(wd_all, wd_sum, 2, 1, False), half_of(wu_all, wu_sum, 3, 1, True))
    out = Reduce(place, wo_share, bufs[20:25], wo_sum, rsend, rrecv, 4, True)
    group = 2 * hd
    packs = [
        Reduce(
            place,
            wu_all,
            bufs[25 + 5 * i : 30 + 5 * i],
            pack_held.at[pl.ds(group * i, group)],
            rsend,
            rrecv,
            5 + i,
            i % 2 == 0,
            group * i,
        )
        for i in range(heads_here + 1)
    ]

    big = count // 2

    def feed_shard(j, carry):
        s = shard_of(j)
        for i, hbm, ref in ((0, wu_hbm, wu_all), (1, wd_hbm, wd_all)):
            pltpu.make_async_copy(hbm, ref.at[s], lsem.at[ring + 2 * j + i]).wait()
        b_up = bias_ref[s, 0:1, pack_lanes:]

        def feed(i, carry):
            here = rows_of(i * big, big, big)
            u = dot(mid_ref[here, :], wu_all[s], 1, 0) + b_up
            grad_act = dot(down_ref[here, :], wd_all[s], 1, 1)
            square = u * u
            t = jnp.tanh(0.7978845608028654 * (u + 0.044715 * u * square))
            act = (0.5 * u * (1.0 + t)).astype(BF)
            slope = 0.5 * (1.0 + t) + (0.5 * 0.7978845608028654) * u * (1.0 - t * t) * (
                1.0 + 0.134145 * square
            )
            grad_up = (grad_act * slope).astype(BF)
            act_ref[s, here, :] = act
            gup_ref[s, here, :] = grad_up
            layer_ref[here, :] += dot(act, wd_all[s], 1, 0)
            grad_in_ref[here, :] += dot(grad_up, wu_all[s], 1, 1)
            return carry + jnp.sum(grad_up.astype(F32), 0, keepdims=True)

        grad_b_up = lax.fori_loop(0, count // big, feed, jnp.zeros((1, wu_all.shape[2]), F32))
        vector_held[0, pl.ds(s, 1), pack_lanes:] = grad_b_up
        return carry

    lax.fori_loop(0, ring, feed_shard, 0)
    load("normed", normed_hbm, mid_ref)

    def middle_back(i, carry):
        here = rows_of(i * tile, tile, tile)
        middle = middle_ref[here, :]
        center = middle - jnp.mean(middle, -1, keepdims=True)
        scale = lax.rsqrt(jnp.mean(center * center, -1, keepdims=True) + EPSILON)
        unit = center * scale
        grad = grad_in_ref[here, :]
        grad_unit = grad * mid_gain
        grad_middle = grad_out_ref[here, :] + scale * (
            grad_unit
            - jnp.mean(grad_unit, -1, keepdims=True)
            - unit * jnp.mean(grad_unit * unit, -1, keepdims=True)
        )
        middle_ref[here, :] = grad_middle
        grad_attn = grad_middle.astype(BF)
        attn_ref[here, :] = grad_attn
        sums = (
            jnp.sum(grad_attn.astype(F32), 0, keepdims=True),
            jnp.sum(grad * unit, 0, keepdims=True),
            jnp.sum(grad, 0, keepdims=True),
        )
        return tuple(x + y for x, y in zip(carry, sums))

    sums = lax.fori_loop(0, count // tile, middle_back, (zero_row,) * 3)
    for i, value in enumerate(sums + (grad_b_down,)):
        vector_held[0, ring + 2 + i : ring + 3 + i, 0:width] = value
    for i in range(ring):
        here = slice(i * out_rows, (i + 1) * out_rows)
        g_ref[here, :] = dot(wo_all[here, :], attn_ref[...], 1, 1).astype(BF)

    def g_copy(slot, to):
        return remote(
            g_ref.at[pl.ds(HEADS_AT[to][slot] * hd, hd)],
            g_all.at[slot, :, own],
            gsend.at[slot, to],
            grecv.at[slot, place.shift_to(to) - 1],
            (place.d, to),
        )

    for slot in range(heads_here):
        for to in range(ring):

            @pl.when(m == to)
            def _(slot=slot, to=to):
                row = HEADS_AT[to][slot] * hd
                g_all[slot, :, own] = g_ref[row : row + hd, :]

            @pl.when(m != to)
            def _(slot=slot, to=to):
                g_copy(slot, to).start()

    for j in range(ring):
        here = rows_of(shard_of(j) * out_rows, out_rows, 16)
        wo_share[shard_of(j), 0:out_rows, :] = dot(
            context_ref[here, :], attn_ref[...], 1, 0
        ).astype(BF)
        out.copy(0, shard_of(j)).start()

    def weigh_shard(j, carry):
        s = shard_of(j)

        def weigh(i, carry):
            here = lanes(i * 256, 256)
            wu_all[s, :, here] = dot(mid_t[...], gup_ref[s, :, here], 1, 0).astype(BF)
            rows = rows_of(i * 256, 256, 256)
            wd_all[s, rows, :] = dot(act_ref[s, :, here], down_ref[...], 0, 0).astype(BF)
            return carry

        lax.fori_loop(0, wu_all.shape[2] // 256, weigh, 0)
        for item in early + late:
            item.copy(0, s).start()

        @pl.when(j > 0)
        def _():
            for item in early:
                item.fold_one(0, shard_of(j - 1))

        return carry

    lax.fori_loop(0, ring, weigh_shard, 0)
    for item in early:
        item.fold_one(0, shard_of(ring - 1))

    def fold_late(j, carry):
        for item in late:
            item.fold_one(0, shard_of(j))
        return carry

    lax.fori_loop(0, ring, fold_late, 0)
    out.fold(0)
    for name in ("v", "qk", "lse", "exact"):
        loads[name].wait()

    def qk_copy(h, j):
        return remote(
            qk_ref.at[h, :, lanes(place.z(j) * count, count)],
            grad_ref.at[place.shard(h), rows_of(2 * hd * h, 2 * hd, 2 * hd)],
            qsend.at[h, j - 1],
            qrecv.at[h, j - 1],
            place.to_z(j),
        )

    v_row = 2 * hd * heads_here

    def v_copy(i, j):
        shard, row, rows, _, row_there = FRESH[i]
        return remote(
            v_ref.at[pl.ds(row_there, rows), lanes(place.z(j) * count, count)],
            grad_ref.at[shard, pl.ds(v_row + row, rows)],
            vsend.at[i, j - 1],
            vrecv.at[i, j - 1],
            place.to_z(j),
        )

    def moved_copy(i):
        to, row, rows, _, row_there = MOVED[i]
        return remote(
            v_ref.at[pl.ds(row_there, rows)],
            first_ref.at[pl.ds(row, rows)],
            fsend.at[0],
            frecv.at[0],
            (place.d, to),
        )

    def send_fresh(slot):
        for i, (shard, row, rows, at, row_there) in enumerate(FRESH):
            if (row_there + rows > 2 * hd) != (slot == 2):
                continue

            @pl.when(m == at)
            def _(i=i, shard=shard, row=row, rows=rows, row_there=row_there):
                for j in range(1, ring):
                    v_copy(i, j).start()
                grad_ref[shard, v_row + row : v_row + row + rows, :] = v_ref[
                    pl.ds(row_there, rows), own
                ]

    def send_reused():
        for i, move in enumerate(MOVED):

            @pl.when(m == move[3])
            def _(i=i):
                moved_copy(i).start()

        for at, row, rows, row_there in KEPT:

            @pl.when(m == at)
            def _(row=row, rows=rows, row_there=row_there):
                first_ref[row : row + rows, :] = v_ref[row_there : row_there + rows, :]

    ones = jnp.ones((8, count), BF)

    def process(i):
        if i == 0:
            for name in ("normed", "wt"):
                loads[name].wait()
            for k in range(ring):
                early[1].copy(0, k).wait_send()
                late[1].copy(0, k).wait_send()
        if i < heads_here:
            for j in range(1, ring):
                qk_copy(i, j).wait_recv()
        begin = group * i
        here = slice(begin, begin + group)
        for k in range(ring):
            wu_all[k, here, :] = dot(grad_ref[k, here, :], mid_ref[...], 1, 0).astype(BF)
            packs[i].copy(0, k).start()
        for k in range(ring):
            sums = dot(ones, grad_ref[k, here, :], 1, 1)
            vector_held[0, k : k + 1, here] = sums[0:1]
        weights = jnp.concatenate([wt_all[k, here, :] for k in range(ring)], 0)

        def add(t, carry):
            toks = lanes(t * tile, tile)
            grads = jnp.concatenate([grad_ref[k, here, toks] for k in range(ring)], 0)
            part = dot(grads, weights, 0, 0)
            rows = rows_of(t * tile, tile, tile)
            grad_in_ref[rows, :] = part if i == 0 else grad_in_ref[rows, :] + part
            return carry

        lax.fori_loop(0, count // tile, add, 0)

    boundary = length_ref[0]
    block = count
    def attend_back(h, carry):
        here_h = rows_of(hd * h, hd, hd)
        keys[...] = jnp.transpose(qk_ref[h, hd : 2 * hd, :])
        vals[...] = jnp.transpose(v_ref[here_h, :])
        for j in range(1, ring):
            remote(
                g_ref.at[pl.ds(0, hd)],
                g_all.at[h, :, own],
                gsend.at[h, 0],
                grecv.at[h, j - 1],
                place.to_z(j),
            ).wait_recv()
        delta[...] = jnp.sum(
            g_all[h].astype(F32) * exact_ref[here_h, :], 0, keepdims=True
        )
        for ki in range(ring):
            key_start = ki * block
            key_rows = keys[key_start : key_start + block, :]
            val_rows = vals[key_start : key_start + block, :]
            key_t = qk_ref[h, hd : 2 * hd, key_start : key_start + block]
            grad_k = None
            for qi in range(ki, ring):
                query_start = qi * block
                here = slice(query_start, query_start + block)
                q = qk_ref[h, 0:hd, here]
                g = g_all[h, :, here]
                scores = dot(key_rows, q, 1, 0) - lse_ref[h, :, here]
                if ki == qi:
                    scores = jnp.where(
                        diagonal_mask(scores, key_start, query_start), scores, NEG_LARGE
                    )
                elif key_start < half <= query_start:
                    scores = scores + other_document(boundary, key_start, query_start)
                p = jnp.exp(scores)
                grad_p = dot(val_rows, g, 1, 0)
                grad_s = (p * (grad_p - delta[:, here])).astype(BF)
                part_v = dot(g, p.astype(BF), 1, 1)
                part_k = dot(q, grad_s, 1, 1)
                if grad_k is None:
                    grad_v, grad_k = part_v, part_k
                else:
                    grad_v, grad_k = grad_v + part_v, grad_k + part_k
                part_q = dot(key_t, grad_s, 1, 0)
                if ki == 0:
                    dq[:, here] = part_q
                else:
                    dq[:, here] += part_q
            qk_ref[h, hd : 2 * hd, key_start : key_start + block] = grad_k.astype(BF)
            v_ref[here_h, key_start : key_start + block] = grad_v.astype(BF)
        qk_ref[h, 0:hd, :] = (dq[...] * (hd**-0.5)).astype(BF)
        for j in range(1, ring):
            qk_copy(h, j).start()
        grad_ref[place.shard(h), rows_of(2 * hd * h, 2 * hd, 2 * hd), :] = qk_ref[h, :, own]

        @pl.when(h == 1)
        def _():
            send_fresh(1)
            for item in early:
                item.fold(1)

        return carry

    lax.fori_loop(0, heads_here, attend_back, 0)
    send_fresh(2)
    send_reused()
    late = late + (out,)
    for item in late:
        item.fold(1)
    process(0)
    process(1)
    for item in early:
        item.fold(2)
    packs[0].fold(0)
    packs[1].fold(0)
    packs[0].fold(1)
    for item in late:
        item.fold(2)
    packs[1].fold(1)
    packs[0].fold(2)
    for to in range(ring):

        @pl.when(m != to)
        def _(to=to):
            for slot in range(heads_here):
                g_copy(slot, to).wait_send()

    for i, (shard, row, rows, at, row_there) in enumerate(FRESH):

        @pl.when(m == at)
        def _(i=i):
            for j in range(1, ring):
                v_copy(i, j).wait_send()

        @pl.when(m != at)
        def _(i=i, shard=shard, row=row, rows=rows, at=at, row_there=row_there):
            shift = lax.rem(m - at + ring, ring)
            remote(
                v_ref.at[pl.ds(row_there, rows), own],
                grad_ref.at[shard, pl.ds(v_row + row, rows)],
                vsend.at[i, shift - 1],
                vrecv.at[i, shift - 1],
                place.to_z(shift),
            ).wait_recv()

    for i, move in enumerate(MOVED):

        @pl.when(m == move[3])
        def _(i=i):
            moved_copy(i).wait_send()

        @pl.when(m == move[0])
        def _(i=i):
            moved_copy(i).wait_recv()

    process(2)
    process(3)

    def input_back(i, carry):
        here = rows_of(i * tile, tile, tile)
        grad = grad_in_ref[here, :]
        value = hidden_ref[here, :]
        center = value - jnp.mean(value, -1, keepdims=True)
        scale = lax.rsqrt(jnp.mean(center * center, -1, keepdims=True) + EPSILON)
        unit = center * scale
        grad_unit = grad * pre_gain
        grad_in_ref[here, :] = middle_ref[here, :] + scale * (
            grad_unit
            - jnp.mean(grad_unit, -1, keepdims=True)
            - unit * jnp.mean(grad_unit * unit, -1, keepdims=True)
        )
        sums = (
            jnp.sum(grad * unit, 0, keepdims=True),
            jnp.sum(grad, 0, keepdims=True),
        )
        return tuple(x + y for x, y in zip(carry, sums))

    sums = lax.fori_loop(0, count // tile, input_back, (zero_row,) * 2)
    for i, value in enumerate(sums):
        vector_held[0, ring + i : ring + 1 + i, 0:width] = value

    turned = jnp.logical_or(m == 1, m == 2)

    def natural(own_row):
        parts = []
        for i in range(heads_here):
            here, turn = group * i, group * ((i - 1) % heads_here)
            parts.append(
                jnp.where(turned, own_row[:, turn : turn + hd], own_row[:, here : here + hd])
            )
        parts.append(jnp.zeros((1, own_row.shape[1] - hd * heads_here), F32))
        return jnp.concatenate(parts, 1)

    routes = [place.to_core, place.to_x, place.to_y]
    routes += [place.to_plane(step) for step in place.steps()]
    bit = 1
    while bit < ring:
        routes.append((place.d, m + bit - 2 * bit * lax.rem(m // bit, 2)))
        bit *= 2

    def vector_copy(k):
        return remote(
            vector_held.at[k], vector_came.at[k], wsend.at[k], wrecv.at[k], routes[k]
        )

    def vector_fold(k):
        vector_copy(k).wait_recv()
        value = vector_held[k] + vector_came[k]
        if k + 1 < len(routes):
            vector_held[k + 1] = value
            vector_copy(k + 1).start()
        else:
            own_row = value[0:1]
            for s in range(1, ring):
                own_row = jnp.where(m == s, value[s : s + 1], own_row)
            vector_sum[...] = jnp.concatenate([value[ring : ring + 6], own_row, natural(own_row)], 0)

    vector_copy(0).start()
    first, second, third, fourth = packs
    for item in early:
        item.fold_pair()
    second.fold(2)
    third.fold(0)
    fourth.fold(0)
    vector_fold(0)
    for item in late:
        item.fold_pair()
    third.fold(1)
    fourth.fold(1)
    vector_fold(1)
    first.fold_pair()
    second.fold_pair()
    for item in early:
        item.finish_sum()
    third.fold(2)
    fourth.fold(2)
    vector_fold(2)
    first.finish_sum()
    second.finish_sum()
    for item in late:
        item.finish_sum()
    third.fold_pair()
    fourth.fold_pair()
    for item in early:
        item.spread(6)
    for k in range(3, len(routes) - 1):
        vector_fold(k)
    first.spread(6)
    second.spread(6)
    third.finish_sum()
    fourth.finish_sum()
    for item in late:
        item.spread(6)
    for item in early:
        item.spread(7)
    vector_fold(len(routes) - 1)
    third.spread(6)
    fourth.spread(6)
    for item in late + (first, second, third, fourth):
        item.spread(7)
    everything = early + late + tuple(packs)
    for item in everything:
        item.wait(7)
        item.drain(1 if item in (early[1], late[1]) else 0)
    for k in range(len(routes)):
        vector_copy(k).wait_send()
    for h in range(heads_here):
        for j in range(1, ring):
            qk_copy(h, j).wait_send()
    for i in range(heads_here):
        at = rows_of(group * jnp.where(turned, (i - 1) % heads_here, i), hd, hd)
        wq_sum[hd * i : hd * i + hd, :] = pack_held[at, :]
        at = rows_of(group * jnp.where(turned, (i - 1) % heads_here, i) + hd, hd, hd)
        wk_sum[hd * i : hd * i + hd, :] = pack_held[at, :]
    wv_sum[...] = pack_held[v_row : v_row + piece, :]


def backward_call(
    ring, heads_here, planes, length, context, hidden, grad_out, pre_gain, b_out, mid_gain, mid_shift,
    b_down, bias,
    qk, v, lse, exact, normed, wt, wo, wo_far, wu, wu_far, wd, wd_far, piece,
):
    count, width = hidden.shape
    total = ring * count
    hd = HEAD_DIM
    others = ring - 1
    sds = jax.ShapeDtypeStruct
    dma = pltpu.SemaphoreType.DMA
    hops = 3 + (planes.bit_length() - 1) + (ring.bit_length() - 1)
    stages = 8 + planes.bit_length() - 1
    pack_rows = wt.shape[1]
    out_pad = wo.shape[0] + -wo.shape[0] % (16 * PLANE)
    sizes = [wd.shape[0] // 2, wu.shape[0] // 2] * 2 + [out_pad] + [2 * hd] * (heads_here + 1)
    bufs = [buf for rows_ in sizes for buf in Reduce.buffers(rows_, width, planes)]
    vector = (ring + 6 + -(ring + 6) % 8, bias.shape[2])
    vm = pltpu.VMEM
    return pl.pallas_call(
        functools.partial(backward_kernel, ring, heads_here, planes),
        out_shape=(
            sds(hidden.shape, F32),
            sds(hidden.shape, F32),
            sds((piece, total), BF),
            sds((heads_here * hd, width), BF),
            sds((heads_here * hd, width), BF),
            sds((piece, width), BF),
            sds((out_pad, width), BF),
            sds(wu.shape, BF),
            sds(wd.shape, BF),
            sds((8, vector[1]), F32),
        ),
        in_specs=[SM] + [VM] * 9 + [ANY] * 12,
        out_specs=[VM] * 10,
        scratch_shapes=[
            vm(qk.shape, BF),
            vm(v.shape, BF),
            vm(lse.shape, F32),
            vm(exact.shape, F32),
            vm(wt.shape, BF),
            vm((ring * wo.shape[0], width), BF),
            vm((ring,) + wu.shape, BF),
            vm((ring,) + wd.shape, BF),
            vm((count, width), F32),
            vm((count, width), BF),
            vm((width, count), BF),
            vm((count, width), BF),
            vm((count, width), BF),
            vm((ring, count, width), BF),
            vm((ring, count, width), BF),
            vm((width, count), BF),
            vm((pack_rows, width), BF),
            vm((ring, out_pad, width), BF),
            vm((heads_here, hd, total), BF),
            vm((total, hd), BF),
            vm((total, hd), BF),
            vm((1, total), F32),
            vm((hd, total), F32),
            vm((ring, pack_rows, count), BF),
            vm((hops,) + vector, F32),
            vm((hops,) + vector, F32),
            dma((3 * ring + 6,)),
            dma((heads_here, ring)),
            dma((heads_here, others)),
            dma((heads_here, others)),
            dma((heads_here, others)),
            dma((len(FRESH), others)),
            dma((len(FRESH), others)),
            dma((1,)),
            dma((1,)),
            dma((5 + heads_here + 1, stages, ring)),
            dma((5 + heads_here + 1, stages, ring)),
            dma((hops,)),
            dma((hops,)),
        ]
        + bufs,
        compiler_params=pltpu.CompilerParams(
            collective_id=1, has_side_effects=True, vmem_limit_bytes=67043328
        ),
        name="backward",
    )(
        length, context, hidden, grad_out, pre_gain, b_out, mid_gain, mid_shift, b_down, bias, qk, v, lse, exact,
        normed, wt, wo, wo_far, wu, wu_far, wd, wd_far,
    )


def shards(
    hidden_in,
    first_values,
    first_length,
    pre_gain,
    pre_shift,
    w_query,
    b_query,
    w_key,
    w_value,
    b_value,
    w_out,
    b_out,
    mid_gain,
    mid_shift,
    w_up,
    b_up,
    w_down,
    b_down,
    grad_out,
):
    ring = lax.axis_size("mp")
    m = lax.axis_index("mp")
    hd = HEAD_DIM
    count, width = hidden_in.shape
    head_width = w_query.shape[1]
    heads_here = head_width // hd
    piece = w_value.shape[1]
    context_t, normed, qk, v, lse, exact, wt_all, bias_all, wo_far, wu_far, wd_far = forward_call(
        ring,
        heads_here,
        first_length,
        hidden_in,
        pre_gain,
        pre_shift,
        w_query.T,
        w_key.T,
        w_value.T,
        b_query,
        b_value,
        b_up,
        first_values.T,
        w_out,
        w_up,
        w_down,
    )
    layer_out, grad_input, grad_first, wq_sum, wk_sum, wv_sum, wo_sum, wu_sum, wd_sum, vector = backward_call(
        ring,
        heads_here,
        lax.axis_size("dp") // PLANE,
        first_length,
        context_t,
        hidden_in,
        grad_out,
        pre_gain,
        b_out,
        mid_gain,
        mid_shift,
        b_down,
        bias_all,
        qk,
        v,
        lse,
        exact,
        normed,
        wt_all,
        w_out,
        wo_far,
        w_up,
        wu_far,
        w_down,
        wd_far,
        piece,
    )
    pack_rows = wt_all.shape[1]
    rows = [vector[i, :width] for i in range(6)]
    return (
        layer_out,
        grad_input,
        grad_first.astype(F32).T,
        rows[0],
        rows[1],
        wq_sum.astype(F32).T,
        vector[7, :head_width],
        wk_sum.astype(F32).T,
        wv_sum.astype(F32).T,
        vector[6, 2 * head_width : 2 * head_width + piece],
        wo_sum[:head_width].astype(F32),
        rows[2],
        rows[3],
        rows[4],
        wu_sum.astype(F32),
        vector[6, pack_rows:],
        wd_sum.astype(F32),
        rows[5],
    )


def solution(mesh):
    rows, cols = P(("dp", "mp"), None), P(None, "mp")
    return jax.shard_map(
        shards,
        mesh=mesh,
        in_specs=(
            rows,
            P("dp", "mp"),
            P("dp"),
            P(),
            P(),
            cols,
            P("mp"),
            cols,
            cols,
            P("mp"),
            P("mp", None),
            P(),
            P(),
            P(),
            cols,
            P("mp"),
            P("mp", None),
            P(),
            rows,
        ),
        out_specs=(
            rows,
            rows,
            P("dp", "mp"),
            P(),
            P(),
            cols,
            P("mp"),
            cols,
            cols,
            P("mp"),
            P("mp", None),
            P(),
            P(),
            P(),
            cols,
            P("mp"),
            P("mp", None),
            P(),
        ),
        check_vma=False,
    )
```

```python
import functools

import jax
import jax.numpy as jnp
from jax import lax
from jax.experimental import pallas as pl
from jax.experimental.pallas import tpu as pltpu
from jax.sharding import PartitionSpec as P

HEAD_DIM = 64
EPSILON = 1e-05
NEG_LARGE = -1e30
MESH = pl.DeviceIdType.MESH
BF = jnp.bfloat16
F32 = jnp.float32
ANY = pl.BlockSpec(memory_space=pl.ANY)
VM = pl.BlockSpec(memory_space=pltpu.VMEM)
SM = pl.BlockSpec(memory_space=pltpu.SMEM)
VMEM_LIMIT = 60 << 20
LANE = 128
PLANE = 8
RING = 4
HEADS_AT = ((0, 1, 6), (7, 8, 2), (9, 10, 3), (4, 5, 11))
FRESH = (
    (0, 0, 96, 0, 0),
    (1, 0, 32, 0, 96),
    (1, 32, 64, 1, 128),
    (2, 0, 64, 2, 128),
    (2, 64, 32, 3, 0),
    (3, 0, 96, 3, 32),
)
KEPT = ((0, 0, 64, 128), (1, 0, 96, 32), (2, 0, 96, 0), (3, 32, 64, 128))
MOVED = ((0, 64, 32, 1, 0), (3, 0, 32, 2, 96))


def dot(left, right, left_dim, right_dim):
    return lax.dot_general(
        left, right, (((left_dim,), (right_dim,)), ((), ())), preferred_element_type=F32
    )


def layer_norm(values, gain, shift):
    center = values - jnp.mean(values, -1, keepdims=True)
    spread = jnp.mean(center * center, -1, keepdims=True)
    return center * lax.rsqrt(spread + EPSILON) * gain + shift


def gelu_tanh(values):
    return (
        0.5
        * values
        * (1.0 + jnp.tanh(0.7978845608028654 * (values + 0.044715 * values * values * values)))
    )


def lanes(start, size):
    return pl.ds(pl.multiple_of(start, LANE), size)


def rows_of(start, size, unit):
    return pl.ds(pl.multiple_of(start, unit), size)


def flat(ref):
    return jnp.reshape(ref[...], (1, ref.shape[0]))


class Place:
    def __init__(self, ring, planes=1):
        self.ring = ring
        self.planes = planes
        self.d = lax.axis_index("dp")
        self.m = lax.axis_index("mp")
        d = self.d
        self.core = lax.rem(d, 2)
        self.x = lax.rem(d // 2, 2)
        self.y = lax.rem(d // 4, 2)
        self.to_core = (d + 1 - 2 * self.core, self.m)
        self.to_x = (d + 2 - 4 * self.x, self.m)
        self.to_y = (d + 4 - 8 * self.y, self.m)
        self.pair = self.m + 1 - 2 * lax.rem(self.m, 2)
        self.across = lax.rem(self.m + 2, RING)
        self.corner = RING - 1 - self.m

    def z(self, shift):
        return lax.rem(self.m + shift, self.ring)

    def to_z(self, shift):
        return (self.d, self.z(shift))

    def shift_to(self, position):
        return lax.rem(position - self.m + self.ring, self.ring)

    def head(self, slot):
        value = 0
        for k, heads in enumerate(HEADS_AT):
            for at, head in enumerate(heads):
                value = jnp.where(jnp.logical_and(self.m == k, slot == at), head, value)
        return value

    def shard(self, slot):
        return self.head(slot) // len(HEADS_AT[0])

    def steps(self):
        return [PLANE << b for b in range(self.planes.bit_length() - 1)]

    def to_plane(self, step):
        return (self.d + step - 2 * step * lax.rem(self.d // step, 2), self.m)

    def barrier(self):
        sem = pltpu.get_barrier_semaphore()
        peers = [self.to_z(j) for j in range(1, self.ring)]
        peers += [self.to_core, self.to_x, self.to_y]
        peers += [self.to_plane(step) for step in self.steps()]
        for peer in peers:
            pl.semaphore_signal(sem, inc=1, device_id=peer, device_id_type=MESH)
        pl.semaphore_wait(sem, len(peers))

    def slot(self, x_first):
        if x_first:
            return self.core * 4 + self.y * 2 + self.x
        return self.core * 4 + self.x * 2 + self.y


def remote(src, dst, send, recv, device):
    return pltpu.make_async_remote_copy(
        src_ref=src,
        dst_ref=dst,
        send_sem=send,
        recv_sem=recv,
        device_id=device,
        device_id_type=MESH,
    )


class Gather:
    def __init__(self, place, src, dst, send, recv, item, first_row, rows, x_first):
        self.place, self.src, self.dst = place, src, dst
        self.send, self.recv, self.item = send, recv, item
        self.first_row, self.part, self.x_first = first_row, rows // PLANE, x_first

    def window(self, start, size):
        part = self.part
        return rows_of(self.first_row + start * part, size * part, part & -part)

    def copy(self, stage, k):
        place = self.place
        slot = place.slot(self.x_first)
        near, far = (place.to_x, place.to_y) if self.x_first else (place.to_y, place.to_x)
        shard = (place.across, place.pair, place.corner)[k]
        window = self.window(slot, 1)
        if stage == 0:
            shard, target = place.m, (place.d, place.across)
        elif stage == 1:
            shard, target = (place.m, place.across)[k], (place.d, place.pair)
        elif stage == 2:
            target = near
        elif stage == 3:
            window, target = self.window((slot // 2) * 2, 2), far
        else:
            window, target = self.window(place.core * 4, 4), place.to_core
        own = stage == 0 or (stage == 1 and k == 0)
        source = self.src.at[window] if own else self.dst.at[shard, window]
        return remote(
            source,
            self.dst.at[shard, window],
            self.send.at[self.item, stage, k],
            self.recv.at[self.item, stage, k],
            target,
        )

    def start(self, stage):
        if stage == 0:
            self.copy(0, 0).start()
            self.copy(1, 0).start()
        elif stage == 1:
            self.copy(0, 0).wait_recv()
            self.copy(1, 1).start()
            self.copy(2, 0).start()
        elif stage == 2:
            for k in range(2):
                self.copy(1, k).wait_recv()
                self.copy(2, k + 1).start()
        else:
            for k in range(3):
                self.copy(stage - 1, k).wait_recv()
                self.copy(stage, k).start()

    def arrive(self):
        for k in range(3):
            self.copy(4, k).wait_recv()

    def drain(self):
        for stage, copies in enumerate((1, 2, 3, 3, 3)):
            for k in range(copies):
                self.copy(stage, k).wait_send()


class Reduce:
    def __init__(self, place, src, bufs, out, send, recv, item, x_first, first_row=0):
        self.place, self.src, self.out = place, src, out
        self.first_row = first_row
        self.r_core, self.r_far, self.r_near, self.r_z, self.r_plane = bufs
        self.send, self.recv, self.item, self.x_first = send, recv, item, x_first
        self.part = out.shape[0] // PLANE
        if x_first:
            self.near, self.far = place.to_x, place.to_y
            self.near_bit, self.far_bit = place.x, place.y
        else:
            self.near, self.far = place.to_y, place.to_x
            self.near_bit, self.far_bit = place.y, place.x

    def rows(self, start, size):
        return rows_of(start * self.part, size * self.part, self.part & -self.part)

    def copy(self, stage, k):
        place = self.place
        if stage == 0:
            begin = self.first_row + (1 - place.core) * 4 * self.part
            src = self.src.at[k, rows_of(begin, 4 * self.part, self.part & -self.part)]
            dst, target = self.r_core.at[k], place.to_core
        elif stage == 1:
            src = self.r_core.at[k, self.rows((1 - self.far_bit) * 2, 2)]
            dst, target = self.r_far.at[k], self.far
        elif stage == 2:
            src = self.r_far.at[k, self.rows(1 - self.near_bit, 1)]
            dst, target = self.r_near.at[k], self.near
        elif stage == 3:
            src = self.r_near.at[(place.pair, place.corner)[k]]
            dst, target = self.r_z.at[k], (place.d, place.pair)
        elif stage == 4:
            src = self.r_near.at[place.across]
            dst, target = self.r_z.at[2], (place.d, place.across)
        else:
            slot = place.slot(self.x_first)
            if stage == 5:
                window, target = self.rows(slot, 1), self.near
            elif stage == 6:
                window, target = self.rows((slot // 2) * 2, 2), self.far
            else:
                window, target = self.rows(place.core * 4, 4), place.to_core
            src = dst = self.out.at[window]
        return remote(
            src, dst, self.send.at[self.item, stage, k], self.recv.at[self.item, stage, k], target
        )

    def members(self, stage):
        return range((RING, RING, RING, 2, 1, 1, 1, 1)[stage])

    def start(self, stage):
        for k in self.members(stage):
            self.copy(stage, k).start()

    def wait(self, stage):
        for k in self.members(stage):
            self.copy(stage, k).wait_recv()

    def fold_one(self, stage, k):
        place, part = self.place, self.part
        if stage == 0:
            base = self.first_row + place.core * 4 * part
            kept, into, size = self.src, self.r_core, 4 * part
        elif stage == 1:
            kept, base, into, size = self.r_core, self.far_bit * 2 * part, self.r_far, 2 * part
        else:
            kept, base, into, size = self.r_far, self.near_bit * part, self.r_near, part
        unit = part & -part
        step = min(unit, 32)
        self.copy(stage, k).wait_recv()

        def add(i, carry):
            mine = kept[k, rows_of(base + i * step, step, min(unit, step)), :].astype(F32)
            here = rows_of(i * step, step, step)
            into[k, here, :] = (into[k, here, :].astype(F32) + mine).astype(BF)
            return carry

        lax.fori_loop(0, size // step, add, 0)
        if stage < 2:
            self.copy(stage + 1, k).start()

    def fold(self, stage):
        for k in self.members(stage):
            self.fold_one(stage, k)
        if stage == 2:
            self.start(3)

    def fold_pair(self):
        place = self.place
        self.wait(3)
        other = self.r_near[place.across].astype(F32) + self.r_z[1].astype(F32)
        self.r_near[place.across] = other.astype(BF)
        self.start(4)
        mine = self.r_near[place.m].astype(F32) + self.r_z[0].astype(F32)
        self.r_near[place.m] = mine.astype(BF)

    def finish_sum(self):
        place = self.place
        self.wait(4)
        here = self.rows(place.slot(self.x_first), 1)
        value = self.r_near[place.m].astype(F32) + self.r_z[2].astype(F32)
        self.out[here, :] = value.astype(BF)
        for b, step in enumerate(place.steps()):
            copy = remote(
                self.out.at[here],
                self.r_plane.at[b],
                self.send.at[self.item, 8 + b, 0],
                self.recv.at[self.item, 8 + b, 0],
                place.to_plane(step),
            )
            copy.start()
            copy.wait()
            mine = self.out[here, :].astype(F32)
            self.out[here, :] = (mine + self.r_plane[b].astype(F32)).astype(BF)
        self.start(5)

    def spread(self, stage):
        self.wait(stage - 1)
        self.start(stage)

    def drain(self, first):
        for stage in range(first, 8):
            for k in self.members(stage):
                self.copy(stage, k).wait_send()

    @staticmethod
    def buffers(rows, width, planes):
        part = rows // PLANE
        extra = max(planes.bit_length() - 1, 1)
        return [
            pltpu.VMEM((RING, 4 * part, width), BF),
            pltpu.VMEM((RING, 2 * part, width), BF),
            pltpu.VMEM((RING, part, width), BF),
            pltpu.VMEM((3, part, width), BF),
            pltpu.VMEM((extra, part, width), BF),
        ]


def diagonal_mask(scores, key_start, query_start):
    keys = lax.broadcasted_iota(jnp.int32, scores.shape, 0) + key_start
    queries = lax.broadcasted_iota(jnp.int32, scores.shape, 1) + query_start
    return keys <= queries


def other_document(boundary, key_start, query_start):
    crossing = jnp.logical_and(boundary > key_start, boundary <= query_start)
    return jnp.where(crossing, NEG_LARGE, 0.0)


def forward_kernel(
    ring,
    heads_here,
    length_ref,
    hidden_ref,
    gain_ref,
    shift_ref,
    wq_ref,
    wk_ref,
    wv_ref,
    bq_ref,
    bv_ref,
    bu_ref,
    first_ref,
    wo_ref,
    wu_ref,
    wd_ref,
    context_ref,
    normed_out,
    qk_out,
    v_out,
    lse_ref,
    exact_out,
    wt_out,
    bias_all,
    wo_far,
    wu_far,
    wd_far,
    normed_ref,
    qk_ref,
    v_ref,
    exact_ref,
    wt_all,
    osem,
    y_send,
    vy_send,
    c_send,
    keys,
    gsend,
    grecv,
    bsend,
    brecv,
    qsend,
    qrecv,
    vsend,
    vrecv,
    fsend,
    frecv,
    csend,
    crecv,
):
    place = Place(ring)

    def keep(i, src, dst):
        return pltpu.make_async_copy(src, dst, osem.at[i])

    m = place.m
    count = hidden_ref.shape[0]
    total = ring * count
    piece = first_ref.shape[0]
    half = total // 2
    hd = HEAD_DIM
    pack_rows = wt_all.shape[1]
    v_row = 2 * hd * heads_here
    turned = jnp.logical_or(m == 1, m == 2)

    def slot_row(slot):
        return rows_of(hd * jnp.where(turned, (slot + 1) % heads_here, slot), hd, hd)

    bq, bv, bu = flat(bq_ref), flat(bv_ref), flat(bu_ref)
    bias_parts = []
    for slot in range(heads_here):
        row = 2 * hd * slot
        wt_all[m, row : row + hd, :] = wq_ref[slot_row(slot), :]
        wt_all[m, row + hd : row + 2 * hd, :] = wk_ref[slot_row(slot), :]
        here, after = hd * slot, hd * ((slot + 1) % heads_here)
        own_bias = jnp.where(turned, bq[:, after : after + hd], bq[:, here : here + hd])
        bias_parts += [own_bias, jnp.zeros_like(own_bias)]
    wt_all[m, v_row : v_row + piece, :] = wv_ref[...]
    spare = pack_rows - v_row - piece
    wt_all[m, v_row + piece :, :] = jnp.zeros((spare, wv_ref.shape[1]), BF)
    bias_parts += [bv, jnp.zeros((1, spare), F32), bu]
    bias_row = jnp.concatenate(bias_parts, 1)
    bias_all[m] = jnp.broadcast_to(bias_row, (8, bias_row.shape[1]))
    wt_ref = wt_all.at[m]
    bias_ref = bias_all.at[m]
    place.barrier()
    half_pack = pack_rows // 2
    small = [
        Gather(place, wt_ref, wt_all, gsend, grecv, i, i * half_pack, half_pack, i == 0)
        for i in range(2)
    ]
    big = [
        Gather(place, wo_ref, wo_far, gsend, grecv, 2, 0, wo_ref.shape[0], True),
        Gather(place, wu_ref, wu_far, gsend, grecv, 3, 0, wu_ref.shape[0], True),
        Gather(place, wd_ref, wd_far, gsend, grecv, 4, 0, wd_ref.shape[0], False),
    ]
    for item in small:
        item.start(0)

    def bias_copy(j):
        return remote(
            bias_ref, bias_all.at[m], bsend.at[j - 1], brecv.at[j - 1], place.to_z(j)
        )

    for j in range(1, ring):
        bias_copy(j).start()

    def moved_copy(i):
        _, row, rows, to, row_there = MOVED[i]
        return remote(
            first_ref.at[pl.ds(row, rows)],
            v_ref.at[pl.ds(row_there, rows)],
            fsend.at[0],
            frecv.at[0],
            (place.d, to),
        )

    for i, move in enumerate(MOVED):

        @pl.when(m == move[0])
        def _(i=i):
            moved_copy(i).start()

    for at, row, rows, row_there in KEPT:

        @pl.when(m == at)
        def _(row=row, rows=rows, row_there=row_there):
            v_ref[row_there : row_there + rows, :] = first_ref[row : row + rows, :]

    normed_ref[...] = layer_norm(hidden_ref[...], flat(gain_ref), flat(shift_ref)).astype(BF)

    for item in small:
        item.start(1)
    for item in big:
        item.start(0)
    for item in small:
        item.start(2)
    for item in big:
        item.start(1)
    for stage in (3, 4):
        for item in small:
            item.start(stage)
    for j in range(1, ring):
        bias_copy(j).wait_recv()
    for item in small:
        item.arrive()

    own = lanes(m * count, count)

    def qk_copy(slot, to):
        return remote(
            y_send.at[to, slot],
            qk_ref.at[slot, :, own],
            qsend.at[to, slot],
            qrecv.at[slot, place.shift_to(to) - 1],
            (place.d, to),
        )

    def v_copy(i):
        shard, row, rows, to, row_there = FRESH[i]
        return remote(
            vy_send.at[shard, pl.ds(row, rows)],
            v_ref.at[pl.ds(row_there, rows), own],
            vsend.at[i],
            vrecv.at[i, place.shift_to(to) - 1],
            (place.d, to),
        )

    where_is = {
        (head // heads_here, slot): to
        for to, heads in enumerate(HEADS_AT)
        for slot, head in enumerate(heads)
    }

    for shard in range(ring):
        out = dot(wt_all[shard], normed_ref[...], 1, 1)
        out = out + jnp.transpose(bias_all[shard, :, 0:pack_rows])[:, 0:1]
        for slot in range(heads_here):
            to = where_is[shard, slot]
            row = 2 * hd * slot
            y_send[to, slot, 0:hd, :] = (out[row : row + hd] * (hd**-0.5)).astype(BF)
            y_send[to, slot, hd : 2 * hd, :] = out[row + hd : row + 2 * hd].astype(BF)
        vy_send[shard] = out[v_row : v_row + piece].astype(BF)

    def share(slot):
        for to in range(ring):

            @pl.when(m == to)
            def _(to=to):
                qk_ref[slot, :, own] = y_send[to, slot]

            @pl.when(m != to)
            def _(to=to):
                qk_copy(slot, to).start()

    share(0)
    for i, (shard, row, rows, to, row_there) in enumerate(FRESH):

        @pl.when(m == to)
        def _(shard=shard, row=row, rows=rows, row_there=row_there):
            v_ref[row_there : row_there + rows, own] = vy_send[shard, row : row + rows, :]

        @pl.when(m != to)
        def _(i=i):
            v_copy(i).start()

    for slot in range(1, heads_here):
        share(slot)
    for stage in (2, 3):
        for item in big:
            item.start(stage)

    def qk_arrive(slot):
        for shift in range(1, ring):
            remote(
                y_send.at[0, slot],
                qk_ref.at[slot, :, own],
                qsend.at[0, slot],
                qrecv.at[slot, shift - 1],
                place.to_z(shift),
            ).wait_recv()

    for i, (shard, row, rows, to, row_there) in enumerate(FRESH):

        @pl.when(m == to)
        def _(i=i, shard=shard, row=row, rows=rows, row_there=row_there):
            for shift in range(1, ring):
                remote(
                    vy_send.at[shard, pl.ds(row, rows)],
                    v_ref.at[pl.ds(row_there, rows), own],
                    vsend.at[i],
                    vrecv.at[i, shift - 1],
                    place.to_z(shift),
                ).wait_recv()

    for i, move in enumerate(MOVED):

        @pl.when(m == move[3])
        def _(i=i):
            moved_copy(i).wait_recv()

    keep(0, normed_ref, normed_out).start()
    keep(1, wt_all, wt_out).start()
    keep(2, v_ref, v_out).start()
    boundary = length_ref[0]
    block = count

    def context_copy(h, to):
        return remote(
            c_send.at[rows_of(hd * h, hd, hd), pl.ds(to * count, count)],
            context_ref.at[rows_of(place.head(h) * hd, hd, hd)],
            csend.at[h, to],
            crecv.at[h, place.shift_to(to) - 1],
            (place.d, to),
        )

    def attend(h, carry):
        qk_arrive(h)
        here_h = rows_of(hd * h, hd, hd)
        keys[...] = jnp.transpose(qk_ref[h, hd : 2 * hd, :])
        for qi in range(ring):
            query_start = qi * block
            queries = slice(query_start, query_start + block)
            q = qk_ref[h, 0:hd, queries]
            top = None
            for ki in range(qi + 1):
                key_start = ki * block
                v = v_ref[here_h, key_start : key_start + block]
                scores = dot(keys[key_start : key_start + block, :], q, 1, 0)
                if ki == qi:
                    scores = jnp.where(
                        diagonal_mask(scores, key_start, query_start), scores, NEG_LARGE
                    )
                elif key_start < half <= query_start:
                    scores = scores + other_document(boundary, key_start, query_start)
                block_top = jnp.max(scores, 0, keepdims=True)
                new_top = block_top if top is None else jnp.maximum(top, block_top)
                p = jnp.exp(scores - new_top)
                p_sum = jnp.sum(p, 0, keepdims=True)
                part = dot(v, p.astype(BF), 1, 0)
                if top is None:
                    run_sum, running = p_sum, part
                else:
                    factor = jnp.exp(top - new_top)
                    run_sum = run_sum * factor + p_sum
                    running = running * factor + part
                top = new_top
            result = running / run_sum
            exact_ref[here_h, queries] = result
            c_send[here_h, queries] = result.astype(BF)
            lse_ref[h, :, queries] = top + jnp.log(run_sum)

            @pl.when(m == qi)
            def _(queries=queries):
                context_ref[rows_of(place.head(h) * hd, hd, hd), :] = c_send[here_h, queries]

            @pl.when(m != qi)
            def _(qi=qi):
                context_copy(h, qi).start()


        keep(3 + h, qk_ref.at[h], qk_out.at[h]).start()
        keep(3 + heads_here + h, exact_ref.at[here_h], exact_out.at[here_h]).start()

        @pl.when(h == 1)
        def _():
            for item in big:
                item.start(4)

        return carry

    lax.fori_loop(0, heads_here, attend, 0)
    for item in big:
        item.arrive()
    for h in range(heads_here):
        for j in range(1, ring):
            remote(
                c_send.at[pl.ds(hd * h, hd), own],
                context_ref.at[pl.ds(0, hd)],
                csend.at[h, 0],
                crecv.at[h, j - 1],
                place.to_z(j),
            ).wait_recv()
    keep(0, normed_ref, normed_out).wait()
    keep(1, wt_all, wt_out).wait()
    keep(2, v_ref, v_out).wait()
    for h in range(heads_here):
        here_h = pl.ds(hd * h, hd)
        keep(3 + h, qk_ref.at[h], qk_out.at[h]).wait()
        keep(3 + heads_here + h, exact_ref.at[here_h], exact_out.at[here_h]).wait()
    for item in small + big:
        item.drain()
    for j in range(1, ring):
        bias_copy(j).wait_send()
    for to in range(ring):

        @pl.when(m != to)
        def _(to=to):
            for slot in range(heads_here):
                qk_copy(slot, to).wait_send()
                context_copy(slot, to).wait_send()

    for i, (shard, row, rows, to, row_there) in enumerate(FRESH):

        @pl.when(m != to)
        def _(i=i):
            v_copy(i).wait_send()

    for i, move in enumerate(MOVED):

        @pl.when(m == move[0])
        def _(i=i):
            moved_copy(i).wait_send()


def forward_call(
    ring, heads_here, length, hidden, gain, shift, wq, wk, wv, bq, bv, bu, first_t, wo, wu, wd
):
    count, width = hidden.shape
    total = ring * count
    hd = HEAD_DIM
    piece = first_t.shape[0]
    others = ring - 1
    pack_rows = 2 * hd * (heads_here + 1)
    sds = jax.ShapeDtypeStruct
    dma = pltpu.SemaphoreType.DMA
    return pl.pallas_call(
        functools.partial(forward_kernel, ring, heads_here),
        out_shape=(
            sds((ring * heads_here * hd, count), BF),
            sds((count, width), BF),
            sds((heads_here, 2 * hd, total), BF),
            sds((heads_here * hd, total), BF),
            sds((heads_here, 1, total), F32),
            sds((heads_here * hd, total), F32),
            sds((ring, pack_rows, width), BF),
            sds((ring, 8, pack_rows + bu.shape[0]), F32),
            sds((ring,) + wo.shape, BF),
            sds((ring,) + wu.shape, BF),
            sds((ring,) + wd.shape, BF),
        ),
        in_specs=[SM] + [VM] * 10 + [ANY] * 3,
        out_specs=[VM] + [ANY] * 3 + [VM] + [ANY] * 2 + [VM] + [ANY] * 3,
        scratch_shapes=[
            pltpu.VMEM((count, width), BF),
            pltpu.VMEM((heads_here, 2 * hd, total), BF),
            pltpu.VMEM((heads_here * hd, total), BF),
            pltpu.VMEM((heads_here * hd, total), F32),
            pltpu.VMEM((ring, pack_rows, width), BF),
            dma((3 + 2 * heads_here,)),
            pltpu.VMEM((ring, heads_here, 2 * hd, count), BF),
            pltpu.VMEM((ring, piece, count), BF),
            pltpu.VMEM((heads_here * hd, total), BF),
            pltpu.VMEM((total, hd), BF),
            dma((5, 5, 3)),
            dma((5, 5, 3)),
            dma((others,)),
            dma((others,)),
            dma((ring, heads_here)),
            dma((heads_here, others)),
            dma((len(FRESH),)),
            dma((len(FRESH), others)),
            dma((1,)),
            dma((1,)),
            dma((heads_here, ring)),
            dma((heads_here, others)),
        ],
        compiler_params=pltpu.CompilerParams(
            collective_id=0, has_side_effects=True, vmem_limit_bytes=VMEM_LIMIT
        ),
        name="forward",
    )(length, hidden, gain, shift, wq, wk, wv, bq, bv, bu, first_t, wo, wu, wd)


def backward_kernel(
    ring,
    heads_here,
    planes,
    length_ref,
    context_ref,
    hidden_ref,
    grad_out_ref,
    pre_gain_ref,
    b_out_ref,
    mid_gain_ref,
    mid_shift_ref,
    b_down_ref,
    bias_ref,
    qk_hbm,
    v_hbm,
    lse_hbm,
    exact_hbm,
    normed_hbm,
    wt_hbm,
    wo_hbm,
    wo_far_hbm,
    wu_hbm,
    wu_far_hbm,
    wd_hbm,
    wd_far_hbm,
    layer_ref,
    grad_in_ref,
    first_ref,
    wq_sum,
    wk_sum,
    wv_sum,
    wo_sum,
    wu_sum,
    wd_sum,
    vector_sum,
    qk_ref,
    v_ref,
    lse_ref,
    exact_ref,
    wt_all,
    wo_all,
    wu_all,
    wd_all,
    middle_ref,
    mid_ref,
    mid_t,
    down_ref,
    down_t,
    act_ref,
    gup_ref,
    g_ref,
    pack_held,
    wo_share,
    g_all,
    keys,
    vals,
    delta,
    dk,
    dv,
    grad_ref,
    vector_held,
    vector_came,
    lsem,
    gsend,
    grecv,
    qsend,
    qrecv,
    vsend,
    vrecv,
    fsend,
    frecv,
    rsend,
    rrecv,
    wsend,
    wrecv,
    *bufs,
):
    place = Place(ring, planes)
    m = place.m
    count, width = hidden_ref.shape
    total = ring * count
    half = total // 2
    hd = HEAD_DIM
    piece = first_ref.shape[0]
    out_rows = wo_hbm.shape[0]
    pack_lanes = grad_ref.shape[1]
    tile = count // 4
    own = lanes(m * count, count)

    def shard_of(j):
        return lax.rem(m - j + ring, ring)

    loads = {}

    def load(name, src, dst):
        loads[name] = pltpu.make_async_copy(src, dst, lsem.at[len(loads)])
        loads[name].start()

    for j in range(ring):
        into = wo_all.at[rows_of(shard_of(j) * out_rows, out_rows, 16)]
        load(("wo", j), wo_hbm if j == 0 else wo_far_hbm.at[shard_of(j)], into)
    for j in range(ring):
        s = shard_of(j)
        load(("wu", j), wu_hbm if j == 0 else wu_far_hbm.at[s], wu_all.at[s])
        load(("wd", j), wd_hbm if j == 0 else wd_far_hbm.at[s], wd_all.at[s])
    load("v", v_hbm, v_ref)
    load("qk", qk_hbm, qk_ref)
    load("lse", lse_hbm, lse_ref)
    load("exact", exact_hbm, exact_ref)
    load("wt", wt_hbm, wt_all)
    place.barrier()

    b_out, mid_gain, mid_shift = flat(b_out_ref), flat(mid_gain_ref), flat(mid_shift_ref)
    b_down, pre_gain = flat(b_down_ref), flat(pre_gain_ref)
    act_ref[0] = jnp.transpose(context_ref[...])
    vector_held[0] = jnp.zeros_like(vector_held[0])
    wo_share[:, out_rows:, :] = jnp.zeros_like(wo_share[:, out_rows:, :])
    grad_ref[:, 2 * hd * heads_here + piece :, :] = jnp.zeros_like(
        grad_ref[:, 2 * hd * heads_here + piece :, :]
    )
    for j in range(ring):
        loads[("wo", j)].wait()

    def project(i, carry):
        here = rows_of(i * tile, tile, tile)
        attended = dot(act_ref[0, here, :], wo_all[...], 1, 0) + b_out
        middle = hidden_ref[here, :] + attended
        middle_ref[here, :] = middle
        layer_ref[here, :] = middle + b_down
        mid_ref[here, :] = layer_norm(middle, mid_gain, mid_shift).astype(BF)
        grad_down = grad_out_ref[here, :].astype(BF)
        down_ref[here, :] = grad_down
        grad_in_ref[here, :] = jnp.zeros((tile, width), F32)
        return carry + jnp.sum(grad_down.astype(F32), 0, keepdims=True)

    zero_row = jnp.zeros((1, width), F32)
    grad_b_down = lax.fori_loop(0, count // tile, project, zero_row)
    mid_t[...] = jnp.transpose(mid_ref[...])
    down_t[...] = jnp.transpose(down_ref[...])

    half_width = width // 2

    def half_of(share, total_ref, at, part, x_first):
        window = pl.ds(part * half_width, half_width)
        here = bufs[5 * at : 5 * at + 5]
        return Reduce(
            place, share, here, total_ref.at[window], rsend, rrecv, at, x_first, part * half_width
        )

    early = (half_of(wd_all, wd_sum, 0, 0, False), half_of(wu_all, wu_sum, 1, 0, True))
    late = (half_of(wd_all, wd_sum, 2, 1, False), half_of(wu_all, wu_sum, 3, 1, True))
    out = Reduce(place, wo_share, bufs[20:25], wo_sum, rsend, rrecv, 4, True)
    group = 2 * hd
    packs = [
        Reduce(
            place,
            wu_all,
            bufs[25 + 5 * i : 30 + 5 * i],
            pack_held.at[pl.ds(group * i, group)],
            rsend,
            rrecv,
            5 + i,
            i % 2 == 0,
            group * i,
        )
        for i in range(heads_here + 1)
    ]

    big = count // 2

    def feed_shard(j, carry):
        s = shard_of(j)
        for i, hbm, ref in ((0, wu_hbm, wu_all), (1, wd_hbm, wd_all)):
            pltpu.make_async_copy(hbm, ref.at[s], lsem.at[ring + 2 * j + i]).wait()
        b_up = bias_ref[s, 0:1, pack_lanes:]

        def feed(i, carry):
            here = rows_of(i * big, big, big)
            u = dot(mid_ref[here, :], wu_all[s], 1, 0) + b_up
            grad_act = dot(down_ref[here, :], wd_all[s], 1, 1)
            square = u * u
            t = jnp.tanh(0.7978845608028654 * (u + 0.044715 * u * square))
            act = (0.5 * u * (1.0 + t)).astype(BF)
            slope = 0.5 * (1.0 + t) + (0.5 * 0.7978845608028654) * u * (1.0 - t * t) * (
                1.0 + 0.134145 * square
            )
            grad_up = (grad_act * slope).astype(BF)
            act_ref[s, here, :] = act
            gup_ref[s, here, :] = grad_up
            layer_ref[here, :] += dot(act, wd_all[s], 1, 0)
            grad_in_ref[here, :] += dot(grad_up, wu_all[s], 1, 1)
            return carry + jnp.sum(grad_up.astype(F32), 0, keepdims=True)

        grad_b_up = lax.fori_loop(0, count // big, feed, jnp.zeros((1, wu_all.shape[2]), F32))
        vector_held[0, pl.ds(s, 1), pack_lanes:] = grad_b_up
        return carry

    lax.fori_loop(0, ring, feed_shard, 0)
    load("normed", normed_hbm, mid_ref)

    def middle_back(i, carry):
        here = rows_of(i * tile, tile, tile)
        middle = middle_ref[here, :]
        center = middle - jnp.mean(middle, -1, keepdims=True)
        scale = lax.rsqrt(jnp.mean(center * center, -1, keepdims=True) + EPSILON)
        unit = center * scale
        grad = grad_in_ref[here, :]
        grad_unit = grad * mid_gain
        grad_middle = grad_out_ref[here, :] + scale * (
            grad_unit
            - jnp.mean(grad_unit, -1, keepdims=True)
            - unit * jnp.mean(grad_unit * unit, -1, keepdims=True)
        )
        middle_ref[here, :] = grad_middle
        grad_attn = grad_middle.astype(BF)
        down_ref[here, :] = grad_attn
        sums = (
            jnp.sum(grad_attn.astype(F32), 0, keepdims=True),
            jnp.sum(grad * unit, 0, keepdims=True),
            jnp.sum(grad, 0, keepdims=True),
        )
        return tuple(x + y for x, y in zip(carry, sums))

    sums = lax.fori_loop(0, count // tile, middle_back, (zero_row,) * 3)
    for i, value in enumerate(sums + (grad_b_down,)):
        vector_held[0, ring + 2 + i : ring + 3 + i, 0:width] = value
    for i in range(ring):
        here = slice(i * out_rows, (i + 1) * out_rows)
        g_ref[here, :] = dot(wo_all[here, :], down_ref[...], 1, 1).astype(BF)

    def g_copy(slot, to):
        return remote(
            g_ref.at[pl.ds(HEADS_AT[to][slot] * hd, hd)],
            g_all.at[slot, :, own],
            gsend.at[slot, to],
            grecv.at[slot, place.shift_to(to) - 1],
            (place.d, to),
        )

    for slot in range(heads_here):
        for to in range(ring):

            @pl.when(m == to)
            def _(slot=slot, to=to):
                row = HEADS_AT[to][slot] * hd
                g_all[slot, :, own] = g_ref[row : row + hd, :]

            @pl.when(m != to)
            def _(slot=slot, to=to):
                g_copy(slot, to).start()

    for j in range(ring):
        here = rows_of(shard_of(j) * out_rows, out_rows, 16)
        wo_share[shard_of(j), 0:out_rows, :] = dot(
            context_ref[here, :], down_ref[...], 1, 0
        ).astype(BF)
        out.copy(0, shard_of(j)).start()

    def weigh_shard(j, carry):
        s = shard_of(j)

        def weigh(i, carry):
            here = lanes(i * 256, 256)
            wu_all[s, :, here] = dot(mid_t[...], gup_ref[s, :, here], 1, 0).astype(BF)
            wd_all[s, :, here] = dot(down_t[...], act_ref[s, :, here], 1, 0).astype(BF)
            return carry

        lax.fori_loop(0, wu_all.shape[2] // 256, weigh, 0)
        for item in early + late:
            item.copy(0, s).start()

        @pl.when(j > 0)
        def _():
            for item in early:
                item.fold_one(0, shard_of(j - 1))

        return carry

    lax.fori_loop(0, ring, weigh_shard, 0)
    for item in early:
        item.fold_one(0, shard_of(ring - 1))

    def fold_late(j, carry):
        for item in late:
            item.fold_one(0, shard_of(j))
        return carry

    lax.fori_loop(0, ring, fold_late, 0)
    out.fold(0)
    for name in ("v", "qk", "lse", "exact"):
        loads[name].wait()

    def qk_copy(h, to):
        return remote(
            qk_ref.at[h, :, pl.ds(to * count, count)],
            grad_ref.at[place.shard(h), rows_of(2 * hd * h, 2 * hd, 2 * hd)],
            qsend.at[h, to],
            qrecv.at[h, place.shift_to(to) - 1],
            (place.d, to),
        )

    v_row = 2 * hd * heads_here

    def v_copy(i, j):
        shard, row, rows, _, row_there = FRESH[i]
        return remote(
            v_ref.at[pl.ds(row_there, rows), lanes(place.z(j) * count, count)],
            grad_ref.at[shard, pl.ds(v_row + row, rows)],
            vsend.at[i, j - 1],
            vrecv.at[i, j - 1],
            place.to_z(j),
        )

    def moved_copy(i):
        to, row, rows, _, row_there = MOVED[i]
        return remote(
            v_ref.at[pl.ds(row_there, rows)],
            first_ref.at[pl.ds(row, rows)],
            fsend.at[0],
            frecv.at[0],
            (place.d, to),
        )

    def send_fresh(slot):
        for i, (shard, row, rows, at, row_there) in enumerate(FRESH):
            if (row_there + rows > 2 * hd) != (slot == 2):
                continue

            @pl.when(m == at)
            def _(i=i, shard=shard, row=row, rows=rows, row_there=row_there):
                for j in range(1, ring):
                    v_copy(i, j).start()
                grad_ref[shard, v_row + row : v_row + row + rows, :] = v_ref[
                    pl.ds(row_there, rows), own
                ]

    def send_reused():
        for i, move in enumerate(MOVED):

            @pl.when(m == move[3])
            def _(i=i):
                moved_copy(i).start()

        for at, row, rows, row_there in KEPT:

            @pl.when(m == at)
            def _(row=row, rows=rows, row_there=row_there):
                first_ref[row : row + rows, :] = v_ref[row_there : row_there + rows, :]

    ones = jnp.ones((8, count), BF)

    def process(i):
        if i == 0:
            for name in ("normed", "wt"):
                loads[name].wait()
            for k in range(ring):
                early[1].copy(0, k).wait_send()
                late[1].copy(0, k).wait_send()
        if i < heads_here:
            for j in range(1, ring):
                remote(
                    qk_ref.at[i, :, own],
                    grad_ref.at[0, pl.ds(2 * hd * i, 2 * hd)],
                    qsend.at[i, 0],
                    qrecv.at[i, j - 1],
                    place.to_z(j),
                ).wait_recv()
        begin = group * i
        here = slice(begin, begin + group)
        for k in range(ring):
            wu_all[k, here, :] = dot(grad_ref[k, here, :], mid_ref[...], 1, 0).astype(BF)
            packs[i].copy(0, k).start()
        for k in range(ring):
            sums = dot(ones, grad_ref[k, here, :], 1, 1)
            vector_held[0, k : k + 1, here] = sums[0:1]
        weights = jnp.concatenate([wt_all[k, here, :] for k in range(ring)], 0)

        def add(t, carry):
            toks = lanes(t * tile, tile)
            grads = jnp.concatenate([grad_ref[k, here, toks] for k in range(ring)], 0)
            part = dot(grads, weights, 0, 0)
            rows = rows_of(t * tile, tile, tile)
            grad_in_ref[rows, :] = part if i == 0 else grad_in_ref[rows, :] + part
            return carry

        lax.fori_loop(0, count // tile, add, 0)

    boundary = length_ref[0]
    block = count
    def attend_back(h, carry):
        here_h = rows_of(hd * h, hd, hd)
        keys[...] = jnp.transpose(qk_ref[h, hd : 2 * hd, :])
        vals[...] = jnp.transpose(v_ref[here_h, :])
        for j in range(1, ring):
            remote(
                g_ref.at[pl.ds(0, hd)],
                g_all.at[h, :, own],
                gsend.at[h, 0],
                grecv.at[h, j - 1],
                place.to_z(j),
            ).wait_recv()
        delta[...] = jnp.sum(
            g_all[h].astype(F32) * exact_ref[here_h, :], 0, keepdims=True
        )
        for qi in reversed(range(ring)):
            query_start = qi * block
            here = slice(query_start, query_start + block)
            q = qk_ref[h, 0:hd, here]
            g = g_all[h, :, here]
            grad_q = None
            for ki in range(qi + 1):
                key_start = ki * block
                there = slice(key_start, key_start + block)
                key_t = qk_ref[h, hd : 2 * hd, there]
                scores = dot(keys[there, :], q, 1, 0) - lse_ref[h, :, here]
                if ki == qi:
                    scores = jnp.where(
                        diagonal_mask(scores, key_start, query_start), scores, NEG_LARGE
                    )
                elif key_start < half <= query_start:
                    scores = scores + other_document(boundary, key_start, query_start)
                p = jnp.exp(scores)
                grad_p = dot(vals[there, :], g, 1, 0)
                grad_s = (p * (grad_p - delta[:, here])).astype(BF)
                grad_v = dot(g, p.astype(BF), 1, 1)
                grad_k = dot(q, grad_s, 1, 1)
                part_q = dot(key_t, grad_s, 1, 0)
                grad_q = part_q if grad_q is None else grad_q + part_q
                if qi < ring - 1:
                    grad_v, grad_k = grad_v + dv[:, there], grad_k + dk[:, there]
                if ki < qi:
                    dv[:, there], dk[:, there] = grad_v, grad_k
            qk_ref[h, 0:hd, here] = (grad_q * (hd**-0.5)).astype(BF)
            qk_ref[h, hd : 2 * hd, here] = grad_k.astype(BF)
            v_ref[here_h, here] = grad_v.astype(BF)

            @pl.when(m == qi)
            def _(here=here):
                grad_ref[place.shard(h), rows_of(2 * hd * h, 2 * hd, 2 * hd), :] = qk_ref[
                    h, :, here
                ]

            @pl.when(m != qi)
            def _(qi=qi):
                qk_copy(h, qi).start()

        @pl.when(h == 1)
        def _():
            send_fresh(1)
            for item in early:
                item.fold(1)

        return carry

    lax.fori_loop(0, heads_here, attend_back, 0)
    send_fresh(2)
    send_reused()
    late = late + (out,)
    for item in late:
        item.fold(1)
    process(0)
    process(1)
    for item in early:
        item.fold(2)
    packs[0].fold(0)
    packs[1].fold(0)
    packs[0].fold(1)
    for item in late:
        item.fold(2)
    packs[1].fold(1)
    packs[0].fold(2)
    for to in range(ring):

        @pl.when(m != to)
        def _(to=to):
            for slot in range(heads_here):
                g_copy(slot, to).wait_send()

    for i, (shard, row, rows, at, row_there) in enumerate(FRESH):

        @pl.when(m == at)
        def _(i=i):
            for j in range(1, ring):
                v_copy(i, j).wait_send()

        @pl.when(m != at)
        def _(i=i, shard=shard, row=row, rows=rows, at=at, row_there=row_there):
            shift = lax.rem(m - at + ring, ring)
            remote(
                v_ref.at[pl.ds(row_there, rows), own],
                grad_ref.at[shard, pl.ds(v_row + row, rows)],
                vsend.at[i, shift - 1],
                vrecv.at[i, shift - 1],
                place.to_z(shift),
            ).wait_recv()

    for i, move in enumerate(MOVED):

        @pl.when(m == move[3])
        def _(i=i):
            moved_copy(i).wait_send()

        @pl.when(m == move[0])
        def _(i=i):
            moved_copy(i).wait_recv()

    process(2)
    process(3)

    def input_back(i, carry):
        here = rows_of(i * tile, tile, tile)
        grad = grad_in_ref[here, :]
        value = hidden_ref[here, :]
        center = value - jnp.mean(value, -1, keepdims=True)
        scale = lax.rsqrt(jnp.mean(center * center, -1, keepdims=True) + EPSILON)
        unit = center * scale
        grad_unit = grad * pre_gain
        grad_in_ref[here, :] = middle_ref[here, :] + scale * (
            grad_unit
            - jnp.mean(grad_unit, -1, keepdims=True)
            - unit * jnp.mean(grad_unit * unit, -1, keepdims=True)
        )
        sums = (
            jnp.sum(grad * unit, 0, keepdims=True),
            jnp.sum(grad, 0, keepdims=True),
        )
        return tuple(x + y for x, y in zip(carry, sums))

    sums = lax.fori_loop(0, count // tile, input_back, (zero_row,) * 2)
    for i, value in enumerate(sums):
        vector_held[0, ring + i : ring + 1 + i, 0:width] = value

    turned = jnp.logical_or(m == 1, m == 2)

    def natural(own_row):
        parts = []
        for i in range(heads_here):
            here, turn = group * i, group * ((i - 1) % heads_here)
            parts.append(
                jnp.where(turned, own_row[:, turn : turn + hd], own_row[:, here : here + hd])
            )
        parts.append(jnp.zeros((1, own_row.shape[1] - hd * heads_here), F32))
        return jnp.concatenate(parts, 1)

    routes = [place.to_core, place.to_x, place.to_y]
    routes += [place.to_plane(step) for step in place.steps()]
    bit = 1
    while bit < ring:
        routes.append((place.d, m + bit - 2 * bit * lax.rem(m // bit, 2)))
        bit *= 2

    def vector_copy(k):
        return remote(
            vector_held.at[k], vector_came.at[k], wsend.at[k], wrecv.at[k], routes[k]
        )

    def vector_fold(k):
        vector_copy(k).wait_recv()
        value = vector_held[k] + vector_came[k]
        if k + 1 < len(routes):
            vector_held[k + 1] = value
            vector_copy(k + 1).start()
        else:
            own_row = value[0:1]
            for s in range(1, ring):
                own_row = jnp.where(m == s, value[s : s + 1], own_row)
            vector_sum[...] = jnp.concatenate([value[ring : ring + 6], own_row, natural(own_row)], 0)

    vector_copy(0).start()
    first, second, third, fourth = packs
    for item in early:
        item.fold_pair()
    second.fold(2)
    third.fold(0)
    fourth.fold(0)
    vector_fold(0)
    for item in late:
        item.fold_pair()
    third.fold(1)
    fourth.fold(1)
    vector_fold(1)
    first.fold_pair()
    second.fold_pair()
    for item in early:
        item.finish_sum()
    third.fold(2)
    fourth.fold(2)
    vector_fold(2)
    first.finish_sum()
    second.finish_sum()
    for item in late:
        item.finish_sum()
    third.fold_pair()
    fourth.fold_pair()
    for item in early:
        item.spread(6)
    for k in range(3, len(routes) - 1):
        vector_fold(k)
    first.spread(6)
    second.spread(6)
    third.finish_sum()
    fourth.finish_sum()
    for item in late:
        item.spread(6)
    for item in early:
        item.spread(7)
    vector_fold(len(routes) - 1)
    third.spread(6)
    fourth.spread(6)
    for item in late + (first, second, third, fourth):
        item.spread(7)
    everything = early + late + tuple(packs)
    for item in everything:
        item.wait(7)
        item.drain(1 if item in (early[1], late[1]) else 0)
    for k in range(len(routes)):
        vector_copy(k).wait_send()
    for to in range(ring):

        @pl.when(m != to)
        def _(to=to):
            for h in range(heads_here):
                qk_copy(h, to).wait_send()

    for i in range(heads_here):
        at = rows_of(group * jnp.where(turned, (i - 1) % heads_here, i), hd, hd)
        wq_sum[hd * i : hd * i + hd, :] = pack_held[at, :]
        at = rows_of(group * jnp.where(turned, (i - 1) % heads_here, i) + hd, hd, hd)
        wk_sum[hd * i : hd * i + hd, :] = pack_held[at, :]
    wv_sum[...] = pack_held[v_row : v_row + piece, :]


def backward_call(
    ring, heads_here, planes, length, context, hidden, grad_out, pre_gain, b_out, mid_gain, mid_shift,
    b_down, bias,
    qk, v, lse, exact, normed, wt, wo, wo_far, wu, wu_far, wd, wd_far, piece,
):
    count, width = hidden.shape
    total = ring * count
    hd = HEAD_DIM
    others = ring - 1
    sds = jax.ShapeDtypeStruct
    dma = pltpu.SemaphoreType.DMA
    hops = 3 + (planes.bit_length() - 1) + (ring.bit_length() - 1)
    stages = 8 + planes.bit_length() - 1
    pack_rows = wt.shape[1]
    out_pad = wo.shape[0] + -wo.shape[0] % (16 * PLANE)
    sizes = [wd.shape[0] // 2, wu.shape[0] // 2] * 2 + [out_pad] + [2 * hd] * (heads_here + 1)
    bufs = [buf for rows_ in sizes for buf in Reduce.buffers(rows_, width, planes)]
    vector = (ring + 6 + -(ring + 6) % 8, bias.shape[2])
    vm = pltpu.VMEM
    return pl.pallas_call(
        functools.partial(backward_kernel, ring, heads_here, planes),
        out_shape=(
            sds(hidden.shape, F32),
            sds(hidden.shape, F32),
            sds((piece, total), BF),
            sds((heads_here * hd, width), BF),
            sds((heads_here * hd, width), BF),
            sds((piece, width), BF),
            sds((out_pad, width), BF),
            sds(wu.shape, BF),
            sds(wd.shape, BF),
            sds((8, vector[1]), F32),
        ),
        in_specs=[SM] + [VM] * 9 + [ANY] * 12,
        out_specs=[VM] * 10,
        scratch_shapes=[
            vm(qk.shape, BF),
            vm(v.shape, BF),
            vm(lse.shape, F32),
            vm(exact.shape, F32),
            vm(wt.shape, BF),
            vm((ring * wo.shape[0], width), BF),
            vm((ring,) + wu.shape, BF),
            vm((ring,) + wd.shape, BF),
            vm((count, width), F32),
            vm((count, width), BF),
            vm((width, count), BF),
            vm((count, width), BF),
            vm((width, count), BF),
            vm((ring, count, width), BF),
            vm((ring, count, width), BF),
            vm((width, count), BF),
            vm((pack_rows, width), BF),
            vm((ring, out_pad, width), BF),
            vm((heads_here, hd, total), BF),
            vm((total, hd), BF),
            vm((total, hd), BF),
            vm((1, total), F32),
            vm((hd, total), F32),
            vm((hd, total), F32),
            vm((ring, pack_rows, count), BF),
            vm((hops,) + vector, F32),
            vm((hops,) + vector, F32),
            dma((3 * ring + 6,)),
            dma((heads_here, ring)),
            dma((heads_here, others)),
            dma((heads_here, ring)),
            dma((heads_here, others)),
            dma((len(FRESH), others)),
            dma((len(FRESH), others)),
            dma((1,)),
            dma((1,)),
            dma((5 + heads_here + 1, stages, ring)),
            dma((5 + heads_here + 1, stages, ring)),
            dma((hops,)),
            dma((hops,)),
        ]
        + bufs,
        compiler_params=pltpu.CompilerParams(
            collective_id=1, has_side_effects=True, vmem_limit_bytes=67043328
        ),
        name="backward",
    )(
        length, context, hidden, grad_out, pre_gain, b_out, mid_gain, mid_shift, b_down, bias, qk, v, lse, exact,
        normed, wt, wo, wo_far, wu, wu_far, wd, wd_far,
    )


def finish_kernel(count_in, turned, pieces, vector_ref, *refs):
    ins, refs = refs[:count_in], refs[count_in:]
    outs, refs = refs[:count_in], refs[count_in:]
    rows, refs = refs[: len(pieces)], refs[len(pieces) :]
    held, wide, sem_in, sem_out = refs[:count_in], refs[count_in:-2], refs[-2], refs[-1]
    rising = iter(wide)
    loads = [pltpu.make_async_copy(a, b, sem_in.at[i]) for i, (a, b) in enumerate(zip(ins, held))]
    for load in loads:
        load.start()
    for ref, (row, start, size) in zip(rows, pieces):
        ref[...] = jnp.reshape(vector_ref[row : row + 1, start : start + size], (size,))
    stores = []
    for i in range(count_in):
        loads[i].wait()
        source = held[i]
        if source.dtype != F32:
            into = next(rising)
            value = source[0 : into.shape[0], :]
            if i == turned:
                value = jnp.transpose(value)
            into[...] = value.astype(F32)
            source = into
        stores.append(pltpu.make_async_copy(source, outs[i], sem_out.at[i]))
        stores[i].start()
    for store in stores:
        store.wait()


def finish_call(vector, pieces, arrays, rows, turned):
    sds = jax.ShapeDtypeStruct
    dma = pltpu.SemaphoreType.DMA
    shapes = [(rows_, array.shape[1]) for array, rows_ in zip(arrays, rows)]
    return pl.pallas_call(
        functools.partial(finish_kernel, len(arrays), turned, pieces),
        out_shape=[sds(shape, F32) for shape in shapes] + [sds((p[2],), F32) for p in pieces],
        in_specs=[VM] + [ANY] * len(arrays),
        out_specs=[ANY] * len(arrays) + [VM] * len(pieces),
        scratch_shapes=[pltpu.VMEM(array.shape, array.dtype) for array in arrays]
        + [pltpu.VMEM(s, F32) for s, array in zip(shapes, arrays) if array.dtype != F32]
        + [dma((len(arrays),)), dma((len(arrays),))],
        compiler_params=pltpu.CompilerParams(vmem_limit_bytes=VMEM_LIMIT),
        name="finish",
    )(vector, *arrays)


def shards(
    hidden_in,
    first_values,
    first_length,
    pre_gain,
    pre_shift,
    w_query,
    b_query,
    w_key,
    w_value,
    b_value,
    w_out,
    b_out,
    mid_gain,
    mid_shift,
    w_up,
    b_up,
    w_down,
    b_down,
    grad_out,
):
    ring = lax.axis_size("mp")
    m = lax.axis_index("mp")
    hd = HEAD_DIM
    count, width = hidden_in.shape
    head_width = w_query.shape[1]
    heads_here = head_width // hd
    piece = w_value.shape[1]
    context_t, normed, qk, v, lse, exact, wt_all, bias_all, wo_far, wu_far, wd_far = forward_call(
        ring,
        heads_here,
        first_length,
        hidden_in,
        pre_gain,
        pre_shift,
        w_query.T,
        w_key.T,
        w_value.T,
        b_query,
        b_value,
        b_up,
        first_values.T,
        w_out,
        w_up,
        w_down,
    )
    layer_out, grad_input, grad_first, wq_sum, wk_sum, wv_sum, wo_sum, wu_sum, wd_sum, vector = backward_call(
        ring,
        heads_here,
        lax.axis_size("dp") // PLANE,
        first_length,
        context_t,
        hidden_in,
        grad_out,
        pre_gain,
        b_out,
        mid_gain,
        mid_shift,
        b_down,
        bias_all,
        qk,
        v,
        lse,
        exact,
        normed,
        wt_all,
        w_out,
        wo_far,
        w_up,
        wu_far,
        w_down,
        wd_far,
        piece,
    )
    pack_rows = wt_all.shape[1]
    pieces = [(i, 0, width) for i in range(6)] + [
        (7, 0, head_width),
        (6, 2 * head_width, piece),
        (6, pack_rows, b_up.shape[0]),
    ]
    arrays = [layer_out, grad_input, wu_sum, wd_sum, grad_first, wq_sum, wk_sum, wo_sum, wv_sum]
    rows = [count, count, width, w_down.shape[0], piece, head_width, head_width, head_width, piece]
    done = finish_call(vector, pieces, arrays, rows, 3)
    layer_out, grad_input, wu_sum, wd_sum, grad_first, wq_sum, wk_sum, wo_sum, wv_sum = done[:9]
    pre_gain_sum, pre_shift_sum, b_out_sum, mid_gain_sum, mid_shift_sum, b_down_sum = done[9:15]
    b_query_sum, b_value_sum, b_up_sum = done[15:]
    return (
        layer_out,
        grad_input,
        grad_first.T,
        pre_gain_sum,
        pre_shift_sum,
        wq_sum.T,
        b_query_sum,
        wk_sum.T,
        wv_sum.T,
        b_value_sum,
        wo_sum,
        b_out_sum,
        mid_gain_sum,
        mid_shift_sum,
        wu_sum,
        b_up_sum,
        wd_sum,
        b_down_sum,
    )


def solution(mesh):
    rows, cols = P(("dp", "mp"), None), P(None, "mp")
    return jax.shard_map(
        shards,
        mesh=mesh,
        in_specs=(
            rows,
            P("dp", "mp"),
            P("dp"),
            P(),
            P(),
            cols,
            P("mp"),
            cols,
            cols,
            P("mp"),
            P("mp", None),
            P(),
            P(),
            P(),
            cols,
            P("mp"),
            P("mp", None),
            P(),
            rows,
        ),
        out_specs=(
            rows,
            rows,
            P("dp", "mp"),
            P(),
            P(),
            cols,
            P("mp"),
            cols,
            cols,
            P("mp"),
            P("mp", None),
            P(),
            P(),
            P(),
            cols,
            P("mp"),
            P("mp", None),
            P(),
        ),
        check_vma=False,
    )
```

```python
import functools

import jax
import jax.numpy as jnp
from jax import lax
from jax.experimental import pallas as pl
from jax.experimental.pallas import tpu as pltpu
from jax.sharding import PartitionSpec as P

HEAD_DIM = 64
EPSILON = 1e-05
NEG_LARGE = -1e30
MESH = pl.DeviceIdType.MESH
BF = jnp.bfloat16
F32 = jnp.float32
ANY = pl.BlockSpec(memory_space=pl.ANY)
VM = pl.BlockSpec(memory_space=pltpu.VMEM)
SM = pl.BlockSpec(memory_space=pltpu.SMEM)
VMEM_LIMIT = 60 << 20
LANE = 128
PLANE = 8
RING = 4
HEADS_AT = ((0, 1, 6), (7, 8, 2), (9, 10, 3), (4, 5, 11))
FRESH = (
    (0, 0, 96, 0, 0),
    (1, 0, 32, 0, 96),
    (1, 32, 64, 1, 128),
    (2, 0, 64, 2, 128),
    (2, 64, 32, 3, 0),
    (3, 0, 96, 3, 32),
)
KEPT = ((0, 0, 64, 128), (1, 0, 96, 32), (2, 0, 96, 0), (3, 32, 64, 128))
MOVED = ((0, 64, 32, 1, 0), (3, 0, 32, 2, 96))


def dot(left, right, left_dim, right_dim):
    return lax.dot_general(
        left, right, (((left_dim,), (right_dim,)), ((), ())), preferred_element_type=F32
    )


def layer_norm(values, gain, shift):
    center = values - jnp.mean(values, -1, keepdims=True)
    spread = jnp.mean(center * center, -1, keepdims=True)
    return center * lax.rsqrt(spread + EPSILON) * gain + shift


def gelu_tanh(values):
    return (
        0.5
        * values
        * (1.0 + jnp.tanh(0.7978845608028654 * (values + 0.044715 * values * values * values)))
    )


def lanes(start, size):
    return pl.ds(pl.multiple_of(start, LANE), size)


def rows_of(start, size, unit):
    return pl.ds(pl.multiple_of(start, unit), size)


def flat(ref):
    return jnp.reshape(ref[...], (1, ref.shape[0]))


class Place:
    def __init__(self, ring, planes=1):
        self.ring = ring
        self.planes = planes
        self.d = lax.axis_index("dp")
        self.m = lax.axis_index("mp")
        d = self.d
        self.core = lax.rem(d, 2)
        self.x = lax.rem(d // 2, 2)
        self.y = lax.rem(d // 4, 2)
        self.to_core = (d + 1 - 2 * self.core, self.m)
        self.to_x = (d + 2 - 4 * self.x, self.m)
        self.to_y = (d + 4 - 8 * self.y, self.m)
        self.pair = self.m + 1 - 2 * lax.rem(self.m, 2)
        self.across = lax.rem(self.m + 2, RING)
        self.corner = RING - 1 - self.m

    def z(self, shift):
        return lax.rem(self.m + shift, self.ring)

    def to_z(self, shift):
        return (self.d, self.z(shift))

    def shift_to(self, position):
        return lax.rem(position - self.m + self.ring, self.ring)

    def head(self, slot):
        value = 0
        for k, heads in enumerate(HEADS_AT):
            for at, head in enumerate(heads):
                value = jnp.where(jnp.logical_and(self.m == k, slot == at), head, value)
        return value

    def shard(self, slot):
        return self.head(slot) // len(HEADS_AT[0])

    def steps(self):
        return [PLANE << b for b in range(self.planes.bit_length() - 1)]

    def to_plane(self, step):
        return (self.d + step - 2 * step * lax.rem(self.d // step, 2), self.m)

    def barrier(self):
        sem = pltpu.get_barrier_semaphore()
        peers = [self.to_z(j) for j in range(1, self.ring)]
        peers += [self.to_core, self.to_x, self.to_y]
        peers += [self.to_plane(step) for step in self.steps()]
        for peer in peers:
            pl.semaphore_signal(sem, inc=1, device_id=peer, device_id_type=MESH)
        pl.semaphore_wait(sem, len(peers))

    def slot(self, x_first):
        if x_first:
            return self.core * 4 + self.y * 2 + self.x
        return self.core * 4 + self.x * 2 + self.y


def remote(src, dst, send, recv, device):
    return pltpu.make_async_remote_copy(
        src_ref=src,
        dst_ref=dst,
        send_sem=send,
        recv_sem=recv,
        device_id=device,
        device_id_type=MESH,
    )


class Gather:
    def __init__(self, place, src, dst, send, recv, item, first_row, rows, x_first):
        self.place, self.src, self.dst = place, src, dst
        self.send, self.recv, self.item = send, recv, item
        self.first_row, self.part, self.x_first = first_row, rows // PLANE, x_first

    def window(self, start, size):
        part = self.part
        return rows_of(self.first_row + start * part, size * part, part & -part)

    def copy(self, stage, k):
        place = self.place
        slot = place.slot(self.x_first)
        near, far = (place.to_x, place.to_y) if self.x_first else (place.to_y, place.to_x)
        shard = (place.across, place.pair, place.corner)[k]
        window = self.window(slot, 1)
        if stage == 0:
            shard, target = place.m, (place.d, place.across)
        elif stage == 1:
            shard, target = (place.m, place.across)[k], (place.d, place.pair)
        elif stage == 2:
            target = near
        elif stage == 3:
            window, target = self.window((slot // 2) * 2, 2), far
        else:
            window, target = self.window(place.core * 4, 4), place.to_core
        own = stage == 0 or (stage == 1 and k == 0)
        source = self.src.at[window] if own else self.dst.at[shard, window]
        return remote(
            source,
            self.dst.at[shard, window],
            self.send.at[self.item, stage, k],
            self.recv.at[self.item, stage, k],
            target,
        )

    def start(self, stage):
        if stage == 0:
            self.copy(0, 0).start()
            self.copy(1, 0).start()
        elif stage == 1:
            self.copy(0, 0).wait_recv()
            self.copy(1, 1).start()
            self.copy(2, 0).start()
        elif stage == 2:
            for k in range(2):
                self.copy(1, k).wait_recv()
                self.copy(2, k + 1).start()
        else:
            for k in range(3):
                self.copy(stage - 1, k).wait_recv()
                self.copy(stage, k).start()

    def arrive(self):
        for k in range(3):
            self.copy(4, k).wait_recv()

    def drain(self):
        for stage, copies in enumerate((1, 2, 3, 3, 3)):
            for k in range(copies):
                self.copy(stage, k).wait_send()


class Reduce:
    def __init__(self, place, src, bufs, out, send, recv, item, x_first, first_row=0):
        self.place, self.src, self.out = place, src, out
        self.first_row = first_row
        self.r_core, self.r_far, self.r_near, self.r_z, self.r_plane = bufs
        self.send, self.recv, self.item, self.x_first = send, recv, item, x_first
        self.part = out.shape[0] // PLANE
        if x_first:
            self.near, self.far = place.to_x, place.to_y
            self.near_bit, self.far_bit = place.x, place.y
        else:
            self.near, self.far = place.to_y, place.to_x
            self.near_bit, self.far_bit = place.y, place.x

    def rows(self, start, size):
        return rows_of(start * self.part, size * self.part, self.part & -self.part)

    def copy(self, stage, k):
        place = self.place
        if stage == 0:
            begin = self.first_row + (1 - place.core) * 4 * self.part
            src = self.src.at[k, rows_of(begin, 4 * self.part, self.part & -self.part)]
            dst, target = self.r_core.at[k], place.to_core
        elif stage == 1:
            src = self.r_core.at[k, self.rows((1 - self.far_bit) * 2, 2)]
            dst, target = self.r_far.at[k], self.far
        elif stage == 2:
            src = self.r_far.at[k, self.rows(1 - self.near_bit, 1)]
            dst, target = self.r_near.at[k], self.near
        elif stage == 3:
            src = self.r_near.at[(place.pair, place.corner)[k]]
            dst, target = self.r_z.at[k], (place.d, place.pair)
        elif stage == 4:
            src = self.r_near.at[place.across]
            dst, target = self.r_z.at[2], (place.d, place.across)
        else:
            slot = place.slot(self.x_first)
            if stage == 5:
                window, target = self.rows(slot, 1), self.near
            elif stage == 6:
                window, target = self.rows((slot // 2) * 2, 2), self.far
            else:
                window, target = self.rows(place.core * 4, 4), place.to_core
            src = dst = self.out.at[window]
        return remote(
            src, dst, self.send.at[self.item, stage, k], self.recv.at[self.item, stage, k], target
        )

    def members(self, stage):
        return range((RING, RING, RING, 2, 1, 1, 1, 1)[stage])

    def start(self, stage):
        for k in self.members(stage):
            self.copy(stage, k).start()

    def wait(self, stage):
        for k in self.members(stage):
            self.copy(stage, k).wait_recv()

    def fold_one(self, stage, k):
        place, part = self.place, self.part
        if stage == 0:
            base = self.first_row + place.core * 4 * part
            kept, into, size = self.src, self.r_core, 4 * part
        elif stage == 1:
            kept, base, into, size = self.r_core, self.far_bit * 2 * part, self.r_far, 2 * part
        else:
            kept, base, into, size = self.r_far, self.near_bit * part, self.r_near, part
        unit = part & -part
        step = min(unit, 32)
        self.copy(stage, k).wait_recv()

        def add(i, carry):
            mine = kept[k, rows_of(base + i * step, step, min(unit, step)), :].astype(F32)
            here = rows_of(i * step, step, step)
            into[k, here, :] = (into[k, here, :].astype(F32) + mine).astype(BF)
            return carry

        lax.fori_loop(0, size // step, add, 0)
        if stage < 2:
            self.copy(stage + 1, k).start()

    def fold(self, stage):
        for k in self.members(stage):
            self.fold_one(stage, k)
        if stage == 2:
            self.start(3)

    def fold_pair(self):
        place = self.place
        self.wait(3)
        other = self.r_near[place.across].astype(F32) + self.r_z[1].astype(F32)
        self.r_near[place.across] = other.astype(BF)
        self.start(4)
        mine = self.r_near[place.m].astype(F32) + self.r_z[0].astype(F32)
        self.r_near[place.m] = mine.astype(BF)

    def finish_sum(self):
        place = self.place
        self.wait(4)
        here = self.rows(place.slot(self.x_first), 1)
        value = self.r_near[place.m].astype(F32) + self.r_z[2].astype(F32)
        self.out[here, :] = value.astype(BF)
        for b, step in enumerate(place.steps()):
            copy = remote(
                self.out.at[here],
                self.r_plane.at[b],
                self.send.at[self.item, 8 + b, 0],
                self.recv.at[self.item, 8 + b, 0],
                place.to_plane(step),
            )
            copy.start()
            copy.wait()
            mine = self.out[here, :].astype(F32)
            self.out[here, :] = (mine + self.r_plane[b].astype(F32)).astype(BF)
        self.start(5)

    def spread(self, stage):
        self.wait(stage - 1)
        self.start(stage)

    def drain(self, first):
        for stage in range(first, 8):
            for k in self.members(stage):
                self.copy(stage, k).wait_send()

    @staticmethod
    def buffers(rows, width, planes):
        part = rows // PLANE
        extra = max(planes.bit_length() - 1, 1)
        return [
            pltpu.VMEM((RING, 4 * part, width), BF),
            pltpu.VMEM((RING, 2 * part, width), BF),
            pltpu.VMEM((RING, part, width), BF),
            pltpu.VMEM((3, part, width), BF),
            pltpu.VMEM((extra, part, width), BF),
        ]


def diagonal_mask(scores, key_start, query_start):
    keys = lax.broadcasted_iota(jnp.int32, scores.shape, 0) + key_start
    queries = lax.broadcasted_iota(jnp.int32, scores.shape, 1) + query_start
    return keys <= queries


def other_document(boundary, key_start, query_start):
    crossing = jnp.logical_and(boundary > key_start, boundary <= query_start)
    return jnp.where(crossing, NEG_LARGE, 0.0)


def forward_kernel(
    ring,
    heads_here,
    length_ref,
    hidden_ref,
    gain_ref,
    shift_ref,
    wq_ref,
    wk_ref,
    wv_ref,
    bq_ref,
    bv_ref,
    bu_ref,
    first_ref,
    wo_ref,
    wu_ref,
    wd_ref,
    context_ref,
    normed_out,
    qk_out,
    v_out,
    lse_ref,
    exact_out,
    wt_out,
    bias_all,
    wo_far,
    wu_far,
    wd_far,
    normed_ref,
    qk_ref,
    v_ref,
    exact_ref,
    wt_all,
    osem,
    y_send,
    vy_send,
    c_send,
    keys,
    gsend,
    grecv,
    bsend,
    brecv,
    qsend,
    qrecv,
    vsend,
    vrecv,
    fsend,
    frecv,
    csend,
    crecv,
):
    place = Place(ring)

    def keep(i, src, dst):
        return pltpu.make_async_copy(src, dst, osem.at[i])

    m = place.m
    count = hidden_ref.shape[0]
    total = ring * count
    piece = first_ref.shape[0]
    half = total // 2
    hd = HEAD_DIM
    pack_rows = wt_all.shape[1]
    v_row = 2 * hd * heads_here
    turned = jnp.logical_or(m == 1, m == 2)

    def slot_row(slot):
        return rows_of(hd * jnp.where(turned, (slot + 1) % heads_here, slot), hd, hd)

    bq, bv, bu = flat(bq_ref), flat(bv_ref), flat(bu_ref)
    bias_parts = []
    for slot in range(heads_here):
        row = 2 * hd * slot
        wt_all[m, row : row + hd, :] = wq_ref[slot_row(slot), :]
        wt_all[m, row + hd : row + 2 * hd, :] = wk_ref[slot_row(slot), :]
        here, after = hd * slot, hd * ((slot + 1) % heads_here)
        own_bias = jnp.where(turned, bq[:, after : after + hd], bq[:, here : here + hd])
        bias_parts += [own_bias, jnp.zeros_like(own_bias)]
    wt_all[m, v_row : v_row + piece, :] = wv_ref[...]
    spare = pack_rows - v_row - piece
    wt_all[m, v_row + piece :, :] = jnp.zeros((spare, wv_ref.shape[1]), BF)
    bias_parts += [bv, jnp.zeros((1, spare), F32), bu]
    bias_row = jnp.concatenate(bias_parts, 1)
    bias_all[m] = jnp.broadcast_to(bias_row, (8, bias_row.shape[1]))
    wt_ref = wt_all.at[m]
    bias_ref = bias_all.at[m]
    place.barrier()
    half_pack = pack_rows // 2
    small = [
        Gather(place, wt_ref, wt_all, gsend, grecv, i, i * half_pack, half_pack, i == 0)
        for i in range(2)
    ]
    big = [
        Gather(place, wo_ref, wo_far, gsend, grecv, 2, 0, wo_ref.shape[0], True),
        Gather(place, wu_ref, wu_far, gsend, grecv, 3, 0, wu_ref.shape[0], True),
        Gather(place, wd_ref, wd_far, gsend, grecv, 4, 0, wd_ref.shape[0], False),
    ]
    for item in small:
        item.start(0)

    def bias_copy(j):
        return remote(
            bias_ref, bias_all.at[m], bsend.at[j - 1], brecv.at[j - 1], place.to_z(j)
        )

    for j in range(1, ring):
        bias_copy(j).start()

    def moved_copy(i):
        _, row, rows, to, row_there = MOVED[i]
        return remote(
            first_ref.at[pl.ds(row, rows)],
            v_ref.at[pl.ds(row_there, rows)],
            fsend.at[0],
            frecv.at[0],
            (place.d, to),
        )

    for i, move in enumerate(MOVED):

        @pl.when(m == move[0])
        def _(i=i):
            moved_copy(i).start()

    for at, row, rows, row_there in KEPT:

        @pl.when(m == at)
        def _(row=row, rows=rows, row_there=row_there):
            v_ref[row_there : row_there + rows, :] = first_ref[row : row + rows, :]

    normed_ref[...] = layer_norm(hidden_ref[...], flat(gain_ref), flat(shift_ref)).astype(BF)

    for item in small:
        item.start(1)
    for item in big:
        item.start(0)
    for item in small:
        item.start(2)
    for item in big:
        item.start(1)
    for stage in (3, 4):
        for item in small:
            item.start(stage)
    for j in range(1, ring):
        bias_copy(j).wait_recv()
    for item in small:
        item.arrive()

    own = lanes(m * count, count)

    def qk_copy(slot, to):
        return remote(
            y_send.at[to, slot],
            qk_ref.at[slot, :, own],
            qsend.at[to, slot],
            qrecv.at[slot, place.shift_to(to) - 1],
            (place.d, to),
        )

    def v_copy(i):
        shard, row, rows, to, row_there = FRESH[i]
        return remote(
            vy_send.at[shard, pl.ds(row, rows)],
            v_ref.at[pl.ds(row_there, rows), own],
            vsend.at[i],
            vrecv.at[i, place.shift_to(to) - 1],
            (place.d, to),
        )

    where_is = {
        (head // heads_here, slot): to
        for to, heads in enumerate(HEADS_AT)
        for slot, head in enumerate(heads)
    }

    for shard in range(ring):
        out = dot(wt_all[shard], normed_ref[...], 1, 1)
        out = out + jnp.transpose(bias_all[shard, :, 0:pack_rows])[:, 0:1]
        for slot in range(heads_here):
            to = where_is[shard, slot]
            row = 2 * hd * slot
            y_send[to, slot, 0:hd, :] = (out[row : row + hd] * (hd**-0.5)).astype(BF)
            y_send[to, slot, hd : 2 * hd, :] = out[row + hd : row + 2 * hd].astype(BF)
        vy_send[shard] = out[v_row : v_row + piece].astype(BF)

    def share(slot):
        for to in range(ring):

            @pl.when(m == to)
            def _(to=to):
                qk_ref[slot, :, own] = y_send[to, slot]

            @pl.when(m != to)
            def _(to=to):
                qk_copy(slot, to).start()

    share(0)
    for i, (shard, row, rows, to, row_there) in enumerate(FRESH):

        @pl.when(m == to)
        def _(shard=shard, row=row, rows=rows, row_there=row_there):
            v_ref[row_there : row_there + rows, own] = vy_send[shard, row : row + rows, :]

        @pl.when(m != to)
        def _(i=i):
            v_copy(i).start()

    for slot in range(1, heads_here):
        share(slot)
    for stage in (2, 3):
        for item in big:
            item.start(stage)

    def qk_arrive(slot):
        for shift in range(1, ring):
            remote(
                y_send.at[0, slot],
                qk_ref.at[slot, :, own],
                qsend.at[0, slot],
                qrecv.at[slot, shift - 1],
                place.to_z(shift),
            ).wait_recv()

    for i, (shard, row, rows, to, row_there) in enumerate(FRESH):

        @pl.when(m == to)
        def _(i=i, shard=shard, row=row, rows=rows, row_there=row_there):
            for shift in range(1, ring):
                remote(
                    vy_send.at[shard, pl.ds(row, rows)],
                    v_ref.at[pl.ds(row_there, rows), own],
                    vsend.at[i],
                    vrecv.at[i, shift - 1],
                    place.to_z(shift),
                ).wait_recv()

    for i, move in enumerate(MOVED):

        @pl.when(m == move[3])
        def _(i=i):
            moved_copy(i).wait_recv()

    keep(0, normed_ref, normed_out).start()
    keep(1, wt_all, wt_out).start()
    keep(2, v_ref, v_out).start()
    boundary = length_ref[0]
    block = count

    def context_copy(h, to):
        return remote(
            c_send.at[rows_of(hd * h, hd, hd), pl.ds(to * count, count)],
            context_ref.at[rows_of(place.head(h) * hd, hd, hd)],
            csend.at[h, to],
            crecv.at[h, place.shift_to(to) - 1],
            (place.d, to),
        )

    def attend(h, carry):
        qk_arrive(h)
        here_h = rows_of(hd * h, hd, hd)
        keys[...] = jnp.transpose(qk_ref[h, hd : 2 * hd, :])
        for qi in range(ring):
            query_start = qi * block
            queries = slice(query_start, query_start + block)
            q = qk_ref[h, 0:hd, queries]
            top = None
            for ki in range(qi + 1):
                key_start = ki * block
                v = v_ref[here_h, key_start : key_start + block]
                scores = dot(keys[key_start : key_start + block, :], q, 1, 0)
                if ki == qi:
                    scores = jnp.where(
                        diagonal_mask(scores, key_start, query_start), scores, NEG_LARGE
                    )
                elif key_start < half <= query_start:
                    scores = scores + other_document(boundary, key_start, query_start)
                block_top = jnp.max(scores, 0, keepdims=True)
                new_top = block_top if top is None else jnp.maximum(top, block_top)
                p = jnp.exp(scores - new_top)
                p_sum = jnp.sum(p, 0, keepdims=True)
                part = dot(v, p.astype(BF), 1, 0)
                if top is None:
                    run_sum, running = p_sum, part
                else:
                    factor = jnp.exp(top - new_top)
                    run_sum = run_sum * factor + p_sum
                    running = running * factor + part
                top = new_top
            result = running / run_sum
            exact_ref[here_h, queries] = result
            c_send[here_h, queries] = result.astype(BF)
            lse_ref[h, :, queries] = top + jnp.log(run_sum)

            @pl.when(m == qi)
            def _(queries=queries):
                context_ref[rows_of(place.head(h) * hd, hd, hd), :] = c_send[here_h, queries]

            @pl.when(m != qi)
            def _(qi=qi):
                context_copy(h, qi).start()


        keep(3 + h, qk_ref.at[h], qk_out.at[h]).start()
        keep(3 + heads_here + h, exact_ref.at[here_h], exact_out.at[here_h]).start()

        @pl.when(h == 1)
        def _():
            for item in big:
                item.start(4)

        return carry

    lax.fori_loop(0, heads_here, attend, 0)
    for item in big:
        item.arrive()
    for h in range(heads_here):
        for j in range(1, ring):
            remote(
                c_send.at[pl.ds(hd * h, hd), own],
                context_ref.at[pl.ds(0, hd)],
                csend.at[h, 0],
                crecv.at[h, j - 1],
                place.to_z(j),
            ).wait_recv()
    keep(0, normed_ref, normed_out).wait()
    keep(1, wt_all, wt_out).wait()
    keep(2, v_ref, v_out).wait()
    for h in range(heads_here):
        here_h = pl.ds(hd * h, hd)
        keep(3 + h, qk_ref.at[h], qk_out.at[h]).wait()
        keep(3 + heads_here + h, exact_ref.at[here_h], exact_out.at[here_h]).wait()
    for item in small + big:
        item.drain()
    for j in range(1, ring):
        bias_copy(j).wait_send()
    for to in range(ring):

        @pl.when(m != to)
        def _(to=to):
            for slot in range(heads_here):
                qk_copy(slot, to).wait_send()
                context_copy(slot, to).wait_send()

    for i, (shard, row, rows, to, row_there) in enumerate(FRESH):

        @pl.when(m != to)
        def _(i=i):
            v_copy(i).wait_send()

    for i, move in enumerate(MOVED):

        @pl.when(m == move[0])
        def _(i=i):
            moved_copy(i).wait_send()


def forward_call(
    ring, heads_here, length, hidden, gain, shift, wq, wk, wv, bq, bv, bu, first_t, wo, wu, wd
):
    count, width = hidden.shape
    total = ring * count
    hd = HEAD_DIM
    piece = first_t.shape[0]
    others = ring - 1
    pack_rows = 2 * hd * (heads_here + 1)
    sds = jax.ShapeDtypeStruct
    dma = pltpu.SemaphoreType.DMA
    return pl.pallas_call(
        functools.partial(forward_kernel, ring, heads_here),
        out_shape=(
            sds((ring * heads_here * hd, count), BF),
            sds((count, width), BF),
            sds((heads_here, 2 * hd, total), BF),
            sds((heads_here * hd, total), BF),
            sds((heads_here, 1, total), F32),
            sds((heads_here * hd, total), F32),
            sds((ring, pack_rows, width), BF),
            sds((ring, 8, pack_rows + bu.shape[0]), F32),
            sds((ring,) + wo.shape, BF),
            sds((ring,) + wu.shape, BF),
            sds((ring,) + wd.shape, BF),
        ),
        in_specs=[SM] + [VM] * 10 + [ANY] * 3,
        out_specs=[VM] + [ANY] * 3 + [VM] + [ANY] * 2 + [VM] + [ANY] * 3,
        scratch_shapes=[
            pltpu.VMEM((count, width), BF),
            pltpu.VMEM((heads_here, 2 * hd, total), BF),
            pltpu.VMEM((heads_here * hd, total), BF),
            pltpu.VMEM((heads_here * hd, total), F32),
            pltpu.VMEM((ring, pack_rows, width), BF),
            dma((3 + 2 * heads_here,)),
            pltpu.VMEM((ring, heads_here, 2 * hd, count), BF),
            pltpu.VMEM((ring, piece, count), BF),
            pltpu.VMEM((heads_here * hd, total), BF),
            pltpu.VMEM((total, hd), BF),
            dma((5, 5, 3)),
            dma((5, 5, 3)),
            dma((others,)),
            dma((others,)),
            dma((ring, heads_here)),
            dma((heads_here, others)),
            dma((len(FRESH),)),
            dma((len(FRESH), others)),
            dma((1,)),
            dma((1,)),
            dma((heads_here, ring)),
            dma((heads_here, others)),
        ],
        compiler_params=pltpu.CompilerParams(
            collective_id=0, has_side_effects=True, vmem_limit_bytes=VMEM_LIMIT
        ),
        name="forward",
    )(length, hidden, gain, shift, wq, wk, wv, bq, bv, bu, first_t, wo, wu, wd)


def backward_kernel(
    ring,
    heads_here,
    planes,
    length_ref,
    context_ref,
    hidden_ref,
    grad_out_ref,
    pre_gain_ref,
    b_out_ref,
    mid_gain_ref,
    mid_shift_ref,
    b_down_ref,
    bias_ref,
    qk_hbm,
    v_hbm,
    lse_hbm,
    exact_hbm,
    normed_hbm,
    wt_hbm,
    wo_hbm,
    wo_far_hbm,
    wu_hbm,
    wu_far_hbm,
    wd_hbm,
    wd_far_hbm,
    layer_out_ref,
    grad_in_ref,
    first_ref,
    wq_sum,
    wk_sum,
    wv_sum,
    wo_sum,
    wu_sum,
    wd_sum,
    vector_sum,
    layer_ref,
    qk_ref,
    v_ref,
    lse_ref,
    exact_ref,
    wt_all,
    wo_all,
    wu_all,
    wd_all,
    middle_ref,
    mid_ref,
    mid_t,
    down_ref,
    down_t,
    act_ref,
    gup_ref,
    g_ref,
    pack_held,
    wo_share,
    g_all,
    keys,
    vals,
    delta,
    dk,
    dv,
    grad_ref,
    vector_held,
    vector_came,
    lsem,
    gsend,
    grecv,
    qsend,
    qrecv,
    vsend,
    vrecv,
    fsend,
    frecv,
    rsend,
    rrecv,
    wsend,
    wrecv,
    *bufs,
):
    place = Place(ring, planes)
    m = place.m
    count, width = hidden_ref.shape
    total = ring * count
    half = total // 2
    hd = HEAD_DIM
    piece = first_ref.shape[0]
    out_rows = wo_hbm.shape[0]
    pack_lanes = grad_ref.shape[1]
    tile = count // 4
    own = lanes(m * count, count)

    def shard_of(j):
        return lax.rem(m - j + ring, ring)

    loads = {}

    def load(name, src, dst):
        loads[name] = pltpu.make_async_copy(src, dst, lsem.at[len(loads)])
        loads[name].start()

    for j in range(ring):
        into = wo_all.at[rows_of(shard_of(j) * out_rows, out_rows, 16)]
        load(("wo", j), wo_hbm if j == 0 else wo_far_hbm.at[shard_of(j)], into)
    for j in range(ring):
        s = shard_of(j)
        load(("wu", j), wu_hbm if j == 0 else wu_far_hbm.at[s], wu_all.at[s])
        load(("wd", j), wd_hbm if j == 0 else wd_far_hbm.at[s], wd_all.at[s])
    load("v", v_hbm, v_ref)
    load("qk", qk_hbm, qk_ref)
    load("lse", lse_hbm, lse_ref)
    load("exact", exact_hbm, exact_ref)
    load("wt", wt_hbm, wt_all)
    place.barrier()

    b_out, mid_gain, mid_shift = flat(b_out_ref), flat(mid_gain_ref), flat(mid_shift_ref)
    b_down, pre_gain = flat(b_down_ref), flat(pre_gain_ref)
    act_ref[0] = jnp.transpose(context_ref[...])
    vector_held[0] = jnp.zeros_like(vector_held[0])
    wo_share[:, out_rows:, :] = jnp.zeros_like(wo_share[:, out_rows:, :])
    grad_ref[:, 2 * hd * heads_here + piece :, :] = jnp.zeros_like(
        grad_ref[:, 2 * hd * heads_here + piece :, :]
    )
    for j in range(ring):
        loads[("wo", j)].wait()

    def project(i, carry):
        here = rows_of(i * tile, tile, tile)
        attended = dot(act_ref[0, here, :], wo_all[...], 1, 0) + b_out
        middle = hidden_ref[here, :] + attended
        middle_ref[here, :] = middle
        layer_ref[here, :] = middle + b_down
        mid_ref[here, :] = layer_norm(middle, mid_gain, mid_shift).astype(BF)
        grad_down = grad_out_ref[here, :].astype(BF)
        down_ref[here, :] = grad_down
        grad_in_ref[here, :] = jnp.zeros((tile, width), F32)
        return carry + jnp.sum(grad_down.astype(F32), 0, keepdims=True)

    zero_row = jnp.zeros((1, width), F32)
    grad_b_down = lax.fori_loop(0, count // tile, project, zero_row)
    mid_t[...] = jnp.transpose(mid_ref[...])
    down_t[...] = jnp.transpose(down_ref[...])

    half_width = width // 2

    def half_of(share, total_ref, at, part, x_first):
        window = pl.ds(part * half_width, half_width)
        here = bufs[5 * at : 5 * at + 5]
        return Reduce(
            place, share, here, total_ref.at[window], rsend, rrecv, at, x_first, part * half_width
        )

    early = (half_of(wd_all, wd_sum, 0, 0, False), half_of(wu_all, wu_sum, 1, 0, True))
    late = (half_of(wd_all, wd_sum, 2, 1, False), half_of(wu_all, wu_sum, 3, 1, True))
    out = Reduce(place, wo_share, bufs[20:25], wo_sum, rsend, rrecv, 4, True)
    group = 2 * hd
    packs = [
        Reduce(
            place,
            wu_all,
            bufs[25 + 5 * i : 30 + 5 * i],
            pack_held.at[pl.ds(group * i, group)],
            rsend,
            rrecv,
            5 + i,
            i % 2 == 0,
            group * i,
        )
        for i in range(heads_here + 1)
    ]

    big = count // 2

    def feed_shard(j, carry):
        s = shard_of(j)
        for i, hbm, ref in ((0, wu_hbm, wu_all), (1, wd_hbm, wd_all)):
            pltpu.make_async_copy(hbm, ref.at[s], lsem.at[ring + 2 * j + i]).wait()
        b_up = bias_ref[s, 0:1, pack_lanes:]

        def feed(i, carry):
            here = rows_of(i * big, big, big)
            u = dot(mid_ref[here, :], wu_all[s], 1, 0) + b_up
            grad_act = dot(down_ref[here, :], wd_all[s], 1, 1)
            square = u * u
            t = jnp.tanh(0.7978845608028654 * (u + 0.044715 * u * square))
            act = (0.5 * u * (1.0 + t)).astype(BF)
            slope = 0.5 * (1.0 + t) + (0.5 * 0.7978845608028654) * u * (1.0 - t * t) * (
                1.0 + 0.134145 * square
            )
            grad_up = (grad_act * slope).astype(BF)
            act_ref[s, here, :] = act
            gup_ref[s, here, :] = grad_up
            layer_ref[here, :] += dot(act, wd_all[s], 1, 0)
            grad_in_ref[here, :] += dot(grad_up, wu_all[s], 1, 1)
            return carry + jnp.sum(grad_up.astype(F32), 0, keepdims=True)

        grad_b_up = lax.fori_loop(0, count // big, feed, jnp.zeros((1, wu_all.shape[2]), F32))
        vector_held[0, pl.ds(s, 1), pack_lanes:] = grad_b_up
        return carry

    lax.fori_loop(0, ring, feed_shard, 0)
    layer_copy = pltpu.make_async_copy(layer_ref, layer_out_ref, lsem.at[3 * ring + 6])
    layer_copy.start()
    load("normed", normed_hbm, mid_ref)

    def middle_back(i, carry):
        here = rows_of(i * tile, tile, tile)
        middle = middle_ref[here, :]
        center = middle - jnp.mean(middle, -1, keepdims=True)
        scale = lax.rsqrt(jnp.mean(center * center, -1, keepdims=True) + EPSILON)
        unit = center * scale
        grad = grad_in_ref[here, :]
        grad_unit = grad * mid_gain
        grad_middle = grad_out_ref[here, :] + scale * (
            grad_unit
            - jnp.mean(grad_unit, -1, keepdims=True)
            - unit * jnp.mean(grad_unit * unit, -1, keepdims=True)
        )
        middle_ref[here, :] = grad_middle
        grad_attn = grad_middle.astype(BF)
        down_ref[here, :] = grad_attn
        sums = (
            jnp.sum(grad_attn.astype(F32), 0, keepdims=True),
            jnp.sum(grad * unit, 0, keepdims=True),
            jnp.sum(grad, 0, keepdims=True),
        )
        return tuple(x + y for x, y in zip(carry, sums))

    sums = lax.fori_loop(0, count // tile, middle_back, (zero_row,) * 3)
    for i, value in enumerate(sums + (grad_b_down,)):
        vector_held[0, ring + 2 + i : ring + 3 + i, 0:width] = value
    for i in range(ring):
        here = slice(i * out_rows, (i + 1) * out_rows)
        g_ref[here, :] = dot(wo_all[here, :], down_ref[...], 1, 1).astype(BF)

    def g_copy(slot, to):
        return remote(
            g_ref.at[pl.ds(HEADS_AT[to][slot] * hd, hd)],
            g_all.at[slot, :, own],
            gsend.at[slot, to],
            grecv.at[slot, place.shift_to(to) - 1],
            (place.d, to),
        )

    for slot in range(heads_here):
        for to in range(ring):

            @pl.when(m == to)
            def _(slot=slot, to=to):
                row = HEADS_AT[to][slot] * hd
                g_all[slot, :, own] = g_ref[row : row + hd, :]

            @pl.when(m != to)
            def _(slot=slot, to=to):
                g_copy(slot, to).start()

    for j in range(ring):
        here = rows_of(shard_of(j) * out_rows, out_rows, 16)
        wo_share[shard_of(j), 0:out_rows, :] = dot(
            context_ref[here, :], down_ref[...], 1, 0
        ).astype(BF)
        out.copy(0, shard_of(j)).start()

    def weigh_shard(j, carry):
        s = shard_of(j)

        def weigh(i, carry):
            here = lanes(i * 256, 256)
            wu_all[s, :, here] = dot(mid_t[...], gup_ref[s, :, here], 1, 0).astype(BF)
            wd_all[s, :, here] = dot(down_t[...], act_ref[s, :, here], 1, 0).astype(BF)
            return carry

        lax.fori_loop(0, wu_all.shape[2] // 256, weigh, 0)
        for item in early + late:
            item.copy(0, s).start()

        @pl.when(j > 0)
        def _():
            for item in early:
                item.fold_one(0, shard_of(j - 1))

        return carry

    lax.fori_loop(0, ring, weigh_shard, 0)
    for item in early:
        item.fold_one(0, shard_of(ring - 1))

    def fold_late(j, carry):
        for item in late:
            item.fold_one(0, shard_of(j))
        return carry

    lax.fori_loop(0, ring, fold_late, 0)
    out.fold(0)
    for name in ("v", "qk", "lse", "exact"):
        loads[name].wait()

    def qk_copy(h, to):
        return remote(
            qk_ref.at[h, :, pl.ds(to * count, count)],
            grad_ref.at[place.shard(h), rows_of(2 * hd * h, 2 * hd, 2 * hd)],
            qsend.at[h, to],
            qrecv.at[h, place.shift_to(to) - 1],
            (place.d, to),
        )

    v_row = 2 * hd * heads_here

    def v_copy(i, j):
        shard, row, rows, _, row_there = FRESH[i]
        return remote(
            v_ref.at[pl.ds(row_there, rows), lanes(place.z(j) * count, count)],
            grad_ref.at[shard, pl.ds(v_row + row, rows)],
            vsend.at[i, j - 1],
            vrecv.at[i, j - 1],
            place.to_z(j),
        )

    def moved_copy(i):
        to, row, rows, _, row_there = MOVED[i]
        return remote(
            v_ref.at[pl.ds(row_there, rows)],
            first_ref.at[pl.ds(row, rows)],
            fsend.at[0],
            frecv.at[0],
            (place.d, to),
        )

    def send_fresh(slot):
        for i, (shard, row, rows, at, row_there) in enumerate(FRESH):
            if (row_there + rows > 2 * hd) != (slot == 2):
                continue

            @pl.when(m == at)
            def _(i=i, shard=shard, row=row, rows=rows, row_there=row_there):
                for j in range(1, ring):
                    v_copy(i, j).start()
                grad_ref[shard, v_row + row : v_row + row + rows, :] = v_ref[
                    pl.ds(row_there, rows), own
                ]

    def send_reused():
        for i, move in enumerate(MOVED):

            @pl.when(m == move[3])
            def _(i=i):
                moved_copy(i).start()

        for at, row, rows, row_there in KEPT:

            @pl.when(m == at)
            def _(row=row, rows=rows, row_there=row_there):
                first_ref[row : row + rows, :] = v_ref[row_there : row_there + rows, :]

    ones = jnp.ones((8, count), BF)

    def process(i):
        if i == 0:
            for name in ("normed", "wt"):
                loads[name].wait()
            for k in range(ring):
                early[1].copy(0, k).wait_send()
                late[1].copy(0, k).wait_send()
        if i < heads_here:
            for j in range(1, ring):
                remote(
                    qk_ref.at[i, :, own],
                    grad_ref.at[0, pl.ds(2 * hd * i, 2 * hd)],
                    qsend.at[i, 0],
                    qrecv.at[i, j - 1],
                    place.to_z(j),
                ).wait_recv()
        begin = group * i
        here = slice(begin, begin + group)
        for k in range(ring):
            wu_all[k, here, :] = dot(grad_ref[k, here, :], mid_ref[...], 1, 0).astype(BF)
            packs[i].copy(0, k).start()
        for k in range(ring):
            sums = dot(ones, grad_ref[k, here, :], 1, 1)
            vector_held[0, k : k + 1, here] = sums[0:1]
        weights = jnp.concatenate([wt_all[k, here, :] for k in range(ring)], 0)

        def add(t, carry):
            toks = lanes(t * tile, tile)
            grads = jnp.concatenate([grad_ref[k, here, toks] for k in range(ring)], 0)
            part = dot(grads, weights, 0, 0)
            rows = rows_of(t * tile, tile, tile)
            grad_in_ref[rows, :] = part if i == 0 else grad_in_ref[rows, :] + part
            return carry

        lax.fori_loop(0, count // tile, add, 0)

    boundary = length_ref[0]
    block = count
    def attend_back(h, carry):
        here_h = rows_of(hd * h, hd, hd)
        keys[...] = jnp.transpose(qk_ref[h, hd : 2 * hd, :])
        vals[...] = jnp.transpose(v_ref[here_h, :])
        for j in range(1, ring):
            remote(
                g_ref.at[pl.ds(0, hd)],
                g_all.at[h, :, own],
                gsend.at[h, 0],
                grecv.at[h, j - 1],
                place.to_z(j),
            ).wait_recv()
        delta[...] = jnp.sum(
            g_all[h].astype(F32) * exact_ref[here_h, :], 0, keepdims=True
        )
        for qi in reversed(range(ring)):
            query_start = qi * block
            here = slice(query_start, query_start + block)
            q = qk_ref[h, 0:hd, here]
            g = g_all[h, :, here]
            grad_q = None
            for ki in range(qi + 1):
                key_start = ki * block
                there = slice(key_start, key_start + block)
                key_t = qk_ref[h, hd : 2 * hd, there]
                scores = dot(keys[there, :], q, 1, 0) - lse_ref[h, :, here]
                if ki == qi:
                    scores = jnp.where(
                        diagonal_mask(scores, key_start, query_start), scores, NEG_LARGE
                    )
                elif key_start < half <= query_start:
                    scores = scores + other_document(boundary, key_start, query_start)
                p = jnp.exp(scores)
                grad_p = dot(vals[there, :], g, 1, 0)
                grad_s = (p * (grad_p - delta[:, here])).astype(BF)
                grad_v = dot(g, p.astype(BF), 1, 1)
                grad_k = dot(q, grad_s, 1, 1)
                part_q = dot(key_t, grad_s, 1, 0)
                grad_q = part_q if grad_q is None else grad_q + part_q
                if qi < ring - 1:
                    grad_v, grad_k = grad_v + dv[:, there], grad_k + dk[:, there]
                if ki < qi:
                    dv[:, there], dk[:, there] = grad_v, grad_k
            qk_ref[h, 0:hd, here] = (grad_q * (hd**-0.5)).astype(BF)
            qk_ref[h, hd : 2 * hd, here] = grad_k.astype(BF)
            v_ref[here_h, here] = grad_v.astype(BF)

            @pl.when(m == qi)
            def _(here=here):
                grad_ref[place.shard(h), rows_of(2 * hd * h, 2 * hd, 2 * hd), :] = qk_ref[
                    h, :, here
                ]

            @pl.when(m != qi)
            def _(qi=qi):
                qk_copy(h, qi).start()

        @pl.when(h == 1)
        def _():
            send_fresh(1)
            for item in early:
                item.fold(1)

        return carry

    lax.fori_loop(0, heads_here, attend_back, 0)
    send_fresh(2)
    send_reused()
    late = late + (out,)
    for item in late:
        item.fold(1)
    process(0)
    process(1)
    for item in early:
        item.fold(2)
    packs[0].fold(0)
    packs[1].fold(0)
    packs[0].fold(1)
    for item in late:
        item.fold(2)
    packs[1].fold(1)
    packs[0].fold(2)
    for to in range(ring):

        @pl.when(m != to)
        def _(to=to):
            for slot in range(heads_here):
                g_copy(slot, to).wait_send()

    for i, (shard, row, rows, at, row_there) in enumerate(FRESH):

        @pl.when(m == at)
        def _(i=i):
            for j in range(1, ring):
                v_copy(i, j).wait_send()

        @pl.when(m != at)
        def _(i=i, shard=shard, row=row, rows=rows, at=at, row_there=row_there):
            shift = lax.rem(m - at + ring, ring)
            remote(
                v_ref.at[pl.ds(row_there, rows), own],
                grad_ref.at[shard, pl.ds(v_row + row, rows)],
                vsend.at[i, shift - 1],
                vrecv.at[i, shift - 1],
                place.to_z(shift),
            ).wait_recv()

    for i, move in enumerate(MOVED):

        @pl.when(m == move[3])
        def _(i=i):
            moved_copy(i).wait_send()

        @pl.when(m == move[0])
        def _(i=i):
            moved_copy(i).wait_recv()

    process(2)
    process(3)
    for item in early:
        item.fold_pair()

    def input_back(i, carry):
        here = rows_of(i * tile, tile, tile)
        grad = grad_in_ref[here, :]
        value = hidden_ref[here, :]
        center = value - jnp.mean(value, -1, keepdims=True)
        scale = lax.rsqrt(jnp.mean(center * center, -1, keepdims=True) + EPSILON)
        unit = center * scale
        grad_unit = grad * pre_gain
        grad_in_ref[here, :] = middle_ref[here, :] + scale * (
            grad_unit
            - jnp.mean(grad_unit, -1, keepdims=True)
            - unit * jnp.mean(grad_unit * unit, -1, keepdims=True)
        )
        sums = (
            jnp.sum(grad * unit, 0, keepdims=True),
            jnp.sum(grad, 0, keepdims=True),
        )
        return tuple(x + y for x, y in zip(carry, sums))

    sums = lax.fori_loop(0, count // tile, input_back, (zero_row,) * 2)
    for i, value in enumerate(sums):
        vector_held[0, ring + i : ring + 1 + i, 0:width] = value

    turned = jnp.logical_or(m == 1, m == 2)

    def natural(own_row):
        parts = []
        for i in range(heads_here):
            here, turn = group * i, group * ((i - 1) % heads_here)
            parts.append(
                jnp.where(turned, own_row[:, turn : turn + hd], own_row[:, here : here + hd])
            )
        parts.append(jnp.zeros((1, own_row.shape[1] - hd * heads_here), F32))
        return jnp.concatenate(parts, 1)

    routes = [place.to_core, place.to_x, place.to_y]
    routes += [place.to_plane(step) for step in place.steps()]
    bit = 1
    while bit < ring:
        routes.append((place.d, m + bit - 2 * bit * lax.rem(m // bit, 2)))
        bit *= 2

    def vector_copy(k):
        return remote(
            vector_held.at[k], vector_came.at[k], wsend.at[k], wrecv.at[k], routes[k]
        )

    def vector_fold(k):
        vector_copy(k).wait_recv()
        value = vector_held[k] + vector_came[k]
        if k + 1 < len(routes):
            vector_held[k + 1] = value
            vector_copy(k + 1).start()
        else:
            own_row = value[0:1]
            for s in range(1, ring):
                own_row = jnp.where(m == s, value[s : s + 1], own_row)
            vector_sum[...] = jnp.concatenate([value[ring : ring + 6], own_row, natural(own_row)], 0)

    vector_copy(0).start()
    first, second, third, fourth = packs
    second.fold(2)
    third.fold(0)
    fourth.fold(0)
    vector_fold(0)
    for item in late:
        item.fold_pair()
    third.fold(1)
    fourth.fold(1)
    vector_fold(1)
    first.fold_pair()
    second.fold_pair()
    for item in early:
        item.finish_sum()
    third.fold(2)
    fourth.fold(2)
    vector_fold(2)
    first.finish_sum()
    second.finish_sum()
    for item in late:
        item.finish_sum()
    third.fold_pair()
    fourth.fold_pair()
    for item in early:
        item.spread(6)
    for k in range(3, len(routes) - 1):
        vector_fold(k)
    first.spread(6)
    second.spread(6)
    third.finish_sum()
    fourth.finish_sum()
    for item in late:
        item.spread(6)
    for item in early:
        item.spread(7)
    vector_fold(len(routes) - 1)
    third.spread(6)
    fourth.spread(6)
    for item in late + (first, second, third, fourth):
        item.spread(7)
    layer_copy.wait()
    everything = early + late + tuple(packs)
    for item in everything:
        item.wait(7)
        item.drain(1 if item in (early[1], late[1]) else 0)
    for k in range(len(routes)):
        vector_copy(k).wait_send()
    for to in range(ring):

        @pl.when(m != to)
        def _(to=to):
            for h in range(heads_here):
                qk_copy(h, to).wait_send()

    for i in range(heads_here):
        at = rows_of(group * jnp.where(turned, (i - 1) % heads_here, i), hd, hd)
        wq_sum[hd * i : hd * i + hd, :] = pack_held[at, :]
        at = rows_of(group * jnp.where(turned, (i - 1) % heads_here, i) + hd, hd, hd)
        wk_sum[hd * i : hd * i + hd, :] = pack_held[at, :]
    wv_sum[...] = pack_held[v_row : v_row + piece, :]


def backward_call(
    ring, heads_here, planes, length, context, hidden, grad_out, pre_gain, b_out, mid_gain, mid_shift,
    b_down, bias,
    qk, v, lse, exact, normed, wt, wo, wo_far, wu, wu_far, wd, wd_far, piece,
):
    count, width = hidden.shape
    total = ring * count
    hd = HEAD_DIM
    others = ring - 1
    sds = jax.ShapeDtypeStruct
    dma = pltpu.SemaphoreType.DMA
    hops = 3 + (planes.bit_length() - 1) + (ring.bit_length() - 1)
    stages = 8 + planes.bit_length() - 1
    pack_rows = wt.shape[1]
    out_pad = wo.shape[0] + -wo.shape[0] % (16 * PLANE)
    sizes = [wd.shape[0] // 2, wu.shape[0] // 2] * 2 + [out_pad] + [2 * hd] * (heads_here + 1)
    bufs = [buf for rows_ in sizes for buf in Reduce.buffers(rows_, width, planes)]
    vector = (ring + 6 + -(ring + 6) % 8, bias.shape[2])
    vm = pltpu.VMEM
    return pl.pallas_call(
        functools.partial(backward_kernel, ring, heads_here, planes),
        out_shape=(
            sds(hidden.shape, F32),
            sds(hidden.shape, F32),
            sds((piece, total), BF),
            sds((heads_here * hd, width), BF),
            sds((heads_here * hd, width), BF),
            sds((piece, width), BF),
            sds((out_pad, width), BF),
            sds(wu.shape, BF),
            sds(wd.shape, BF),
            sds((8, vector[1]), F32),
        ),
        in_specs=[SM] + [VM] * 9 + [ANY] * 12,
        out_specs=[ANY] + [VM] * 9,
        scratch_shapes=[
            vm((count, width), F32),
            vm(qk.shape, BF),
            vm(v.shape, BF),
            vm(lse.shape, F32),
            vm(exact.shape, F32),
            vm(wt.shape, BF),
            vm((ring * wo.shape[0], width), BF),
            vm((ring,) + wu.shape, BF),
            vm((ring,) + wd.shape, BF),
            vm((count, width), F32),
            vm((count, width), BF),
            vm((width, count), BF),
            vm((count, width), BF),
            vm((width, count), BF),
            vm((ring, count, width), BF),
            vm((ring, count, width), BF),
            vm((width, count), BF),
            vm((pack_rows, width), BF),
            vm((ring, out_pad, width), BF),
            vm((heads_here, hd, total), BF),
            vm((total, hd), BF),
            vm((total, hd), BF),
            vm((1, total), F32),
            vm((hd, total), F32),
            vm((hd, total), F32),
            vm((ring, pack_rows, count), BF),
            vm((hops,) + vector, F32),
            vm((hops,) + vector, F32),
            dma((3 * ring + 7,)),
            dma((heads_here, ring)),
            dma((heads_here, others)),
            dma((heads_here, ring)),
            dma((heads_here, others)),
            dma((len(FRESH), others)),
            dma((len(FRESH), others)),
            dma((1,)),
            dma((1,)),
            dma((5 + heads_here + 1, stages, ring)),
            dma((5 + heads_here + 1, stages, ring)),
            dma((hops,)),
            dma((hops,)),
        ]
        + bufs,
        compiler_params=pltpu.CompilerParams(
            collective_id=1, has_side_effects=True, vmem_limit_bytes=67043328
        ),
        name="backward",
    )(
        length, context, hidden, grad_out, pre_gain, b_out, mid_gain, mid_shift, b_down, bias, qk, v, lse, exact,
        normed, wt, wo, wo_far, wu, wu_far, wd, wd_far,
    )


def finish_kernel(count_in, turned, pieces, vector_ref, *refs):
    ins, refs = refs[:count_in], refs[count_in:]
    outs, refs = refs[:count_in], refs[count_in:]
    rows, refs = refs[: len(pieces)], refs[len(pieces) :]
    held, wide, sem_in, sem_out = refs[:count_in], refs[count_in:-2], refs[-2], refs[-1]
    rising = iter(wide)
    loads = [pltpu.make_async_copy(a, b, sem_in.at[i]) for i, (a, b) in enumerate(zip(ins, held))]
    for load in loads:
        load.start()
    for ref, (row, start, size) in zip(rows, pieces):
        ref[...] = jnp.reshape(vector_ref[row : row + 1, start : start + size], (size,))
    stores = []
    for i in range(count_in):
        loads[i].wait()
        source = held[i]
        if source.dtype != F32:
            into = next(rising)
            value = source[0 : into.shape[0], :]
            if i == turned:
                value = jnp.transpose(value)
            into[...] = value.astype(F32)
            source = into
        stores.append(pltpu.make_async_copy(source, outs[i], sem_out.at[i]))
        stores[i].start()
    for store in stores:
        store.wait()


def finish_call(vector, pieces, arrays, rows, turned):
    sds = jax.ShapeDtypeStruct
    dma = pltpu.SemaphoreType.DMA
    shapes = [(rows_, array.shape[1]) for array, rows_ in zip(arrays, rows)]
    return pl.pallas_call(
        functools.partial(finish_kernel, len(arrays), turned, pieces),
        out_shape=[sds(shape, F32) for shape in shapes] + [sds((p[2],), F32) for p in pieces],
        in_specs=[VM] + [ANY] * len(arrays),
        out_specs=[ANY] * len(arrays) + [VM] * len(pieces),
        scratch_shapes=[pltpu.VMEM(array.shape, array.dtype) for array in arrays]
        + [pltpu.VMEM(s, F32) for s, array in zip(shapes, arrays) if array.dtype != F32]
        + [dma((len(arrays),)), dma((len(arrays),))],
        compiler_params=pltpu.CompilerParams(vmem_limit_bytes=VMEM_LIMIT),
        name="finish",
    )(vector, *arrays)


def shards(
    hidden_in,
    first_values,
    first_length,
    pre_gain,
    pre_shift,
    w_query,
    b_query,
    w_key,
    w_value,
    b_value,
    w_out,
    b_out,
    mid_gain,
    mid_shift,
    w_up,
    b_up,
    w_down,
    b_down,
    grad_out,
):
    ring = lax.axis_size("mp")
    m = lax.axis_index("mp")
    hd = HEAD_DIM
    count, width = hidden_in.shape
    head_width = w_query.shape[1]
    heads_here = head_width // hd
    piece = w_value.shape[1]
    context_t, normed, qk, v, lse, exact, wt_all, bias_all, wo_far, wu_far, wd_far = forward_call(
        ring,
        heads_here,
        first_length,
        hidden_in,
        pre_gain,
        pre_shift,
        w_query.T,
        w_key.T,
        w_value.T,
        b_query,
        b_value,
        b_up,
        first_values.T,
        w_out,
        w_up,
        w_down,
    )
    layer_out, grad_input, grad_first, wq_sum, wk_sum, wv_sum, wo_sum, wu_sum, wd_sum, vector = backward_call(
        ring,
        heads_here,
        lax.axis_size("dp") // PLANE,
        first_length,
        context_t,
        hidden_in,
        grad_out,
        pre_gain,
        b_out,
        mid_gain,
        mid_shift,
        b_down,
        bias_all,
        qk,
        v,
        lse,
        exact,
        normed,
        wt_all,
        w_out,
        wo_far,
        w_up,
        wu_far,
        w_down,
        wd_far,
        piece,
    )
    pack_rows = wt_all.shape[1]
    pieces = [(i, 0, width) for i in range(6)] + [
        (7, 0, head_width),
        (6, 2 * head_width, piece),
        (6, pack_rows, b_up.shape[0]),
    ]
    arrays = [layer_out, grad_input, wu_sum, wd_sum, grad_first, wq_sum, wk_sum, wo_sum, wv_sum]
    rows = [count, count, width, w_down.shape[0], piece, head_width, head_width, head_width, piece]
    done = finish_call(vector, pieces, arrays, rows, 3)
    layer_out, grad_input, wu_sum, wd_sum, grad_first, wq_sum, wk_sum, wo_sum, wv_sum = done[:9]
    pre_gain_sum, pre_shift_sum, b_out_sum, mid_gain_sum, mid_shift_sum, b_down_sum = done[9:15]
    b_query_sum, b_value_sum, b_up_sum = done[15:]
    return (
        layer_out,
        grad_input,
        grad_first.T,
        pre_gain_sum,
        pre_shift_sum,
        wq_sum.T,
        b_query_sum,
        wk_sum.T,
        wv_sum.T,
        b_value_sum,
        wo_sum,
        b_out_sum,
        mid_gain_sum,
        mid_shift_sum,
        wu_sum,
        b_up_sum,
        wd_sum,
        b_down_sum,
    )


def solution(mesh):
    rows, cols = P(("dp", "mp"), None), P(None, "mp")
    return jax.shard_map(
        shards,
        mesh=mesh,
        in_specs=(
            rows,
            P("dp", "mp"),
            P("dp"),
            P(),
            P(),
            cols,
            P("mp"),
            cols,
            cols,
            P("mp"),
            P("mp", None),
            P(),
            P(),
            P(),
            cols,
            P("mp"),
            P("mp", None),
            P(),
            rows,
        ),
        out_specs=(
            rows,
            rows,
            P("dp", "mp"),
            P(),
            P(),
            cols,
            P("mp"),
            cols,
            cols,
            P("mp"),
            P("mp", None),
            P(),
            P(),
            P(),
            cols,
            P("mp"),
            P("mp", None),
            P(),
        ),
        check_vma=False,
    )
```
